32 devices in a mesh: dp: 8 (over z, y), tensor: 4 (over x, core).
Axes of the slice: x: 2, y: 2, z: 4, core: 2. Of those that a mesh axis runs over, the one named last changes fastest.
Arguments:
- tokens: bfloat16 [7168, 1024], P(('dp', 'tensor')), may hold values from -6 to 6
- frames: bfloat16 [24000, 1024], P(('dp', 'tensor')), may hold values from -6 to 6, as said below
- cotangent: bfloat16 [7168, 1024], P(('dp', 'tensor')), may hold values from -6 to 6
- attention_weights: bfloat16 [2, 4, 1024, 1024], P(None, None, 'dp', 'tensor'), as said below
- dense_weights: bfloat16 [2, 1024, 4, 1024], P(None, 'dp', None, 'tensor'), may hold values from -0.1875 to 0.1875
- unit_bias: bfloat16 [16, 512], P('tensor', 'dp'), may hold values from -3 to 3, as said below
- norm_bias: bfloat16 [9, 1024], P(None, 'dp'), as said below
- attention_mean: float32 [2, 4, 1024, 1024], P(None, None, 'dp', 'tensor'), may hold values from -0.0625 to 0.0625
- dense_mean: float32 [2, 1024, 4, 1024], P(None, 'dp', None, 'tensor'), may hold values from -0.0625 to 0.0625
- unit_mean: float32 [16, 512], P('tensor', 'dp'), may hold values from -0.0625 to 0.0625
- norm_mean: float32 [9, 1024], P(None, 'dp'), may hold values from -0.0625 to 0.0625
- attention_square: float32 [2, 4, 1024, 1024], P(None, None, 'dp', 'tensor'), as said below
- dense_square: float32 [2, 1024, 4, 1024], P(None, 'dp', None, 'tensor'), as said below
- unit_square: float32 [16, 512], P('tensor', 'dp'), as said below
- norm_square: float32 [9, 1024], P(None, 'dp'), as said below
Outputs:
- layer_out: bfloat16 [7168, 1024], P(('dp', 'tensor'))
- input_gradient: float32 [7168, 1024], P(('dp', 'tensor'))
- frame_gradient: float32 [24000, 1024], P(('dp', 'tensor'))
- attention_gradient: float32 [2, 4, 1024, 1024], P(None, None, 'dp', 'tensor')
- dense_gradient: float32 [2, 1024, 4, 1024], P(None, 'dp', None, 'tensor')
- unit_gradient: float32 [16, 512], P('tensor', 'dp')
- norm_gradient: float32 [9, 1024], P(None, 'dp')
- attention_mean_new: float32 [2, 4, 1024, 1024], P(None, None, 'dp', 'tensor')
- dense_mean_new: float32 [2, 1024, 4, 1024], P(None, 'dp', None, 'tensor')
- unit_mean_new: float32 [16, 512], P('tensor', 'dp')
- norm_mean_new: float32 [9, 1024], P(None, 'dp')
- attention_square_new: float32 [2, 4, 1024, 1024], P(None, None, 'dp', 'tensor')
- dense_square_new: float32 [2, 1024, 4, 1024], P(None, 'dp', None, 'tensor')
- unit_square_new: float32 [16, 512], P('tensor', 'dp')
- norm_square_new: float32 [9, 1024], P(None, 'dp')
- attention_step: float32 [2, 4, 1024, 1024], P(None, None, 'dp', 'tensor')
- dense_step: float32 [2, 1024, 4, 1024], P(None, 'dp', None, 'tensor')
- unit_step: float32 [16, 512], P('tensor', 'dp')
- norm_step: float32 [9, 1024], P(None, 'dp')
- weight_norms: float32 [27], replicated
- step_norms: float32 [27], replicated
The draws below stay inside these ranges and needn't reach their ends.
Inputs may be any that keep to these rules, and one draw needn't show every extreme that they name: `frames`: independent entries of spread about one. `attention_weights`: entries are independent and normal; the output matrices have a larger spread than the others. `unit_bias`: independent entries of spread about one half. `norm_bias`: gains (rows 0, 2, 4) lie between 0.5 and 1.5; the other rows are small and of both signs. `attention_square`: Positive. `dense_square`: Positive. `unit_square`: Positive. `norm_square`: Positive.
All inputs are finite; a program needn't handle non-finite values.
Results may differ from the reference program's by a relative error of at most 0.02.
Values may be sent and summed in bfloat16 or wider, within the bound.
A program may use at most 192 MiB of HBM per device.

```python
import math
import jax
import jax.numpy as jnp
from jax import lax

D = 1024
HEADS = 16
HD = 64
FF = 4096
L = 448
FRAMES = 1500
CLIPS_DP = 2
TOKENS = 7168
FRAME_ROWS = 24000


def drawn_values(key, array_dims, scale):
    return jnp.clip(jax.random.normal(key, array_dims, jnp.float32), -6.0, 6.0) * scale


def draw_frames(key, part):
    return drawn_values(key, (FRAME_ROWS, D), 1.0).astype(jnp.bfloat16)


def draw_unit_bias(key, part):
    return drawn_values(key, (HEADS, 8 * HD), 0.5).astype(jnp.bfloat16)


def draw_attention_weights(key, part):
    factors = jnp.array([1.2, 1.2, 1.0, 6.0], jnp.float32)[None, :, None, None]
    return (jax.random.normal(key, (2, 4, D, D), jnp.float32) * factors / math.sqrt(D)).astype(jnp.bfloat16)


def draw_norm_bias(key, part):
    gain_key = jax.random.fold_in(key, 11)
    shift_key = jax.random.fold_in(key, 12)
    gains = jax.random.uniform(gain_key, (9, D), jnp.float32, 0.5, 1.5)
    shifts = 0.3 * jax.random.normal(shift_key, (9, D), jnp.float32)
    row_index = jnp.arange(9)
    is_gain = (row_index % 2 == 0) & (row_index < 6)
    return jnp.where(is_gain[:, None], gains, shifts).astype(jnp.bfloat16)


def second_moment(key, array_dims):
    spread = jax.random.uniform(key, array_dims, jnp.float32, math.log(0.1), math.log(10.0))
    return jnp.exp(spread) / TOKENS


def draw_attention_square(key, part):
    return second_moment(key, (2, 4, D, D))


def draw_dense_square(key, part):
    return second_moment(key, (2, D, 4, D))


def draw_unit_square(key, part):
    return second_moment(key, (HEADS, 8 * HD)) * 64.0


def draw_norm_square(key, part):
    return second_moment(key, (9, D))


def shard_levels(key, shape, pieces, least, largest):
    factor_of = 1.0
    for position, blocks in pieces:
        steps = jax.random.uniform(jax.random.fold_in(jax.random.fold_in(key, 6), position), (blocks,), jnp.float32, least / len(pieces), largest / len(pieces))
        factor_of = factor_of * jnp.repeat(jnp.exp(steps), shape[position] // blocks).reshape((-1,) + (1,) * (len(shape) - 1 - position))
    return factor_of


def normal_values(rng, extent, scale, bound, shards=(), dtype=jnp.bfloat16):
    drawn = scale * jax.random.normal(rng, extent, jnp.float32)
    if shards:
        drawn = drawn * shard_levels(rng, extent, shards, -0.22, 0.18)
    return jnp.clip(drawn, -bound, bound).astype(dtype)


def setup_inputs(seed: int = 0) -> dict:
    splits = jax.random.split(jax.random.key(seed), 16)
    tokens = normal_values(splits[0], (TOKENS, D), 1.0, 6.0, ((0, 32),))
    frames = draw_frames(jax.random.fold_in(splits[15], 71), 0)
    cotangent = normal_values(splits[2], (TOKENS, D), 1.0, 6.0, ((0, 32),))
    attention_weights = draw_attention_weights(jax.random.fold_in(splits[15], 71), 0)
    dense_weights = normal_values(splits[4], (2, D, 4, D), D ** -0.5, 0.1875, ((1, 8), (3, 4)))
    unit_bias = draw_unit_bias(jax.random.fold_in(splits[15], 71), 0)
    norm_bias = draw_norm_bias(jax.random.fold_in(splits[15], 71), 0)
    attention_mean = normal_values(splits[7], (2, 4, D, D), TOKENS ** -0.5, 0.0625, ((2, 8), (3, 4)), jnp.float32)
    dense_mean = normal_values(splits[8], (2, D, 4, D), TOKENS ** -0.5, 0.0625, ((1, 8), (3, 4)), jnp.float32)
    unit_mean = normal_values(splits[9], (HEADS, 8 * HD), TOKENS ** -0.5, 0.0625, ((0, 4), (1, 8)), jnp.float32)
    norm_mean = normal_values(splits[10], (9, D), TOKENS ** -0.5, 0.0625, ((1, 8),), jnp.float32)
    attention_square = draw_attention_square(jax.random.fold_in(splits[15], 71), 0)
    dense_square = draw_dense_square(jax.random.fold_in(splits[15], 71), 0)
    unit_square = draw_unit_square(jax.random.fold_in(splits[15], 71), 0)
    norm_square = draw_norm_square(jax.random.fold_in(splits[15], 71), 0)
    return dict(tokens=tokens, frames=frames, cotangent=cotangent, attention_weights=attention_weights, dense_weights=dense_weights, unit_bias=unit_bias, norm_bias=norm_bias, attention_mean=attention_mean, dense_mean=dense_mean, unit_mean=unit_mean, norm_mean=norm_mean, attention_square=attention_square, dense_square=dense_square, unit_square=unit_square, norm_square=norm_square)


@jax.custom_vjp
def low(v):
    return lax.optimization_barrier(v.astype(jnp.bfloat16)).astype(jnp.float32)

@jax.custom_vjp
def low_back(v):
    return v

def low_keep(v):
    return (low(v), None)

def low_pass(kept, grad):
    return (grad,)

def back_keep(v):
    return (v, None)

def back_low(kept, grad):
    return (low(grad),)
low.defvjp(low_keep, low_pass)
low_back.defvjp(back_keep, back_low)

def product(left, right):
    return jnp.dot(left, right, precision=lax.Precision.HIGHEST)

def rounded(values):
    return low_back(low(values))

def layer_norm(values, gain_row, offset):
    centre = values - lax.optimization_barrier(jnp.mean(values, axis=-1, keepdims=True))
    spread = lax.optimization_barrier(jnp.mean(centre * centre, axis=-1, keepdims=True))
    return centre * lax.rsqrt(spread + 1e-05) * gain_row + offset

def gelu_value(values):
    return 0.5 * values * (1.0 + jax.scipy.special.erf(values * 0.7071067811865476))

def attention(queries, key_rows, values, causal):
    scores = jnp.einsum('clhd,cshd->chls', queries, key_rows, precision=lax.Precision.HIGHEST)
    scores = low_back(0.125 * scores)
    if causal:
        length = queries.shape[1]
        allowed = lax.broadcasted_iota(jnp.int32, (length, length), 0) >= lax.broadcasted_iota(jnp.int32, (length, length), 1)
        scores = jnp.where(allowed[None, None], scores, -1e+30)
    weights = jax.nn.softmax(scores, axis=-1)
    context = jnp.einsum('chls,cshd->clhd', low(weights), values, precision=lax.Precision.HIGHEST)
    return rounded(context)

def group_forward(attn, dense, unit_rows, norms, row_data, frame_data):
    clip_count = row_data.shape[0] // L
    first_in = low(layer_norm(row_data, norms[0], norms[1]))
    self_query = rounded(product(first_in, attn[0, 0]) + unit_rows[0])
    self_keys = rounded(product(first_in, attn[0, 1]))
    self_values = rounded(product(first_in, attn[0, 2]) + unit_rows[1])
    context = attention(self_query.reshape(clip_count, L, HEADS, HD), self_keys.reshape(clip_count, L, HEADS, HD), self_values.reshape(clip_count, L, HEADS, HD), True).reshape(-1, D)
    hidden_one = row_data + norms[6] + low_back(product(context, attn[0, 3].T))
    second_in = low(layer_norm(hidden_one, norms[2], norms[3]))
    cross_query = rounded(product(second_in, attn[1, 0]) + unit_rows[2])
    cross_keys = rounded(product(frame_data, attn[1, 1]))
    cross_values = rounded(product(frame_data, attn[1, 2]) + unit_rows[3])
    cross_context = attention(cross_query.reshape(clip_count, L, HEADS, HD), cross_keys.reshape(clip_count, FRAMES, HEADS, HD), cross_values.reshape(clip_count, FRAMES, HEADS, HD), False).reshape(-1, D)
    hidden_two = hidden_one + norms[7] + low_back(product(cross_context, attn[1, 3].T))
    third_in = low(layer_norm(hidden_two, norms[4], norms[5]))
    before = low_back(product(third_in, dense[0].reshape(D, FF)) + unit_rows[4:8].reshape(FF))
    activated = low(gelu_value(before))
    return hidden_two + norms[8] + low_back(product(activated, dense[1].reshape(D, FF).T))

def whole(attn, dense, unit_rows, norms, row_data, frame_data):
    group_rows = row_data.reshape(-1, CLIPS_DP * L, D)
    group_frames = frame_data.reshape(-1, CLIPS_DP * FRAMES, D)

    def one_group(paired):
        return group_forward(attn, dense, unit_rows, norms, paired[0], paired[1])
    return lax.map(jax.checkpoint(one_group), (group_rows, group_frames)).reshape(-1, D)

def to_rows(stored):
    return stored.reshape(HEADS, 8, HD).transpose(1, 0, 2).reshape(8, D)

def from_rows(row_form):
    return row_form.reshape(8, HEADS, HD).transpose(1, 0, 2).reshape(HEADS, 8 * HD)

def adapt(weight, gradient, moment, second):
    scaled_grad = gradient / TOKENS
    new_moment = 0.5 * moment + 0.5 * scaled_grad
    new_second = 0.5 * second + 0.5 * scaled_grad * scaled_grad
    direction = new_moment / (jnp.sqrt(new_second) + 1e-06) + 0.01 * weight
    return (new_moment, new_second, direction)

def square_rows(attn, dense, unit, norms):
    parts = [attn.reshape(8, -1), dense.reshape(2, -1), to_rows(unit), norms]
    return jnp.concatenate([lax.optimization_barrier(jnp.sum(block * block, axis=1)) for block in parts])

def reference(tokens, frames, cotangent, attention_weights, dense_weights, unit_bias, norm_bias, attention_mean, dense_mean, unit_mean, norm_mean, attention_square, dense_square, unit_square, norm_square):
    attn = attention_weights.astype(jnp.float32)
    dense = dense_weights.astype(jnp.float32)
    unit = unit_bias.astype(jnp.float32)
    norms = norm_bias.astype(jnp.float32)
    outputs, pullback = jax.vjp(whole, attn, dense, to_rows(unit), norms, tokens.astype(jnp.float32), frames.astype(jnp.float32))
    attn_grad, dense_grad, unit_rows_grad, norm_grad, input_grad, frame_grad = pullback(cotangent.astype(jnp.float32))
    unit_grad = from_rows(unit_rows_grad)
    attn_mom, attn_sec, attn_dir = adapt(attn, attn_grad, attention_mean, attention_square)
    dense_mom, dense_sec, dense_dir = adapt(dense, dense_grad, dense_mean, dense_square)
    unit_mom, unit_sec, unit_dir = adapt(unit, unit_grad, unit_mean, unit_square)
    norm_mom, norm_sec, norm_dir = adapt(norms, norm_grad, norm_mean, norm_square)
    weight_norms = jnp.sqrt(square_rows(attn, dense, unit, norms))
    step_norms = jnp.sqrt(square_rows(attn_dir, dense_dir, unit_dir, norm_dir))
    trust = weight_norms / step_norms
    attn_step = -0.3 * trust[0:8].reshape(2, 4, 1, 1) * attn_dir
    dense_step = -0.3 * trust[8:10].reshape(2, 1, 1, 1) * dense_dir
    unit_factor = from_rows(jnp.broadcast_to(trust[10:18][:, None], (8, D)))
    unit_step = -0.3 * unit_factor * unit_dir
    norm_step = -0.3 * trust[18:27][:, None] * norm_dir
    return (outputs.astype(jnp.bfloat16), input_grad, frame_grad, attn_grad, dense_grad, unit_grad, norm_grad, attn_mom, dense_mom, unit_mom, norm_mom, attn_sec, dense_sec, unit_sec, norm_sec, attn_step, dense_step, unit_step, norm_step, weight_norms, step_norms)
```

```python
from functools import partial

import jax
import jax.numpy as jnp
from jax import lax
from jax.experimental import pallas as pl
from jax.experimental.pallas import tpu as pltpu
from jax.sharding import Mesh, PartitionSpec as P

D = 1024
HEADS = 16
HD = 64
L = 448
FRAMES = 1500
MATS = 16
COLS = 256

learning_rate = 0.3
DT = pl.DeviceIdType.MESH
AXES = ("dp", "side", "core")


def place():
    dp = lax.axis_index("dp")
    return dp // 2, lax.rem(dp, 2), lax.axis_index("side"), lax.axis_index("core")


def device(z, y, x, c):
    return (z * 2 + y, x, c)


def greet_neighbours(levels):
    z, y, x, c = place()
    bar = pltpu.get_barrier_semaphore()
    pl.semaphore_signal(bar, inc=1, device_id=device(z, y, 1 - x, c), device_id_type=DT)
    pl.semaphore_signal(bar, inc=1, device_id=device(z, 1 - y, x, c), device_id_type=DT)

    @pl.when(z > 0)
    def _():
        pl.semaphore_signal(bar, inc=1, device_id=device(z - 1, y, x, c), device_id_type=DT)

    @pl.when(z < levels - 1)
    def _():
        pl.semaphore_signal(bar, inc=1, device_id=device(z + 1, y, x, c), device_id_type=DT)

    pl.semaphore_wait(
        bar, 2 + jnp.where(z > 0, 1, 0) + jnp.where(z < levels - 1, 1, 0)
    )


def gather_kernel(levels, groups, shard, wide, own_sem, z_send, z_recv, x_send, x_recv, y_send, y_recv):
    z, y, x, c = place()
    size = MATS // groups
    greet_neighbours(levels)
    local = pltpu.make_async_copy(shard, wide.at[:, x, z, y], own_sem)
    local.start()

    def block(g, xx, zz, yy):
        return wide.at[pl.ds(g * size, size), xx, zz, yy]

    def source(g, zz, own):
        return shard.at[pl.ds(g * size, size)] if own else block(g, x, zz, y)

    def z_copy(g, zz, target, own):
        return pltpu.make_async_remote_copy(
            source(g, zz, own), block(g, x, zz, y), z_send.at[g, zz, jnp.where(target > z, 1, 0)],
            z_recv.at[g, zz], device_id=device(target, y, x, c), device_id_type=DT,
        )

    def x_copy(g, zz, yy, own):
        src = source(g, zz, True) if own else block(g, x, zz, yy)
        return pltpu.make_async_remote_copy(
            src, block(g, x, zz, yy), x_send.at[g, zz, yy], x_recv.at[g, zz, yy],
            device_id=device(z, y, 1 - x, c), device_id_type=DT,
        )

    def y_copy(g, zz, xx, own):
        src = source(g, zz, True) if own else block(g, xx, zz, y)
        return pltpu.make_async_remote_copy(
            src, block(g, xx, zz, y), y_send.at[g, zz, xx], y_recv.at[g, zz, xx],
            device_id=device(z, 1 - y, x, c), device_id_type=DT,
        )

    def spread(g, zz, own):
        if g % 2 == 0:
            x_copy(g, zz, y, own).start()
            y_copy(g, zz, x, own).start()
        else:
            y_copy(g, zz, x, own).start()
            x_copy(g, zz, y, own).start()

    def first(g):
        @pl.when(z < levels - 1)
        def _():
            z_copy(g, z, z + 1, True).start()

        @pl.when(z > 0)
        def _():
            z_copy(g, z, z - 1, True).start()

        spread(g, z, True)
        for d in range(1, levels):
            @pl.when(z - d >= 0)
            def _():
                z_copy(g, z - d, z - 1, False).wait_recv()

                @pl.when(z < levels - 1)
                def _():
                    z_copy(g, z - d, z + 1, False).start()

                spread(g, z - d, False)

            @pl.when(z + d < levels)
            def _():
                z_copy(g, z + d, z + 1, False).wait_recv()

                @pl.when(z > 0)
                def _():
                    z_copy(g, z + d, z - 1, False).start()

                spread(g, z + d, False)

    def order(body):
        def run(d, carry):
            @pl.when(z - d >= 0)
            def _():
                body(z - d)

            if True:
                @pl.when((z + d < levels) & (d > 0))
                def _():
                    body(z + d)

            return carry

        lax.fori_loop(0, levels, run, 0)

    def second(g):
        def relay(zz):
            if g % 2 == 0:
                x_copy(g, zz, y, False).wait_recv()
                y_copy(g, zz, 1 - x, False).start()
            else:
                y_copy(g, zz, x, False).wait_recv()
                x_copy(g, zz, 1 - y, False).start()

        order(relay)

    def third(g):
        def finish(zz):
            if g % 2 == 0:
                y_copy(g, zz, x, False).wait_recv()
                y_copy(g, zz, 1 - x, False).wait_recv()
            else:
                x_copy(g, zz, y, False).wait_recv()
                x_copy(g, zz, 1 - y, False).wait_recv()

        order(finish)

    def drain(g):
        def sent(zz):
            if g % 2 == 0:
                x_copy(g, zz, y, False).wait_send()
                y_copy(g, zz, x, False).wait_send()
                y_copy(g, zz, 1 - x, False).wait_send()
            else:
                y_copy(g, zz, x, False).wait_send()
                x_copy(g, zz, y, False).wait_send()
                x_copy(g, zz, 1 - y, False).wait_send()

            @pl.when((z < levels - 1) & (zz <= z))
            def _():
                z_copy(g, zz, z + 1, False).wait_send()

            @pl.when((z > 0) & (zz >= z))
            def _():
                z_copy(g, zz, z - 1, False).wait_send()

        order(sent)

    for step in range(groups + 1):
        if step < groups:
            first(step)
        if step >= 1:
            second(step - 1)
    for g in range(groups):
        third(g)
        drain(g)
    local.wait()


def gather_weights(shard, shards):
    rows = shard.shape[1]
    levels = shards // 2
    groups = 8 if levels <= 4 else 2
    sem = pltpu.SemaphoreType.DMA
    wide = pl.pallas_call(
        partial(gather_kernel, levels, groups),
        out_shape=jax.ShapeDtypeStruct((MATS, 2, levels, 2, rows, COLS), jnp.bfloat16),
        in_specs=[pl.BlockSpec(memory_space=pltpu.VMEM)],
        out_specs=pl.BlockSpec(memory_space=pl.ANY),
        scratch_shapes=[
            sem, sem((groups, levels, 2)), sem((groups, levels)), sem((groups, levels, 2)),
            sem((groups, levels, 2)), sem((groups, levels, 2)), sem((groups, levels, 2)),
        ],
        compiler_params=pltpu.CompilerParams(collective_id=0, has_side_effects=True),
        name="gather_weights",
    )(shard)
    return wide.reshape(MATS, 2, D, COLS)


def scatter_kernel(levels, groups, part, out, even, odd, two, line, s1, r1, s2, r2, s3, r3):
    z, y, x, c = place()
    size = MATS // groups
    greet_neighbours(levels)

    def span(g):
        return pl.ds(g * size, size)

    def first(g):
        if g % 2 == 0:
            src, dev = part.at[span(g), :, :, 1 - y], device(z, 1 - y, x, c)
        else:
            src, dev = part.at[span(g), 1 - x, :, :], device(z, y, 1 - x, c)
        return pltpu.make_async_remote_copy(
            src, (odd if g % 2 else even).at[g // 2], s1.at[g], r1.at[g], device_id=dev, device_id_type=DT
        )

    def second(g):
        if g % 2 == 0:
            dev = device(z, y, 1 - x, c)
            src = part.at[span(g), 1 - x, :, y]
        else:
            dev = device(z, 1 - y, x, c)
            src = part.at[span(g), x, :, 1 - y]
        return pltpu.make_async_remote_copy(
            src, two.at[g], s2.at[g], r2.at[g], device_id=dev, device_id_type=DT
        )

    def add_first(g):
        for m in range(size):
            for k in range(2):
                def body(zz, carry):
                    if g % 2 == 0:
                        at = (g * size + m, k, zz, y)
                    else:
                        at = (g * size + m, x, zz, k)
                    got = even[g // 2, m, k, zz] if g % 2 == 0 else odd[g // 2, m, zz, k]
                    part[at] = (part[at].astype(jnp.float32) + got.astype(jnp.float32)).astype(jnp.bfloat16)
                    return carry

                lax.fori_loop(0, levels, body, 0)

    def add_second(g):
        for m in range(size):
            def body(zz, carry):
                at = (g * size + m, x, zz, y)
                part[at] = (part[at].astype(jnp.float32) + two[g, m, zz].astype(jnp.float32)).astype(jnp.bfloat16)
                return carry

            lax.fori_loop(0, levels, body, 0)

    def z_copy(g, zz, up):
        return pltpu.make_async_remote_copy(
            part.at[span(g), x, zz, y], line.at[g, up, zz], s3.at[g, zz], r3.at[g, up, zz],
            device_id=device(z + 1 if up else z - 1, y, x, c), device_id_type=DT,
        )

    def add_line(g, zz, up):
        for m in range(size):
            at = (g * size + m, x, zz, y)
            part[at] = (part[at].astype(jnp.float32) + line[g, up, zz, m].astype(jnp.float32)).astype(jnp.bfloat16)

    def third(g):
        def run(k, carry):
            top = levels - 1 - k

            @pl.when(top > z)
            def _():
                @pl.when(z > 0)
                def _():
                    z_copy(g, top, 1).wait_recv()
                    add_line(g, top, 1)

                z_copy(g, top, 1).start()

            @pl.when(k < z)
            def _():
                @pl.when(z < levels - 1)
                def _():
                    z_copy(g, k, 0).wait_recv()
                    add_line(g, k, 0)

                z_copy(g, k, 0).start()

            return carry

        lax.fori_loop(0, levels, run, 0)

    def last(g):
        @pl.when(z > 0)
        def _():
            z_copy(g, z, 1).wait_recv()

        @pl.when(z < levels - 1)
        def _():
            z_copy(g, z, 0).wait_recv()

        for m in range(size):
            i = g * size + m
            own = part[i, x, z, y].astype(jnp.float32)
            below = jnp.where(z > 0, line[g, 1, z, m].astype(jnp.float32), 0.0)
            above = jnp.where(z < levels - 1, line[g, 0, z, m].astype(jnp.float32), 0.0)
            out[i] = own + below + above

    def drain(g):
        first(g).wait_send()
        second(g).wait_send()

        def run(zz, carry):
            @pl.when(zz > z)
            def _():
                z_copy(g, zz, 1).wait_send()

            @pl.when(zz < z)
            def _():
                z_copy(g, zz, 0).wait_send()

            return carry

        lax.fori_loop(0, levels, run, 0)

    for g in range(groups):
        first(g).start()
    for step in range(groups + 2):
        if step < groups:
            first(step).wait_recv()
            add_first(step)
            second(step).start()
        if 1 <= step <= groups:
            second(step - 1).wait_recv()
            add_second(step - 1)
            third(step - 1)
        if step >= 2:
            last(step - 2)
    for g in range(groups):
        drain(g)


def scatter_grads(part, shards):
    levels = shards // 2
    rows = D // shards
    groups = 8
    size = MATS // groups
    sem = pltpu.SemaphoreType.DMA
    bf = jnp.bfloat16
    vm = pl.BlockSpec(memory_space=pltpu.VMEM)

    def kernel(levels, groups, given, out, part, *rest):
        load = pltpu.make_async_copy(given, part, rest[-1])
        load.start()
        load.wait()
        scatter_kernel(levels, groups, part, out, *rest[:-1])

    return pl.pallas_call(
        partial(kernel, levels, groups),
        out_shape=jax.ShapeDtypeStruct((MATS, rows, COLS), jnp.float32),
        in_specs=[pl.BlockSpec(memory_space=pl.ANY)],
        out_specs=vm,
        scratch_shapes=[
            pltpu.VMEM((MATS, 2, levels, 2, rows, COLS), bf),
            pltpu.VMEM((groups // 2, size, 2, levels, rows, COLS), bf),
            pltpu.VMEM((groups // 2, size, levels, 2, rows, COLS), bf),
            pltpu.VMEM((groups, size, levels, rows, COLS), bf),
            pltpu.VMEM((groups, 2, levels, size, rows, COLS), bf),
            sem((groups,)), sem((groups,)), sem((groups,)), sem((groups,)),
            sem((groups, levels)), sem((groups, 2, levels)), sem,
        ],
        compiler_params=pltpu.CompilerParams(
            collective_id=1, has_side_effects=True, vmem_limit_bytes=62 * 2**20
        ),
        name="scatter_grads",
    )(part.reshape(MATS, 2, levels, 2, rows, COLS))


def small_kernel(shards, every, scatter, src, out, own_sem, send_sem, recv_sem):
    dp, x, c = (lax.axis_index(a) for a in AXES)
    cores = 2 if every else 1
    count = shards * 2 * cores
    me = (dp * 2 + x) * cores + (c if every else 0)

    def peer(i):
        if every:
            return (i // 4, lax.rem(i // 2, 2), lax.rem(i, 2))
        return (i // 2, lax.rem(i, 2), c)

    bar = pltpu.get_barrier_semaphore()

    def greet(k, carry):
        pl.semaphore_signal(bar, inc=1, device_id=peer(lax.rem(me + k, count)), device_id_type=DT)
        return carry

    lax.fori_loop(1, count, greet, 0)
    pl.semaphore_wait(bar, count - 1)

    def copy(k):
        i = lax.rem(me + k, count)
        return pltpu.make_async_remote_copy(
            src.at[i] if scatter else src, out.at[me], send_sem.at[k], recv_sem.at[me],
            device_id=peer(i), device_id_type=DT,
        )

    def send(k, carry):
        copy(k).start()
        return carry

    own = pltpu.make_async_copy(src.at[me] if scatter else src, out.at[me], own_sem)
    own.start()
    lax.fori_loop(1, count, send, 0)
    own.wait()

    def finish(k, carry):
        i = lax.rem(me + k, count)
        pltpu.make_async_remote_copy(
            src.at[i] if scatter else src, out.at[i], send_sem.at[k], recv_sem.at[i],
            device_id=peer(i), device_id_type=DT,
        ).wait_recv()
        copy(k).wait_send()
        return carry

    lax.fori_loop(1, count, finish, 0)


def small_exchange(src, shards, every, scatter, call_id):
    count = shards * 2 * (2 if every else 1)
    shape = src.shape[1:] if scatter else src.shape
    sem = pltpu.SemaphoreType.DMA
    vm = pl.BlockSpec(memory_space=pltpu.VMEM)
    return pl.pallas_call(
        partial(small_kernel, shards, every, scatter),
        out_shape=jax.ShapeDtypeStruct((count, *shape), src.dtype),
        in_specs=[vm],
        out_specs=vm,
        scratch_shapes=[sem, sem((count,)), sem((count,))],
        compiler_params=pltpu.CompilerParams(collective_id=call_id, has_side_effects=True),
        name=f"small_exchange_{call_id}",
    )(src)


def pair_kernel(src, out, own_sem, send_sem, recv_sem):
    dp, x, c = (lax.axis_index(a) for a in AXES)
    bar = pltpu.get_barrier_semaphore()
    pl.semaphore_signal(bar, inc=1, device_id=(dp, x, 1 - c), device_id_type=DT)
    pl.semaphore_wait(bar, 1)
    copy = pltpu.make_async_remote_copy(
        src, out.at[c], send_sem, recv_sem, device_id=(dp, x, 1 - c), device_id_type=DT
    )
    copy.start()
    own = pltpu.make_async_copy(src, out.at[c], own_sem)
    own.start()
    own.wait()
    copy.wait_send()
    pltpu.make_async_remote_copy(
        src, out.at[1 - c], send_sem, recv_sem, device_id=(dp, x, 1 - c), device_id_type=DT
    ).wait_recv()


def pair_gather(src, call_id):
    sem = pltpu.SemaphoreType.DMA
    vm = pl.BlockSpec(memory_space=pltpu.VMEM)
    return pl.pallas_call(
        pair_kernel,
        out_shape=jax.ShapeDtypeStruct((2, *src.shape), src.dtype),
        in_specs=[vm],
        out_specs=vm,
        scratch_shapes=[sem, sem, sem],
        compiler_params=pltpu.CompilerParams(collective_id=call_id, has_side_effects=True),
        name=f"pair_gather_{call_id}",
    )(src)


def pair_sum(part, call_id):
    both = pair_gather(part.astype(jnp.bfloat16), call_id)
    return both[0].astype(jnp.float32) + both[1].astype(jnp.float32)


def norm_forward(values, gain_row, offset):
    centre = values - jnp.mean(values, axis=-1, keepdims=True)
    spread = jnp.mean(centre * centre, axis=-1, keepdims=True)
    scaled = lax.rsqrt(spread + 1e-05)
    normed = centre * scaled
    return (normed * gain_row + offset, normed, scaled)


def norm_backward(gradient, normed, scaled, gain_row):
    inner_grad = gradient * gain_row
    result = scaled * (
        inner_grad
        - jnp.mean(inner_grad, axis=-1, keepdims=True)
        - normed * jnp.mean(inner_grad * normed, axis=-1, keepdims=True)
    )
    return (result, jnp.sum(gradient * normed, axis=0), jnp.sum(gradient, axis=0))


def gelu_value(values):
    return 0.5 * values * (1.0 + jax.scipy.special.erf(values * 0.7071067811865476))


def gelu_slope(values):
    return (
        0.5 * (1.0 + jax.scipy.special.erf(values * 0.7071067811865476))
        + values * jnp.exp(-0.5 * values * values) * 0.3989422804014327
    )


def clip_scores(queries, key_rows, causal):
    scores = (
        jnp.einsum("qhd,khd->hqk", queries, key_rows, preferred_element_type=jnp.float32) * 0.125
    )
    if causal:
        allowed = lax.broadcasted_iota(jnp.int32, scores.shape, 1) >= lax.broadcasted_iota(
            jnp.int32, scores.shape, 2
        )
        scores = jnp.where(allowed, scores, -1e30)
    return scores


def clip_forward(causal, queries, key_rows, values):
    scores = clip_scores(queries, key_rows, causal)
    row_max = jnp.max(scores, axis=-1, keepdims=True)
    shifted = jnp.exp(scores - row_max)
    row_sum = jnp.sum(shifted, axis=-1, keepdims=True)
    weights = (shifted / row_sum).astype(jnp.bfloat16)
    context = jnp.einsum("hqk,khd->qhd", weights, values, preferred_element_type=jnp.float32)
    return (context.astype(jnp.bfloat16), (row_max + jnp.log(row_sum))[..., 0])


def clip_backward(causal, queries, key_rows, values, log_total, context_grad):
    scores = clip_scores(queries, key_rows, causal)
    probs = jnp.exp(scores - log_total[..., None])
    value_grad = jnp.einsum(
        "hqk,qhd->khd", probs.astype(jnp.bfloat16), context_grad, preferred_element_type=jnp.float32
    )
    prob_grad = jnp.einsum("qhd,khd->hqk", context_grad, values, preferred_element_type=jnp.float32)
    score_grad = (probs * (prob_grad - jnp.sum(probs * prob_grad, axis=-1, keepdims=True))).astype(
        jnp.bfloat16
    )
    query_grad = (
        jnp.einsum("hqk,khd->qhd", score_grad, key_rows, preferred_element_type=jnp.float32) * 0.125
    )
    key_grad = (
        jnp.einsum("hqk,qhd->khd", score_grad, queries, preferred_element_type=jnp.float32) * 0.125
    )
    return (
        query_grad.astype(jnp.bfloat16),
        key_grad.astype(jnp.bfloat16),
        value_grad.astype(jnp.bfloat16),
    )


def adapt(weight, gradient, moment, second, token_total):
    scaled_grad = gradient / token_total
    new_moment = 0.5 * moment + 0.5 * scaled_grad
    new_second = 0.5 * second + 0.5 * scaled_grad * scaled_grad
    direction = new_moment / (jnp.sqrt(new_second) + 1e-06) + 0.01 * weight
    return (new_moment, new_second, direction)


def shards_fn(
    tokens, frames, cotangent, attention_weights, dense_weights, unit_bias, norm_bias,
    attention_mean, dense_mean, unit_mean, norm_mean,
    attention_square, dense_square, unit_square, norm_square,
):
    f32, bf = jnp.float32, jnp.bfloat16
    shards = lax.axis_size("dp")
    rows = D // shards
    c = lax.axis_index("core")
    unit_cols = unit_bias.shape[1]
    column_rows = (lax.axis_index("dp") * unit_cols + jnp.arange(unit_cols, dtype=jnp.int32)) // HD
    row_pick = (column_rows[:, None] == jnp.arange(8, dtype=jnp.int32)[None, :]).astype(f32)
    leader = ((lax.axis_index("side") == 0) & (c == 0)).astype(f32)

    def square_rows(attn_part, dense_part, unit_part, norm_part):
        unit_sums = jnp.sum(jnp.sum(unit_part * unit_part, axis=0)[:, None] * row_pick, axis=0)
        return jnp.concatenate(
            [
                jnp.sum(attn_part * attn_part, axis=(2, 3)).reshape(8),
                jnp.sum(dense_part * dense_part, axis=(1, 2, 3)),
                unit_sums,
                jnp.sum(norm_part * norm_part, axis=1) * leader,
            ]
        )

    own_attn = attention_weights.astype(f32)
    own_dense = dense_weights.astype(f32)
    own_unit = unit_bias.astype(f32)
    own_norm = norm_bias.astype(f32)

    pack = jnp.concatenate([norm_bias.reshape(-1), unit_bias.reshape(-1)])
    pack = jnp.pad(pack, (0, 2048 - pack.shape[0])).reshape(16, 128)
    packs = small_exchange(pack, shards, False, False, 2).reshape(shards, 2, 2048)
    norm_rows = (
        packs[:, 0, : 9 * rows].reshape(shards, 9, rows).transpose(1, 0, 2).reshape(9, D).astype(f32)
    )
    unit_all = packs[:, :, 9 * rows : 9 * rows + 4 * unit_cols].reshape(shards, 2, 4, unit_cols)
    bias_rows = (
        unit_all.transpose(1, 2, 0, 3).reshape(8, 8, HD).transpose(1, 0, 2).reshape(8, 512).astype(f32)
    )

    shard = jnp.concatenate(
        [attention_weights.reshape(8, rows, COLS), dense_weights.transpose(0, 2, 1, 3).reshape(8, rows, COLS)]
    )
    wide = gather_weights(shard, shards)

    def project(left, mat):
        return jnp.einsum("rd,xde->rxe", left, wide[mat], preferred_element_type=f32).reshape(-1, 512)

    def project_hidden(left, base):
        return jnp.einsum("rd,mxde->rmxe", left, wide[base : base + 4], preferred_element_type=f32).reshape(-1, 2048)

    def collect(left, mat):
        return jnp.einsum("rxe,xde->rd", left.reshape(-1, 2, COLS), wide[mat], preferred_element_type=f32)

    def collect_hidden(left, base):
        return jnp.einsum("rmxe,mxde->rd", left.reshape(-1, 4, 2, COLS), wide[base : base + 4], preferred_element_type=f32)

    def weight_grad(left, right):
        return jnp.einsum("rd,rme->mde", left, right.reshape(right.shape[0], -1, COLS), preferred_element_type=f32).astype(bf)

    def by_head(flat):
        return flat.reshape(-1, 8, HD)

    row_data = pair_gather(tokens, 3).reshape(L, D).astype(f32)
    out_grad_low = pair_gather(cotangent, 4).reshape(L, D)
    frame_rows = pair_gather(frames, 5).reshape(FRAMES, D)

    first_in, first_normed, first_scale = norm_forward(row_data, norm_rows[0], norm_rows[1])
    first_in = first_in.astype(bf)
    self_query = (project(first_in, 0) + bias_rows[0]).astype(bf)
    self_keys = project(first_in, 1).astype(bf)
    self_values = (project(first_in, 2) + bias_rows[1]).astype(bf)
    self_context, self_total = clip_forward(
        True, by_head(self_query), by_head(self_keys), by_head(self_values)
    )
    self_flat = self_context.reshape(L, 512)
    hidden_one = row_data + norm_rows[6] + pair_sum(collect(self_flat, 3), 6)
    second_in, second_normed, second_scale = norm_forward(hidden_one, norm_rows[2], norm_rows[3])
    second_in = second_in.astype(bf)
    cross_query = (project(second_in, 4) + bias_rows[2]).astype(bf)
    cross_keys = project(frame_rows, 5).astype(bf)
    cross_values = (project(frame_rows, 6) + bias_rows[3]).astype(bf)
    cross_context, cross_total = clip_forward(
        False, by_head(cross_query), by_head(cross_keys), by_head(cross_values)
    )
    cross_flat = cross_context.reshape(L, 512)
    hidden_two = hidden_one + norm_rows[7] + pair_sum(collect(cross_flat, 7), 7)
    third_in, third_normed, third_scale = norm_forward(hidden_two, norm_rows[4], norm_rows[5])
    third_in = third_in.astype(bf)
    before = project_hidden(third_in, 8) + bias_rows[4:8].reshape(2048)
    activated = gelu_value(before).astype(bf)
    result_rows = hidden_two + norm_rows[8] + pair_sum(collect_hidden(activated, 12), 8)
    layer_out = lax.dynamic_slice_in_dim(result_rows, c * (L // 2), L // 2, 0).astype(bf)

    out_grad = out_grad_low.astype(f32)
    act_grad = project_hidden(out_grad_low, 12)
    down_grad = weight_grad(out_grad_low, activated)
    before_grad = (act_grad * gelu_slope(before)).astype(bf)
    hidden_bias_grad = jnp.sum(before_grad, axis=0, dtype=f32)
    up_grad = weight_grad(third_in, before_grad)
    third_back = pair_sum(collect_hidden(before_grad, 8), 9)
    third_input_grad, third_gain_grad, third_offset_grad = norm_backward(
        third_back, third_normed, third_scale, norm_rows[4]
    )
    two_grad = out_grad + third_input_grad
    two_low = two_grad.astype(bf)
    cross_ctx_grad = project(two_low, 7).astype(bf)
    cross_out_grad = weight_grad(two_low, cross_flat)
    cross_qgrad, cross_kgrad, cross_vgrad = clip_backward(
        False, by_head(cross_query), by_head(cross_keys), by_head(cross_values), cross_total,
        by_head(cross_ctx_grad),
    )
    cross_qflat = cross_qgrad.reshape(L, 512)
    cross_kflat = cross_kgrad.reshape(FRAMES, 512)
    cross_vflat = cross_vgrad.reshape(FRAMES, 512)
    frame_part = collect(cross_kflat, 5) + collect(cross_vflat, 6)
    frame_both = pair_gather(frame_part.astype(bf), 10)
    frame_gradient = jnp.sum(
        lax.dynamic_slice_in_dim(frame_both, c * (FRAMES // 2), FRAMES // 2, 1).astype(f32), axis=0
    )
    second_back = pair_sum(collect(cross_qflat, 4), 11)
    second_input_grad, second_gain_grad, second_offset_grad = norm_backward(
        second_back, second_normed, second_scale, norm_rows[2]
    )
    one_grad = two_grad + second_input_grad
    one_low = one_grad.astype(bf)
    self_ctx_grad = project(one_low, 3).astype(bf)
    self_out_grad = weight_grad(one_low, self_flat)
    self_qgrad, self_kgrad, self_vgrad = clip_backward(
        True, by_head(self_query), by_head(self_keys), by_head(self_values), self_total,
        by_head(self_ctx_grad),
    )
    self_qflat, self_kflat, self_vflat = (v.reshape(L, 512) for v in (self_qgrad, self_kgrad, self_vgrad))
    first_back = pair_sum(
        collect(self_qflat, 0) + collect(self_kflat, 1) + collect(self_vflat, 2), 12
    )
    first_input_grad, first_gain_grad, first_offset_grad = norm_backward(
        first_back, first_normed, first_scale, norm_rows[0]
    )
    input_gradient = lax.dynamic_slice_in_dim(one_grad + first_input_grad, c * (L // 2), L // 2, 0)

    parts = jnp.concatenate(
        [
            weight_grad(first_in, self_qflat), weight_grad(first_in, self_kflat),
            weight_grad(first_in, self_vflat), self_out_grad,
            weight_grad(second_in, cross_qflat), weight_grad(frame_rows, cross_kflat),
            weight_grad(frame_rows, cross_vflat), cross_out_grad, up_grad, down_grad,
        ]
    )
    owned = scatter_grads(parts, shards)
    attention_owned = owned[:8].reshape(2, 4, rows, COLS)
    dense_owned = owned[8:].reshape(2, 4, rows, COLS).transpose(0, 2, 1, 3)

    def column(v):
        return jnp.sum(v, axis=0, dtype=f32)

    unit_rows_grad = jnp.concatenate(
        [
            jnp.stack([column(self_qflat), column(self_vflat), column(cross_qflat), column(cross_vflat)]),
            hidden_bias_grad.reshape(4, 512),
        ]
    )
    unit_grads = (
        unit_rows_grad.reshape(8, 2, 4, HD).transpose(1, 2, 0, 3).reshape(2, 4, shards, unit_cols)
        .transpose(2, 0, 1, 3).reshape(shards, 2, 4 * unit_cols)
    )
    norm_grads = jnp.stack(
        [
            first_gain_grad, first_offset_grad, second_gain_grad, second_offset_grad,
            third_gain_grad, third_offset_grad, column(one_grad), column(two_grad), column(out_grad),
        ]
    )
    norm_parts = norm_grads.reshape(9, shards, rows).transpose(1, 0, 2).reshape(shards, 1, 9 * rows)
    small = jnp.concatenate([jnp.broadcast_to(norm_parts, (shards, 2, 9 * rows)), unit_grads], axis=2)
    small = jnp.pad(small, ((0, 0), (0, 0), (0, 2048 - small.shape[2]))).reshape(shards * 2, 16, 128)
    small = jnp.sum(small_exchange(small, shards, False, True, 13), axis=0).reshape(2048)
    norm_owned = small[: 9 * rows].reshape(9, rows)
    unit_owned = small[9 * rows : 9 * rows + 4 * unit_cols].reshape(4, unit_cols)

    token_total = float(tokens.shape[0] * shards * 4)
    attn_moment, attn_second, attn_dir = adapt(
        own_attn, attention_owned, attention_mean, attention_square, token_total
    )
    dense_moment, dense_second, dense_dir = adapt(
        own_dense, dense_owned, dense_mean, dense_square, token_total
    )
    unit_moment, unit_second, unit_dir = adapt(
        own_unit, unit_owned, unit_mean, unit_square, token_total
    )
    norm_moment, norm_second, norm_dir = adapt(
        own_norm, norm_owned, norm_mean, norm_square, token_total
    )
    sums = jnp.concatenate(
        [
            square_rows(own_attn, own_dense, own_unit, own_norm),
            square_rows(attn_dir, dense_dir, unit_dir, norm_dir),
        ]
    )
    sums = jnp.pad(sums, (0, 1024 - 54)).reshape(8, 128)
    sums = jnp.sum(small_exchange(sums, shards, True, False, 14), axis=0).reshape(1024)
    weight_norms = jnp.sqrt(sums[:27])
    step_norms = jnp.sqrt(sums[27:54])
    trust = weight_norms / step_norms
    attention_step = -learning_rate * trust[0:8].reshape(2, 4, 1, 1) * attn_dir
    dense_step = -learning_rate * trust[8:10].reshape(2, 1, 1, 1) * dense_dir
    unit_factor = jnp.sum(row_pick * trust[10:18][None, :], axis=1)
    unit_step = -learning_rate * unit_factor[None, :] * unit_dir
    norm_step = -learning_rate * trust[18:27][:, None] * norm_dir
    return (
        layer_out, input_gradient, frame_gradient,
        attention_owned, dense_owned, unit_owned, norm_owned,
        attn_moment, dense_moment, unit_moment, norm_moment,
        attn_second, dense_second, unit_second, norm_second,
        attention_step, dense_step, unit_step, norm_step,
        weight_norms, step_norms,
    )


def solution(mesh):
    shards = mesh.shape["dp"]
    inner = Mesh(mesh.devices.reshape(shards, 2, 2), AXES)
    tensor = ("side", "core")
    rows = P(("dp", *tensor), None)
    state = (P(None, None, "dp", tensor), P(None, "dp", None, tensor), P(tensor, "dp"), P(None, "dp"))
    return jax.shard_map(
        shards_fn,
        mesh=inner,
        in_specs=(rows, rows, rows) + state * 3,
        out_specs=(rows, rows, rows) + state * 4 + (P(), P()),
        check_vma=False,
    )
```

```python
from functools import partial

import jax
import jax.numpy as jnp
from jax import lax
from jax.experimental import pallas as pl
from jax.experimental.pallas import tpu as pltpu
from jax.sharding import Mesh, PartitionSpec as P

D = 1024
HEADS = 16
HD = 64
L = 448
FRAMES = 1500
MATS = 16
COLS = 256

learning_rate = 0.3
DT = pl.DeviceIdType.MESH
AXES = ("dp", "side", "core")


def place():
    dp = lax.axis_index("dp")
    return dp // 2, lax.rem(dp, 2), lax.axis_index("side"), lax.axis_index("core")


def device(z, y, x, c):
    return (z * 2 + y, x, c)


def greet_neighbours(levels):
    z, y, x, c = place()
    bar = pltpu.get_barrier_semaphore()
    pl.semaphore_signal(bar, inc=1, device_id=device(z, y, 1 - x, c), device_id_type=DT)
    pl.semaphore_signal(bar, inc=1, device_id=device(z, 1 - y, x, c), device_id_type=DT)

    @pl.when(z > 0)
    def _():
        pl.semaphore_signal(bar, inc=1, device_id=device(z - 1, y, x, c), device_id_type=DT)

    @pl.when(z < levels - 1)
    def _():
        pl.semaphore_signal(bar, inc=1, device_id=device(z + 1, y, x, c), device_id_type=DT)

    pl.semaphore_wait(
        bar, 2 + jnp.where(z > 0, 1, 0) + jnp.where(z < levels - 1, 1, 0)
    )


def start_when(cond, copy):
    @pl.when(cond)
    def _():
        copy.start()


class Gather:
    def __init__(self, levels, groups, shard, wide, sems):
        self.levels, self.groups, self.size = levels, groups, MATS // groups
        self.shard, self.wide = shard, wide
        self.own, self.zs, self.zr, self.xs, self.xr, self.ys, self.yr = sems
        self.at = place()
        self.done = 0
        self.total = (groups + 1) * levels

    @staticmethod
    def semaphores(levels, groups):
        sem = pltpu.SemaphoreType.DMA
        pair = sem((groups, levels, 2))
        return [sem, pair, sem((groups, levels)), pair, pair, pair, pair]

    def block(self, g, xx, zz, yy):
        return self.wide.at[pl.ds(g * self.size, self.size), xx, zz, yy]

    def source(self, g, xx, zz, yy, own):
        return self.shard.at[pl.ds(g * self.size, self.size)] if own else self.block(g, xx, zz, yy)

    def z_copy(self, g, zz, up, own):
        z, y, x, c = self.at
        return pltpu.make_async_remote_copy(
            self.source(g, x, zz, y, own), self.block(g, x, zz, y), self.zs.at[g, zz, up], self.zr.at[g, zz],
            device_id=device(z + 1 if up else z - 1, y, x, c), device_id_type=DT,
        )

    def x_copy(self, g, zz, yy, own):
        z, y, x, c = self.at
        return pltpu.make_async_remote_copy(
            self.source(g, x, zz, yy, own), self.block(g, x, zz, yy), self.xs.at[g, zz, yy],
            self.xr.at[g, zz, yy], device_id=device(z, y, 1 - x, c), device_id_type=DT,
        )

    def y_copy(self, g, zz, xx, own):
        z, y, x, c = self.at
        return pltpu.make_async_remote_copy(
            self.source(g, xx, zz, y, own), self.block(g, xx, zz, y), self.ys.at[g, zz, xx],
            self.yr.at[g, zz, xx], device_id=device(z, 1 - y, x, c), device_id_type=DT,
        )

    def begin(self):
        z, y, x, c = self.at
        self.local = pltpu.make_async_copy(self.shard, self.wide.at[:, x, z, y], self.own)
        self.local.start()

    def first(self, g, d):
        z, y, x, c = self.at
        top = self.levels - 1

        @pl.when(d == 0)
        def _():
            start_when(z < top, self.z_copy(g, z, 1, True))
            start_when(z > 0, self.z_copy(g, z, 0, True))
            self.x_copy(g, z, y, True).start()
            self.y_copy(g, z, x, True).start()

        for up in (1, 0):
            zz = z - d if up else z + d
            here = (zz >= 0) if up else (zz <= top)

            @pl.when((d > 0) & here)
            def _():
                self.z_copy(g, zz, up, False).wait_recv()
                start_when((z < top) if up else (z > 0), self.z_copy(g, zz, up, False))
                self.x_copy(g, zz, y, False).start()
                self.y_copy(g, zz, x, False).start()

    def second(self, g, d):
        z, y, x, c = self.at
        even = lax.rem(g, 2) == 0
        for up in (1, 0):
            zz = z - d if up else z + d
            here = (zz >= 0) if up else ((zz < self.levels) & (d > 0))

            @pl.when(here & even)
            def _():
                self.x_copy(g, zz, y, False).wait_recv()
                self.y_copy(g, zz, 1 - x, False).start()

            @pl.when(here & jnp.logical_not(even))
            def _():
                self.y_copy(g, zz, x, False).wait_recv()
                self.x_copy(g, zz, 1 - y, False).start()

    def tick(self, t):
        g, d = t // self.levels, lax.rem(t, self.levels)

        @pl.when(g < self.groups)
        def _():
            self.first(g, d)

        @pl.when(g >= 1)
        def _():
            self.second(g - 1, d)

    def run(self, count):
        count = max(0, min(count, self.total - self.done))
        start = self.done
        self.done += count
        if count:
            def body(i, carry):
                self.tick(start + i)
                return carry

            lax.fori_loop(0, count, body, 0)

    def reserve(self, count):
        if self.total - self.done < count:
            return lambda i: None
        start = self.done
        self.done += count
        return lambda i: self.tick(start + i)

    def need(self, g):
        self.run((g + 2) * self.levels - self.done)
        z, y, x, c = self.at

        def body(zz, carry):
            if g % 2 == 0:
                self.y_copy(g, zz, x, False).wait_recv()
                self.y_copy(g, zz, 1 - x, False).wait_recv()
            else:
                self.x_copy(g, zz, y, False).wait_recv()
                self.x_copy(g, zz, 1 - y, False).wait_recv()
            return carry

        lax.fori_loop(0, self.levels, body, 0)
        if g == 0:
            self.local.wait()

    def drain(self):
        z, y, x, c = self.at

        def group(g, carry):
            def sent(zz, inner):
                self.x_copy(g, zz, y, False).wait_send()
                self.y_copy(g, zz, x, False).wait_send()

                @pl.when(lax.rem(g, 2) == 0)
                def _():
                    self.y_copy(g, zz, 1 - x, False).wait_send()

                @pl.when(lax.rem(g, 2) == 1)
                def _():
                    self.x_copy(g, zz, 1 - y, False).wait_send()

                @pl.when((z < self.levels - 1) & (zz <= z))
                def _():
                    self.z_copy(g, zz, 1, False).wait_send()

                @pl.when((z > 0) & (zz >= z))
                def _():
                    self.z_copy(g, zz, 0, False).wait_send()

                return inner

            return lax.fori_loop(0, self.levels, sent, carry)

        lax.fori_loop(0, self.groups, group, 0)


HALF = L // 2
KEYS = 768
HALF_FRAMES = FRAMES // 2
BLOCK = 32


def dot(a, b, dims):
    return lax.dot_general(a, b, (dims, ((), ())), preferred_element_type=jnp.float32)


NN, NT, TN = ((1,), (0,)), ((1,), (1,)), ((0,), (0,))


def flat_panel(ref, mat, side):
    return ref[mat, side].reshape(D, COLS)


def rows_loop(count, body):
    def run(i, carry):
        body(pl.ds(pl.multiple_of(i * BLOCK, BLOCK), BLOCK), i)
        return carry

    lax.fori_loop(0, count // BLOCK, run, 0)


def loop(count, body):
    def run(i, carry):
        body(i)
        return carry

    lax.fori_loop(0, count, run, 0)


def normed_block(values):
    centre = values - jnp.mean(values, axis=-1, keepdims=True)
    spread = jnp.mean(centre * centre, axis=-1, keepdims=True)
    scaled = lax.rsqrt(spread + 1e-05)
    return centre * scaled, scaled


def panels_row(ref, rows):
    return jnp.concatenate([ref[j, rows, :].astype(jnp.float32) for j in range(4)], axis=1)


def forward_kernel(levels, groups, fast, *refs):
    f32, bf = jnp.float32, jnp.bfloat16
    names = FORWARD_IN + (("pack",) if fast else ("norm_in", "bias_in")) + tuple(n for n, _, _ in FORWARD_OUT) + (
        "wide", "x", "dy", "e", "norm", "bias", "a1", "a2", "a3", "h1", "h2", "qkv", "c1", "q2", "c2", "ek", "ev",
        "lse1", "lse2", "z", "slope", "s", "p", "acc", "part", "got", "packs", "padrow", "outrows",
        "in_sem", "swap_send", "swap_recv", "part_send", "part_recv", "pack_send", "pack_recv", "out_sem",
    )
    r = dict(zip(names, refs))
    gather = Gather(levels, groups, r["shard"], r["wide"], refs[len(names):])
    z, y, x, c = place()
    dp = z * 2 + y
    mate = (dp, x, 1 - c)
    count = levels * 4
    me = dp * 2 + x

    def peer(i):
        return (i // 2, lax.rem(i, 2), c)

    bar = pltpu.get_barrier_semaphore()
    loop(count - 1, lambda k: pl.semaphore_signal(
        bar, inc=1, device_id=peer(lax.rem(me + k + 1, count)), device_id_type=DT))
    pl.semaphore_signal(bar, inc=1, device_id=mate, device_id_type=DT)
    pl.semaphore_wait(bar, count)

    def remote(src, dst, send, recv, dev):
        return pltpu.make_async_remote_copy(src, dst, send, recv, device_id=dev, device_id_type=DT)

    inputs = (("tokens", "x"), ("frames", "e"), ("cotangent", "dy"))

    def swap(k, slot):
        src, dst = inputs[k]
        return remote(r[src], r[dst].at[slot], r["swap_send"].at[k], r["swap_recv"].at[k], mate)

    def local(k):
        src, dst = inputs[k]
        return pltpu.make_async_copy(r[src], r[dst].at[c], r["in_sem"].at[k])

    if fast:
        def pack_copy(k, slot):
            return remote(r["pack"], r["packs"].at[slot], r["pack_send"].at[k], r["pack_recv"].at[slot],
                          peer(lax.rem(me + k + 1, count)))

        loop(count - 1, lambda k: pack_copy(k, me).start())
        own_pack = pltpu.make_async_copy(r["pack"], r["packs"].at[me], r["in_sem"].at[3])
        own_pack.start()
    swap(0, c).start()
    local(0).start()
    gather.begin()
    gather.run(1)
    for k in (1, 2):
        swap(k, c).start()
        local(k).start()

    def arrived(k):
        local(k).wait()
        swap(k, 1 - c).wait_recv()

    outs = {}

    def emit(out, scratch):
        k = len(outs)
        outs[out] = pltpu.make_async_copy(scratch, r[out], r["out_sem"].at[k])
        outs[out].start()

    if fast:
        own_pack.wait()
        loop(count - 1, lambda k: pack_copy(k, lax.rem(me + k + 1, count)).wait_recv())
        for i in range(2 * levels):
            for xx in range(2):
                block = r["packs"][i * 2 + xx]
                if xx == 0:
                    r["norm"][:, i * 128 : (i + 1) * 128] = block
                r["bias"][i * 2 + xx : i * 2 + xx + 1, 0:128] = block[9:10]
                r["bias"][i * 2 + xx : i * 2 + xx + 1, 128:256] = block[10:11]
    else:
        r["norm"][...] = r["norm_in"][...]
        r["bias"][...] = r["bias_in"][...]
    emit("norm_out", r["norm"])

    def norm_row(k):
        return r["norm"][k : k + 1, :]

    def bias_row(k, side):
        return r["bias"][pl.ds(k * 2 + side, 1), :]

    key = lax.broadcasted_iota(jnp.int32, (1, 2 * KEYS), 1)
    real = lax.rem(key, KEYS) < HALF_FRAMES
    r["padrow"][0:1, :] = jnp.where(real, 0.0, -1e30).astype(f32)
    for i in range(3):
        for side in range(2):
            r["qkv"][i, side, L:512, :] = jnp.zeros((512 - L, COLS), bf)

    arrived(0)

    def ln1(half):
        def body(rows, i):
            normed, _ = normed_block(r["x"][half, rows, :].astype(f32))
            out = (normed * norm_row(0) + norm_row(1)).astype(bf)
            r["a1"][pl.ds(pl.multiple_of(half * HALF + i * BLOCK, BLOCK), BLOCK), :] = out

        rows_loop(HALF, body)

    ln1(0)
    ln1(1)
    emit("a1_out", r["a1"])
    emit("x_out", r["x"])

    def project_one(i, side):
        bias = bias_row(0, side) if i == 0 else bias_row(1, side)
        acc = dot(r["a1"][...], flat_panel(r["wide"], i, side), NN)
        if i != 1:
            acc = acc + bias
        r["qkv"][i, side, 0:L, :] = acc.astype(bf)

    gather.need(0)
    for i in range(2):
        loop(2, lambda side: project_one(i, side))
    gather.need(1)
    loop(2, lambda side: project_one(2, side))
    emit("qkv_out", r["qkv"])

    lane = lax.broadcasted_iota(jnp.int32, (1, 128), 1)
    low = lane < HD

    def attend(query, key_parts, values, width, causal, lse, ctx, tick):
        def body(t):
            side, half = t // 2, lax.rem(t, 2)
            lanes = pl.ds(pl.multiple_of(half * 128, 128), 128)
            q = query(side, lanes)
            found = []
            for sub in range(2):
                mine = low if sub == 0 else jnp.logical_not(low)
                qh = jnp.where(mine, q.astype(f32) * 0.125, 0.0).astype(bf)
                for n, part in enumerate(key_parts(side, lanes)):
                    r["s"][:, n * width : (n + 1) * width] = dot(qh, part, NT)
                total = width * len(key_parts(side, lanes))

                def rows_body(rows, i):
                    s = r["s"][rows, 0:total]
                    if causal:
                        row = i * BLOCK + lax.broadcasted_iota(jnp.int32, (BLOCK, total), 0)
                        col = lax.broadcasted_iota(jnp.int32, (BLOCK, total), 1)
                        s = jnp.where(col <= row, s, -1e30)
                    else:
                        s = s + r["padrow"][0:1, 0:total]
                    top = jnp.max(s, axis=-1, keepdims=True)
                    e = jnp.exp(s - top)
                    weight = jnp.sum(e, axis=-1, keepdims=True)
                    r["p"][rows, 0:total] = (e * (1.0 / weight)).astype(bf)
                    lse[t * 2 + sub, rows, :] = top + jnp.log(weight)

                rows_loop(L, rows_body)
                acc = None
                for n, part in enumerate(values(side, lanes)):
                    more = dot(r["p"][:, n * width : (n + 1) * width], part, NN)
                    acc = more if acc is None else acc + more
                found.append(acc)
                tick(t * 2 + sub)
            ctx[side, :, lanes] = jnp.where(low, found[0], found[1]).astype(bf)

        loop(4, body)

    attend(
        lambda side, lanes: r["qkv"][0, side, 0:L, lanes],
        lambda side, lanes: [r["qkv"][1, side, :, lanes]],
        lambda side, lanes: [r["qkv"][2, side, :, lanes]],
        512, True, r["lse1"], r["c1"], gather.reserve(8) if levels == 4 else (lambda i: None),
    )
    emit("lse1_out", r["lse1"])
    emit("c1_out", r["c1"])

    def collect(n, ctx, mat):
        def body(j):
            rows = pl.ds(pl.multiple_of(j * COLS, COLS), COLS)
            acc = None
            for side in range(2):
                w = r["wide"].at[mat, side]
                per = COLS // w.shape[2] if w.shape[2] < COLS else 1
                tile = flat_rows(w, j)
                more = dot(ctx[side], tile, NT)
                acc = more if acc is None else acc + more
            r["part"][n, j] = acc.astype(bf)
            trade(n, j).start()

        loop(4, body)

    def flat_rows(w, j):
        depth = w.shape[2]
        if 2 * depth >= COLS:
            per = COLS // (2 * depth)
            return w[pl.ds(j * per, per)].reshape(COLS, COLS)
        per = COLS // (2 * depth)
        return w[pl.ds(j * per, per)].reshape(COLS, COLS)

    def trade(n, j):
        return remote(r["part"].at[n, j], r["got"].at[n, j], r["part_send"].at[n, j], r["part_recv"].at[n, j], mate)

    def traded(n):
        loop(4, lambda j: trade(n, j).wait_recv())

    def residual(n, base, bias_k, out, gain_k, normed_out):
        def body(rows, i):
            v = base(rows, i) + norm_row(bias_k) + (panels_row(r["part"].at[n], rows) + panels_row(r["got"].at[n], rows))
            out[rows, :] = v
            normed, _ = normed_block(v)
            normed_out[rows, :] = (normed * norm_row(gain_k) + norm_row(gain_k + 1)).astype(bf)

        rows_loop(L, body)

    def x_rows(rows, i):
        half = i // (HALF // BLOCK)
        inner = pl.ds(pl.multiple_of((i - half * (HALF // BLOCK)) * BLOCK, BLOCK), BLOCK)
        return r["x"][half, inner, :].astype(f32)

    collect(0, r["c1"], 3)
    traded(0)
    residual(0, x_rows, 6, r["h1"], 2, r["a2"])
    emit("h1_out", r["h1"])
    emit("a2_out", r["a2"])

    gather.need(2)

    def query_two(side):
        acc = dot(r["a2"][...], flat_panel(r["wide"], 4, side), NN) + bias_row(2, side)
        r["q2"][side] = acc.astype(bf)

    loop(2, query_two)
    emit("q2_out", r["q2"])
    arrived(1)
    emit("e_out", r["e"])

    def frame_keys(t):
        side, half = t // 2, lax.rem(t, 2)
        r["ek"][side, half] = dot(r["e"][half], flat_panel(r["wide"], 5, side), NN).astype(bf)

    loop(4, frame_keys)
    emit("ek_out", r["ek"])
    gather.need(3)

    def frame_values(t):
        side, half = t // 2, lax.rem(t, 2)
        acc = dot(r["e"][half], flat_panel(r["wide"], 6, side), NN) + bias_row(3, side)
        r["ev"][side, half] = acc.astype(bf)

    loop(4, frame_values)
    emit("ev_out", r["ev"])
    attend(
        lambda side, lanes: r["q2"][side, :, lanes],
        lambda side, lanes: [r["ek"][side, half, :, lanes] for half in range(2)],
        lambda side, lanes: [r["ev"][side, half, :, lanes] for half in range(2)],
        KEYS, False, r["lse2"], r["c2"], gather.reserve(8) if levels == 4 else (lambda i: None),
    )
    emit("lse2_out", r["lse2"])
    emit("c2_out", r["c2"])
    collect(1, r["c2"], 7)
    traded(1)
    residual(1, lambda rows, i: r["h1"][rows, :], 7, r["h2"], 4, r["a3"])
    emit("h2_out", r["h2"])
    emit("a3_out", r["a3"])
    arrived(2)
    emit("dy_out", r["dy"])

    def hidden(t):
        m, side = t // 2, lax.rem(t, 2)
        u = dot(r["a3"][...], flat_panel(r["wide"], 8 + m, side), NN) + bias_row(4 + m, side)
        half = 0.5 * (1.0 + lax.erf(u * 0.7071067811865476))
        r["z"][t] = (u * half).astype(bf)
        r["slope"][t] = (half + u * jnp.exp(-0.5 * u * u) * 0.3989422804014327).astype(bf)

    def result(t):
        m, side = t // 2, lax.rem(t, 2)

        def tile(j):
            cols = pl.ds(pl.multiple_of(j * COLS, COLS), COLS)
            more = dot(r["z"][t], flat_rows(r["wide"].at[12 + m, side], j), NT)

            @pl.when(t == 0)
            def _():
                r["acc"][:, cols] = more

            @pl.when(t > 0)
            def _():
                r["acc"][:, cols] += more

        loop(4, tile)

    per = groups // 4
    mats = MATS // groups
    for k in range(max(1, groups // 4)):
        gather.need(groups // 2 + k)
        span = 8 // max(1, groups // 4)
        loop(span, lambda t: hidden(k * span + t))
    emit("z_out", r["z"])
    emit("slope_out", r["slope"])
    for k in range(max(1, groups // 4)):
        gather.need(groups * 3 // 4 + k if groups >= 4 else groups - 1)
        span = 8 // max(1, groups // 4)
        loop(span, lambda t: result(k * span + t))

    emit("wide_out", r["wide"])

    for half in range(2):
        @pl.when(c == half)
        def _():
            far = (1 - half) * HALF

            def body(j):
                cols = pl.ds(pl.multiple_of(j * COLS, COLS), COLS)
                r["part"][2, j, 0:HALF, :] = r["acc"][far : far + HALF, cols].astype(bf)

            loop(4, body)

    last = remote(
        r["part"].at[2, :, 0:HALF], r["got"].at[2, :, 0:HALF], r["part_send"].at[2, 0], r["part_recv"].at[2, 0], mate
    )
    last.start()
    last.wait_recv()

    def finish(rows, i):
        here = pl.ds(pl.multiple_of(c * HALF + i * BLOCK, BLOCK), BLOCK)
        own = r["acc"][here, :].astype(bf).astype(f32)
        v = r["h2"][here, :] + norm_row(8) + (own + panels_row(r["got"].at[2], rows))
        r["outrows"][rows, :] = v.astype(bf)

    rows_loop(HALF, finish)
    emit("layer_out", r["outrows"])

    for k in range(3):
        swap(k, c).wait_send()
    if fast:
        loop(count - 1, lambda k: pack_copy(k, me).wait_send())
    for n in range(2):
        loop(4, lambda j: trade(n, j).wait_send())
    last.wait_send()
    gather.drain()
    for copy in outs.values():
        copy.wait()


FORWARD_IN = ("shard", "tokens", "frames", "cotangent")
FORWARD_OUT = (
    ("layer_out", (HALF, D), jnp.bfloat16), ("norm_out", (16, D), jnp.float32),
    ("a1_out", (L, D), jnp.bfloat16), ("x_out", (2, HALF, D), jnp.bfloat16),
    ("qkv_out", (3, 2, 512, COLS), jnp.bfloat16), ("lse1_out", (8, L, 1), jnp.float32),
    ("c1_out", (2, L, COLS), jnp.bfloat16), ("h1_out", (L, D), jnp.float32), ("a2_out", (L, D), jnp.bfloat16),
    ("q2_out", (2, L, COLS), jnp.bfloat16), ("e_out", (2, KEYS, D), jnp.bfloat16),
    ("ek_out", (2, 2, KEYS, COLS), jnp.bfloat16), ("ev_out", (2, 2, KEYS, COLS), jnp.bfloat16),
    ("lse2_out", (8, L, 1), jnp.float32), ("c2_out", (2, L, COLS), jnp.bfloat16),
    ("h2_out", (L, D), jnp.float32), ("a3_out", (L, D), jnp.bfloat16), ("dy_out", (2, HALF, D), jnp.bfloat16),
    ("z_out", (8, L, COLS), jnp.bfloat16), ("slope_out", (8, L, COLS), jnp.bfloat16), ("wide_out", None, jnp.bfloat16),
)


def forward(shard, tokens, frames, cotangent, small, shards):
    levels, rows = shards // 2, D // shards
    groups = 8 if levels <= 4 else 4
    fast = len(small) == 1
    f32, bf = jnp.float32, jnp.bfloat16
    sem = pltpu.SemaphoreType.DMA
    vm, hbm = pl.BlockSpec(memory_space=pltpu.VMEM), pl.BlockSpec(memory_space=pl.ANY)
    wide = (MATS, 2, levels, 2, rows, COLS)
    shapes = [(n, wide if s is None else s, t) for n, s, t in FORWARD_OUT]
    peers = shards * 2
    scratch = [
        pltpu.VMEM(wide, bf), pltpu.VMEM((2, HALF, D), bf), pltpu.VMEM((2, HALF, D), bf), pltpu.VMEM((2, KEYS, D), bf),
        pltpu.VMEM((16, D), f32), pltpu.VMEM((16, COLS), f32),
        pltpu.VMEM((L, D), bf), pltpu.VMEM((L, D), bf), pltpu.VMEM((L, D), bf),
        pltpu.VMEM((L, D), f32), pltpu.VMEM((L, D), f32),
        pltpu.VMEM((3, 2, 512, COLS), bf), pltpu.VMEM((2, L, COLS), bf), pltpu.VMEM((2, L, COLS), bf),
        pltpu.VMEM((2, L, COLS), bf), pltpu.VMEM((2, 2, KEYS, COLS), bf), pltpu.VMEM((2, 2, KEYS, COLS), bf),
        pltpu.VMEM((8, L, 1), f32), pltpu.VMEM((8, L, 1), f32),
        pltpu.VMEM((8, L, COLS), bf), pltpu.VMEM((8, L, COLS), bf),
        pltpu.VMEM((L, 2 * KEYS), f32), pltpu.VMEM((L, 2 * KEYS), bf), pltpu.VMEM((L, D), f32),
        pltpu.VMEM((3, 4, L, COLS), bf), pltpu.VMEM((3, 4, L, COLS), bf),
        pltpu.VMEM((peers, 16, 128) if fast else (1, 16, 128), f32), pltpu.VMEM((8, 2 * KEYS), f32),
        pltpu.VMEM((HALF, D), bf),
        sem((4,)), sem((3,)), sem((3,)), sem((3, 4)), sem((3, 4)), sem((peers,)), sem((peers,)),
        sem((len(FORWARD_OUT),)),
    ]
    outs = pl.pallas_call(
        partial(forward_kernel, levels, groups, fast),
        out_shape=[jax.ShapeDtypeStruct(s, t) for _, s, t in shapes],
        in_specs=[vm, hbm, hbm, hbm] + [vm] * len(small),
        out_specs=[hbm] * len(shapes),
        scratch_shapes=scratch + Gather.semaphores(levels, groups),
        compiler_params=pltpu.CompilerParams(
            collective_id=0, has_side_effects=True, vmem_limit_bytes=63 * 2**20
        ),
        name="forward",
    )(shard, tokens, frames, cotangent, *small)
    return {n.removesuffix("_out") if n != "layer_out" else n: v for (n, _, _), v in zip(shapes, outs)}


def scatter_kernel(levels, groups, part, out, even, odd, two, line, s1, r1, s2, r2, s3, r3):
    z, y, x, c = place()
    size = MATS // groups
    greet_neighbours(levels)

    def span(g):
        return pl.ds(g * size, size)

    def first(g):
        if g % 2 == 0:
            src, dev = part.at[span(g), :, :, 1 - y], device(z, 1 - y, x, c)
        else:
            src, dev = part.at[span(g), 1 - x, :, :], device(z, y, 1 - x, c)
        return pltpu.make_async_remote_copy(
            src, (odd if g % 2 else even).at[g // 2], s1.at[g], r1.at[g], device_id=dev, device_id_type=DT
        )

    def second(g):
        if g % 2 == 0:
            dev = device(z, y, 1 - x, c)
            src = part.at[span(g), 1 - x, :, y]
        else:
            dev = device(z, 1 - y, x, c)
            src = part.at[span(g), x, :, 1 - y]
        return pltpu.make_async_remote_copy(
            src, two.at[g], s2.at[g], r2.at[g], device_id=dev, device_id_type=DT
        )

    def add_first(g):
        for m in range(size):
            for k in range(2):
                def body(zz, carry):
                    if g % 2 == 0:
                        at = (g * size + m, k, zz, y)
                    else:
                        at = (g * size + m, x, zz, k)
                    got = even[g // 2, m, k, zz] if g % 2 == 0 else odd[g // 2, m, zz, k]
                    part[at] = (part[at].astype(jnp.float32) + got.astype(jnp.float32)).astype(jnp.bfloat16)
                    return carry

                lax.fori_loop(0, levels, body, 0)

    def add_second(g):
        for m in range(size):
            def body(zz, carry):
                at = (g * size + m, x, zz, y)
                part[at] = (part[at].astype(jnp.float32) + two[g, m, zz].astype(jnp.float32)).astype(jnp.bfloat16)
                return carry

            lax.fori_loop(0, levels, body, 0)

    def z_copy(g, zz, up):
        return pltpu.make_async_remote_copy(
            part.at[span(g), x, zz, y], line.at[g, up, zz], s3.at[g, zz], r3.at[g, up, zz],
            device_id=device(z + 1 if up else z - 1, y, x, c), device_id_type=DT,
        )

    def add_line(g, zz, up):
        for m in range(size):
            at = (g * size + m, x, zz, y)
            part[at] = (part[at].astype(jnp.float32) + line[g, up, zz, m].astype(jnp.float32)).astype(jnp.bfloat16)

    def third(g):
        def run(k, carry):
            top = levels - 1 - k

            @pl.when(top > z)
            def _():
                @pl.when(z > 0)
                def _():
                    z_copy(g, top, 1).wait_recv()
                    add_line(g, top, 1)

                z_copy(g, top, 1).start()

            @pl.when(k < z)
            def _():
                @pl.when(z < levels - 1)
                def _():
                    z_copy(g, k, 0).wait_recv()
                    add_line(g, k, 0)

                z_copy(g, k, 0).start()

            return carry

        lax.fori_loop(0, levels, run, 0)

    def last(g):
        @pl.when(z > 0)
        def _():
            z_copy(g, z, 1).wait_recv()

        @pl.when(z < levels - 1)
        def _():
            z_copy(g, z, 0).wait_recv()

        for m in range(size):
            i = g * size + m
            own = part[i, x, z, y].astype(jnp.float32)
            below = jnp.where(z > 0, line[g, 1, z, m].astype(jnp.float32), 0.0)
            above = jnp.where(z < levels - 1, line[g, 0, z, m].astype(jnp.float32), 0.0)
            out[i] = own + below + above

    def drain(g):
        first(g).wait_send()
        second(g).wait_send()

        def run(zz, carry):
            @pl.when(zz > z)
            def _():
                z_copy(g, zz, 1).wait_send()

            @pl.when(zz < z)
            def _():
                z_copy(g, zz, 0).wait_send()

            return carry

        lax.fori_loop(0, levels, run, 0)

    for g in range(groups):
        first(g).start()
    for step in range(groups + 2):
        if step < groups:
            first(step).wait_recv()
            add_first(step)
            second(step).start()
        if 1 <= step <= groups:
            second(step - 1).wait_recv()
            add_second(step - 1)
            third(step - 1)
        if step >= 2:
            last(step - 2)
    for g in range(groups):
        drain(g)


def scatter_grads(part, shards):
    levels = shards // 2
    rows = D // shards
    groups = 8
    size = MATS // groups
    sem = pltpu.SemaphoreType.DMA
    bf = jnp.bfloat16
    vm = pl.BlockSpec(memory_space=pltpu.VMEM)

    def kernel(levels, groups, given, out, part, *rest):
        load = pltpu.make_async_copy(given, part, rest[-1])
        load.start()
        load.wait()
        scatter_kernel(levels, groups, part, out, *rest[:-1])

    return pl.pallas_call(
        partial(kernel, levels, groups),
        out_shape=jax.ShapeDtypeStruct((MATS, rows, COLS), jnp.float32),
        in_specs=[pl.BlockSpec(memory_space=pl.ANY)],
        out_specs=vm,
        scratch_shapes=[
            pltpu.VMEM((MATS, 2, levels, 2, rows, COLS), bf),
            pltpu.VMEM((groups // 2, size, 2, levels, rows, COLS), bf),
            pltpu.VMEM((groups // 2, size, levels, 2, rows, COLS), bf),
            pltpu.VMEM((groups, size, levels, rows, COLS), bf),
            pltpu.VMEM((groups, 2, levels, size, rows, COLS), bf),
            sem((groups,)), sem((groups,)), sem((groups,)), sem((groups,)),
            sem((groups, levels)), sem((groups, 2, levels)), sem,
        ],
        compiler_params=pltpu.CompilerParams(
            collective_id=1, has_side_effects=True, vmem_limit_bytes=62 * 2**20
        ),
        name="scatter_grads",
    )(part.reshape(MATS, 2, levels, 2, rows, COLS))


def small_kernel(shards, every, scatter, src, out, own_sem, send_sem, recv_sem):
    dp, x, c = (lax.axis_index(a) for a in AXES)
    cores = 2 if every else 1
    count = shards * 2 * cores
    me = (dp * 2 + x) * cores + (c if every else 0)

    def peer(i):
        if every:
            return (i // 4, lax.rem(i // 2, 2), lax.rem(i, 2))
        return (i // 2, lax.rem(i, 2), c)

    bar = pltpu.get_barrier_semaphore()

    def greet(k, carry):
        pl.semaphore_signal(bar, inc=1, device_id=peer(lax.rem(me + k, count)), device_id_type=DT)
        return carry

    lax.fori_loop(1, count, greet, 0)
    pl.semaphore_wait(bar, count - 1)

    def copy(k):
        i = lax.rem(me + k, count)
        return pltpu.make_async_remote_copy(
            src.at[i] if scatter else src, out.at[me], send_sem.at[k], recv_sem.at[me],
            device_id=peer(i), device_id_type=DT,
        )

    def send(k, carry):
        copy(k).start()
        return carry

    own = pltpu.make_async_copy(src.at[me] if scatter else src, out.at[me], own_sem)
    own.start()
    lax.fori_loop(1, count, send, 0)
    own.wait()

    def finish(k, carry):
        i = lax.rem(me + k, count)
        pltpu.make_async_remote_copy(
            src.at[i] if scatter else src, out.at[i], send_sem.at[k], recv_sem.at[i],
            device_id=peer(i), device_id_type=DT,
        ).wait_recv()
        copy(k).wait_send()
        return carry

    lax.fori_loop(1, count, finish, 0)


def small_exchange(src, shards, every, scatter, call_id):
    count = shards * 2 * (2 if every else 1)
    shape = src.shape[1:] if scatter else src.shape
    sem = pltpu.SemaphoreType.DMA
    vm = pl.BlockSpec(memory_space=pltpu.VMEM)
    return pl.pallas_call(
        partial(small_kernel, shards, every, scatter),
        out_shape=jax.ShapeDtypeStruct((count, *shape), src.dtype),
        in_specs=[vm],
        out_specs=vm,
        scratch_shapes=[sem, sem((count,)), sem((count,))],
        compiler_params=pltpu.CompilerParams(collective_id=call_id, has_side_effects=True),
        name=f"small_exchange_{call_id}",
    )(src)


def pair_kernel(src, out, own_sem, send_sem, recv_sem):
    dp, x, c = (lax.axis_index(a) for a in AXES)
    bar = pltpu.get_barrier_semaphore()
    pl.semaphore_signal(bar, inc=1, device_id=(dp, x, 1 - c), device_id_type=DT)
    pl.semaphore_wait(bar, 1)
    copy = pltpu.make_async_remote_copy(
        src, out.at[c], send_sem, recv_sem, device_id=(dp, x, 1 - c), device_id_type=DT
    )
    copy.start()
    own = pltpu.make_async_copy(src, out.at[c], own_sem)
    own.start()
    own.wait()
    copy.wait_send()
    pltpu.make_async_remote_copy(
        src, out.at[1 - c], send_sem, recv_sem, device_id=(dp, x, 1 - c), device_id_type=DT
    ).wait_recv()


def pair_gather(src, call_id):
    sem = pltpu.SemaphoreType.DMA
    vm = pl.BlockSpec(memory_space=pltpu.VMEM)
    return pl.pallas_call(
        pair_kernel,
        out_shape=jax.ShapeDtypeStruct((2, *src.shape), src.dtype),
        in_specs=[vm],
        out_specs=vm,
        scratch_shapes=[sem, sem, sem],
        compiler_params=pltpu.CompilerParams(collective_id=call_id, has_side_effects=True),
        name=f"pair_gather_{call_id}",
    )(src)


def pair_sum(part, call_id):
    both = pair_gather(part.astype(jnp.bfloat16), call_id)
    return both[0].astype(jnp.float32) + both[1].astype(jnp.float32)


def norm_forward(values, gain_row, offset):
    centre = values - jnp.mean(values, axis=-1, keepdims=True)
    spread = jnp.mean(centre * centre, axis=-1, keepdims=True)
    scaled = lax.rsqrt(spread + 1e-05)
    normed = centre * scaled
    return (normed * gain_row + offset, normed, scaled)


def norm_backward(gradient, normed, scaled, gain_row):
    inner_grad = gradient * gain_row
    result = scaled * (
        inner_grad
        - jnp.mean(inner_grad, axis=-1, keepdims=True)
        - normed * jnp.mean(inner_grad * normed, axis=-1, keepdims=True)
    )
    return (result, jnp.sum(gradient * normed, axis=0), jnp.sum(gradient, axis=0))


def gelu_value(values):
    return 0.5 * values * (1.0 + jax.scipy.special.erf(values * 0.7071067811865476))


def gelu_slope(values):
    return (
        0.5 * (1.0 + jax.scipy.special.erf(values * 0.7071067811865476))
        + values * jnp.exp(-0.5 * values * values) * 0.3989422804014327
    )


def clip_scores(queries, key_rows, causal):
    scores = (
        jnp.einsum("qhd,khd->hqk", queries, key_rows, preferred_element_type=jnp.float32) * 0.125
    )
    if causal:
        allowed = lax.broadcasted_iota(jnp.int32, scores.shape, 1) >= lax.broadcasted_iota(
            jnp.int32, scores.shape, 2
        )
        scores = jnp.where(allowed, scores, -1e30)
    return scores


def clip_forward(causal, queries, key_rows, values):
    scores = clip_scores(queries, key_rows, causal)
    row_max = jnp.max(scores, axis=-1, keepdims=True)
    shifted = jnp.exp(scores - row_max)
    row_sum = jnp.sum(shifted, axis=-1, keepdims=True)
    weights = (shifted / row_sum).astype(jnp.bfloat16)
    context = jnp.einsum("hqk,khd->qhd", weights, values, preferred_element_type=jnp.float32)
    return (context.astype(jnp.bfloat16), (row_max + jnp.log(row_sum))[..., 0])


def clip_backward(causal, queries, key_rows, values, log_total, context_grad):
    scores = clip_scores(queries, key_rows, causal)
    probs = jnp.exp(scores - log_total[..., None])
    value_grad = jnp.einsum(
        "hqk,qhd->khd", probs.astype(jnp.bfloat16), context_grad, preferred_element_type=jnp.float32
    )
    prob_grad = jnp.einsum("qhd,khd->hqk", context_grad, values, preferred_element_type=jnp.float32)
    score_grad = (probs * (prob_grad - jnp.sum(probs * prob_grad, axis=-1, keepdims=True))).astype(
        jnp.bfloat16
    )
    query_grad = (
        jnp.einsum("hqk,khd->qhd", score_grad, key_rows, preferred_element_type=jnp.float32) * 0.125
    )
    key_grad = (
        jnp.einsum("hqk,qhd->khd", score_grad, queries, preferred_element_type=jnp.float32) * 0.125
    )
    return (
        query_grad.astype(jnp.bfloat16),
        key_grad.astype(jnp.bfloat16),
        value_grad.astype(jnp.bfloat16),
    )


def adapt(weight, gradient, moment, second, token_total):
    scaled_grad = gradient / token_total
    new_moment = 0.5 * moment + 0.5 * scaled_grad
    new_second = 0.5 * second + 0.5 * scaled_grad * scaled_grad
    direction = new_moment / (jnp.sqrt(new_second) + 1e-06) + 0.01 * weight
    return (new_moment, new_second, direction)


def shards_fn(
    tokens, frames, cotangent, attention_weights, dense_weights, unit_bias, norm_bias,
    attention_mean, dense_mean, unit_mean, norm_mean,
    attention_square, dense_square, unit_square, norm_square,
):
    f32, bf = jnp.float32, jnp.bfloat16
    shards = lax.axis_size("dp")
    rows = D // shards
    c = lax.axis_index("core")
    unit_cols = unit_bias.shape[1]
    column_rows = (lax.axis_index("dp") * unit_cols + jnp.arange(unit_cols, dtype=jnp.int32)) // HD
    row_pick = (column_rows[:, None] == jnp.arange(8, dtype=jnp.int32)[None, :]).astype(f32)
    leader = ((lax.axis_index("side") == 0) & (c == 0)).astype(f32)

    def square_rows(attn_part, dense_part, unit_part, norm_part):
        unit_sums = jnp.sum(jnp.sum(unit_part * unit_part, axis=0)[:, None] * row_pick, axis=0)
        return jnp.concatenate(
            [
                jnp.sum(attn_part * attn_part, axis=(2, 3)).reshape(8),
                jnp.sum(dense_part * dense_part, axis=(1, 2, 3)),
                unit_sums,
                jnp.sum(norm_part * norm_part, axis=1) * leader,
            ]
        )

    own_attn = attention_weights.astype(f32)
    own_dense = dense_weights.astype(f32)
    own_unit = unit_bias.astype(f32)
    own_norm = norm_bias.astype(f32)

    if rows == 128:
        pack = jnp.concatenate([norm_bias.astype(f32), unit_bias.astype(f32).reshape(2, 128)])
        small = (jnp.pad(pack, ((0, 5), (0, 0))),)
    else:
        pack = jnp.concatenate([norm_bias.reshape(-1), unit_bias.reshape(-1)])
        pack = jnp.pad(pack, (0, 2048 - pack.shape[0])).reshape(16, 128)
        packs = small_exchange(pack, shards, False, False, 2).reshape(shards, 2, 2048)
        norm_rows = packs[:, 0, : 9 * rows].reshape(shards, 9, rows).transpose(1, 0, 2).reshape(9, D).astype(f32)
        unit_all = packs[:, :, 9 * rows : 9 * rows + 4 * unit_cols].reshape(shards, 2, 4, unit_cols)
        bias_rows = (
            unit_all.transpose(1, 2, 0, 3).reshape(2, 4, 8, HD).transpose(2, 0, 1, 3).reshape(16, COLS).astype(f32)
        )
        small = (jnp.pad(norm_rows, ((0, 7), (0, 0))), bias_rows)

    shard = jnp.concatenate(
        [attention_weights.reshape(8, rows, COLS), dense_weights.transpose(0, 2, 1, 3).reshape(8, rows, COLS)]
    )
    kept = forward(shard, tokens, jnp.pad(frames, ((0, KEYS - HALF_FRAMES), (0, 0))), cotangent, small, shards)
    wide = kept["wide"].reshape(MATS, 2, D, COLS)
    norm_rows = kept["norm"]

    def project(left, mat):
        return jnp.einsum("rd,xde->rxe", left, wide[mat], preferred_element_type=f32).reshape(-1, 512)

    def project_hidden(left, base):
        return jnp.einsum("rd,mxde->rmxe", left, wide[base : base + 4], preferred_element_type=f32).reshape(-1, 2048)

    def collect(left, mat):
        return jnp.einsum("rxe,xde->rd", left.reshape(-1, 2, COLS), wide[mat], preferred_element_type=f32)

    def collect_hidden(left, base):
        return jnp.einsum("rmxe,mxde->rd", left.reshape(-1, 4, 2, COLS), wide[base : base + 4], preferred_element_type=f32)

    def weight_grad(left, right):
        return jnp.einsum("rd,rme->mde", left, right.reshape(right.shape[0], -1, COLS), preferred_element_type=f32).astype(bf)

    def by_head(flat):
        return flat.reshape(-1, 8, HD)

    def joined(panels):
        return panels.transpose(1, 0, 2).reshape(panels.shape[1], -1)

    def unpadded(halves):
        return halves[:, :HALF_FRAMES].reshape(FRAMES, -1)

    row_data = kept["x"].reshape(L, D).astype(f32)
    out_grad_low = kept["dy"].reshape(L, D)
    frame_rows = unpadded(kept["e"])
    first_in, second_in, third_in = kept["a1"], kept["a2"], kept["a3"]
    _, first_normed, first_scale = norm_forward(row_data, norm_rows[0], norm_rows[1])
    _, second_normed, second_scale = norm_forward(kept["h1"], norm_rows[2], norm_rows[3])
    _, third_normed, third_scale = norm_forward(kept["h2"], norm_rows[4], norm_rows[5])
    self_query, self_keys, self_values = (joined(kept["qkv"][i, :, :L]) for i in range(3))
    self_total, cross_total = kept["lse1"][..., 0], kept["lse2"][..., 0]
    self_flat, cross_flat, cross_query = joined(kept["c1"]), joined(kept["c2"]), joined(kept["q2"])
    cross_keys, cross_values = (
        jnp.concatenate([unpadded(kept[n][side]) for side in range(2)], axis=1) for n in ("ek", "ev")
    )
    activated = joined(kept["z"])
    slope = joined(kept["slope"]).astype(f32)
    layer_out = kept["layer_out"]

    out_grad = out_grad_low.astype(f32)
    act_grad = project_hidden(out_grad_low, 12)
    down_grad = weight_grad(out_grad_low, activated)
    before_grad = (act_grad * slope).astype(bf)
    hidden_bias_grad = jnp.sum(before_grad, axis=0, dtype=f32)
    up_grad = weight_grad(third_in, before_grad)
    third_back = pair_sum(collect_hidden(before_grad, 8), 9)
    third_input_grad, third_gain_grad, third_offset_grad = norm_backward(
        third_back, third_normed, third_scale, norm_rows[4]
    )
    two_grad = out_grad + third_input_grad
    two_low = two_grad.astype(bf)
    cross_ctx_grad = project(two_low, 7).astype(bf)
    cross_out_grad = weight_grad(two_low, cross_flat)
    cross_qgrad, cross_kgrad, cross_vgrad = clip_backward(
        False, by_head(cross_query), by_head(cross_keys), by_head(cross_values), cross_total,
        by_head(cross_ctx_grad),
    )
    cross_qflat = cross_qgrad.reshape(L, 512)
    cross_kflat = cross_kgrad.reshape(FRAMES, 512)
    cross_vflat = cross_vgrad.reshape(FRAMES, 512)
    frame_part = collect(cross_kflat, 5) + collect(cross_vflat, 6)
    frame_both = pair_gather(frame_part.astype(bf), 10)
    frame_gradient = jnp.sum(
        lax.dynamic_slice_in_dim(frame_both, c * (FRAMES // 2), FRAMES // 2, 1).astype(f32), axis=0
    )
    second_back = pair_sum(collect(cross_qflat, 4), 11)
    second_input_grad, second_gain_grad, second_offset_grad = norm_backward(
        second_back, second_normed, second_scale, norm_rows[2]
    )
    one_grad = two_grad + second_input_grad
    one_low = one_grad.astype(bf)
    self_ctx_grad = project(one_low, 3).astype(bf)
    self_out_grad = weight_grad(one_low, self_flat)
    self_qgrad, self_kgrad, self_vgrad = clip_backward(
        True, by_head(self_query), by_head(self_keys), by_head(self_values), self_total,
        by_head(self_ctx_grad),
    )
    self_qflat, self_kflat, self_vflat = (v.reshape(L, 512) for v in (self_qgrad, self_kgrad, self_vgrad))
    first_back = pair_sum(
        collect(self_qflat, 0) + collect(self_kflat, 1) + collect(self_vflat, 2), 12
    )
    first_input_grad, first_gain_grad, first_offset_grad = norm_backward(
        first_back, first_normed, first_scale, norm_rows[0]
    )
    input_gradient = lax.dynamic_slice_in_dim(one_grad + first_input_grad, c * (L // 2), L // 2, 0)

    parts = jnp.concatenate(
        [
            weight_grad(first_in, self_qflat), weight_grad(first_in, self_kflat),
            weight_grad(first_in, self_vflat), self_out_grad,
            weight_grad(second_in, cross_qflat), weight_grad(frame_rows, cross_kflat),
            weight_grad(frame_rows, cross_vflat), cross_out_grad, up_grad, down_grad,
        ]
    )
    owned = scatter_grads(parts, shards)
    attention_owned = owned[:8].reshape(2, 4, rows, COLS)
    dense_owned = owned[8:].reshape(2, 4, rows, COLS).transpose(0, 2, 1, 3)

    def column(v):
        return jnp.sum(v, axis=0, dtype=f32)

    unit_rows_grad = jnp.concatenate(
        [
            jnp.stack([column(self_qflat), column(self_vflat), column(cross_qflat), column(cross_vflat)]),
            hidden_bias_grad.reshape(4, 512),
        ]
    )
    unit_grads = (
        unit_rows_grad.reshape(8, 2, 4, HD).transpose(1, 2, 0, 3).reshape(2, 4, shards, unit_cols)
        .transpose(2, 0, 1, 3).reshape(shards, 2, 4 * unit_cols)
    )
    norm_grads = jnp.stack(
        [
            first_gain_grad, first_offset_grad, second_gain_grad, second_offset_grad,
            third_gain_grad, third_offset_grad, column(one_grad), column(two_grad), column(out_grad),
        ]
    )
    norm_parts = norm_grads.reshape(9, shards, rows).transpose(1, 0, 2).reshape(shards, 1, 9 * rows)
    small = jnp.concatenate([jnp.broadcast_to(norm_parts, (shards, 2, 9 * rows)), unit_grads], axis=2)
    small = jnp.pad(small, ((0, 0), (0, 0), (0, 2048 - small.shape[2]))).reshape(shards * 2, 16, 128)
    small = jnp.sum(small_exchange(small, shards, False, True, 13), axis=0).reshape(2048)
    norm_owned = small[: 9 * rows].reshape(9, rows)
    unit_owned = small[9 * rows : 9 * rows + 4 * unit_cols].reshape(4, unit_cols)

    token_total = float(tokens.shape[0] * shards * 4)
    attn_moment, attn_second, attn_dir = adapt(
        own_attn, attention_owned, attention_mean, attention_square, token_total
    )
    dense_moment, dense_second, dense_dir = adapt(
        own_dense, dense_owned, dense_mean, dense_square, token_total
    )
    unit_moment, unit_second, unit_dir = adapt(
        own_unit, unit_owned, unit_mean, unit_square, token_total
    )
    norm_moment, norm_second, norm_dir = adapt(
        own_norm, norm_owned, norm_mean, norm_square, token_total
    )
    sums = jnp.concatenate(
        [
            square_rows(own_attn, own_dense, own_unit, own_norm),
            square_rows(attn_dir, dense_dir, unit_dir, norm_dir),
        ]
    )
    sums = jnp.pad(sums, (0, 1024 - 54)).reshape(8, 128)
    sums = jnp.sum(small_exchange(sums, shards, True, False, 14), axis=0).reshape(1024)
    weight_norms = jnp.sqrt(sums[:27])
    step_norms = jnp.sqrt(sums[27:54])
    trust = weight_norms / step_norms
    attention_step = -learning_rate * trust[0:8].reshape(2, 4, 1, 1) * attn_dir
    dense_step = -learning_rate * trust[8:10].reshape(2, 1, 1, 1) * dense_dir
    unit_factor = jnp.sum(row_pick * trust[10:18][None, :], axis=1)
    unit_step = -learning_rate * unit_factor[None, :] * unit_dir
    norm_step = -learning_rate * trust[18:27][:, None] * norm_dir
    return (
        layer_out, input_gradient, frame_gradient,
        attention_owned, dense_owned, unit_owned, norm_owned,
        attn_moment, dense_moment, unit_moment, norm_moment,
        attn_second, dense_second, unit_second, norm_second,
        attention_step, dense_step, unit_step, norm_step,
        weight_norms, step_norms,
    )


def solution(mesh):
    shards = mesh.shape["dp"]
    inner = Mesh(mesh.devices.reshape(shards, 2, 2), AXES)
    tensor = ("side", "core")
    rows = P(("dp", *tensor), None)
    state = (P(None, None, "dp", tensor), P(None, "dp", None, tensor), P(tensor, "dp"), P(None, "dp"))
    return jax.shard_map(
        shards_fn,
        mesh=inner,
        in_specs=(rows, rows, rows) + state * 3,
        out_specs=(rows, rows, rows) + state * 4 + (P(), P()),
        check_vma=False,
    )
```

```python
from functools import partial

import jax
import jax.numpy as jnp
from jax import lax
from jax.experimental import pallas as pl
from jax.experimental.pallas import tpu as pltpu
from jax.sharding import Mesh, PartitionSpec as P

D = 1024
HEADS = 16
HD = 64
L = 448
FRAMES = 1500
MATS = 16
COLS = 256

learning_rate = 0.3
DT = pl.DeviceIdType.MESH
AXES = ("dp", "side", "core")


def place():
    dp = lax.axis_index("dp")
    return dp // 2, lax.rem(dp, 2), lax.axis_index("side"), lax.axis_index("core")


def device(z, y, x, c):
    return (z * 2 + y, x, c)


def greet_neighbours(levels):
    z, y, x, c = place()
    bar = pltpu.get_barrier_semaphore()
    pl.semaphore_signal(bar, inc=1, device_id=device(z, y, 1 - x, c), device_id_type=DT)
    pl.semaphore_signal(bar, inc=1, device_id=device(z, 1 - y, x, c), device_id_type=DT)

    @pl.when(z > 0)
    def _():
        pl.semaphore_signal(bar, inc=1, device_id=device(z - 1, y, x, c), device_id_type=DT)

    @pl.when(z < levels - 1)
    def _():
        pl.semaphore_signal(bar, inc=1, device_id=device(z + 1, y, x, c), device_id_type=DT)

    pl.semaphore_wait(
        bar, 2 + jnp.where(z > 0, 1, 0) + jnp.where(z < levels - 1, 1, 0)
    )


def start_when(cond, copy):
    @pl.when(cond)
    def _():
        copy.start()


class Gather:
    def __init__(self, levels, groups, shard, wide, sems):
        self.levels, self.groups, self.size = levels, groups, MATS // groups
        self.shard, self.wide = shard, wide
        self.own, self.zs, self.zr, self.xs, self.xr, self.ys, self.yr = sems
        self.at = place()
        self.done = 0
        self.total = (groups + 1) * levels

    @staticmethod
    def semaphores(levels, groups):
        sem = pltpu.SemaphoreType.DMA
        pair = sem((groups, levels, 2))
        return [sem, pair, sem((groups, levels)), pair, pair, pair, pair]

    def block(self, g, xx, zz, yy):
        return self.wide.at[pl.ds(g * self.size, self.size), xx, zz, yy]

    def source(self, g, xx, zz, yy, own):
        return self.shard.at[pl.ds(g * self.size, self.size)] if own else self.block(g, xx, zz, yy)

    def z_copy(self, g, zz, up, own):
        z, y, x, c = self.at
        return pltpu.make_async_remote_copy(
            self.source(g, x, zz, y, own), self.block(g, x, zz, y), self.zs.at[g, zz, up], self.zr.at[g, zz],
            device_id=device(z + 1 if up else z - 1, y, x, c), device_id_type=DT,
        )

    def x_copy(self, g, zz, yy, own):
        z, y, x, c = self.at
        return pltpu.make_async_remote_copy(
            self.source(g, x, zz, yy, own), self.block(g, x, zz, yy), self.xs.at[g, zz, yy],
            self.xr.at[g, zz, yy], device_id=device(z, y, 1 - x, c), device_id_type=DT,
        )

    def y_copy(self, g, zz, xx, own):
        z, y, x, c = self.at
        return pltpu.make_async_remote_copy(
            self.source(g, xx, zz, y, own), self.block(g, xx, zz, y), self.ys.at[g, zz, xx],
            self.yr.at[g, zz, xx], device_id=device(z, 1 - y, x, c), device_id_type=DT,
        )

    def begin(self):
        z, y, x, c = self.at
        self.local = pltpu.make_async_copy(self.shard, self.wide.at[:, x, z, y], self.own)
        self.local.start()

    def first(self, g, d):
        z, y, x, c = self.at
        top = self.levels - 1

        @pl.when(d == 0)
        def _():
            start_when(z < top, self.z_copy(g, z, 1, True))
            start_when(z > 0, self.z_copy(g, z, 0, True))
            self.x_copy(g, z, y, True).start()
            self.y_copy(g, z, x, True).start()

        for up in (1, 0):
            zz = z - d if up else z + d
            here = (zz >= 0) if up else (zz <= top)

            @pl.when((d > 0) & here)
            def _():
                self.z_copy(g, zz, up, False).wait_recv()
                start_when((z < top) if up else (z > 0), self.z_copy(g, zz, up, False))
                self.x_copy(g, zz, y, False).start()
                self.y_copy(g, zz, x, False).start()

    def second(self, g, d):
        z, y, x, c = self.at
        even = lax.rem(g, 2) == 0
        for up in (1, 0):
            zz = z - d if up else z + d
            here = (zz >= 0) if up else ((zz < self.levels) & (d > 0))

            @pl.when(here & even)
            def _():
                self.x_copy(g, zz, y, False).wait_recv()
                self.y_copy(g, zz, 1 - x, False).start()

            @pl.when(here & jnp.logical_not(even))
            def _():
                self.y_copy(g, zz, x, False).wait_recv()
                self.x_copy(g, zz, 1 - y, False).start()

    def tick(self, t):
        g, d = t // self.levels, lax.rem(t, self.levels)

        @pl.when(g < self.groups)
        def _():
            self.first(g, d)

        @pl.when(g >= 1)
        def _():
            self.second(g - 1, d)

    def run(self, count):
        count = max(0, min(count, self.total - self.done))
        start = self.done
        self.done += count
        if count:
            def body(i, carry):
                self.tick(start + i)
                return carry

            lax.fori_loop(0, count, body, 0)

    def reserve(self, count):
        if self.total - self.done < count:
            return lambda i: None
        start = self.done
        self.done += count
        return lambda i: self.tick(start + i)

    def need(self, g):
        self.run((g + 2) * self.levels - self.done)
        z, y, x, c = self.at

        def body(zz, carry):
            if g % 2 == 0:
                self.y_copy(g, zz, x, False).wait_recv()
                self.y_copy(g, zz, 1 - x, False).wait_recv()
            else:
                self.x_copy(g, zz, y, False).wait_recv()
                self.x_copy(g, zz, 1 - y, False).wait_recv()
            return carry

        lax.fori_loop(0, self.levels, body, 0)
        if g == 0:
            self.local.wait()

    def drain(self):
        z, y, x, c = self.at

        def group(g, carry):
            def sent(zz, inner):
                self.x_copy(g, zz, y, False).wait_send()
                self.y_copy(g, zz, x, False).wait_send()

                @pl.when(lax.rem(g, 2) == 0)
                def _():
                    self.y_copy(g, zz, 1 - x, False).wait_send()

                @pl.when(lax.rem(g, 2) == 1)
                def _():
                    self.x_copy(g, zz, 1 - y, False).wait_send()

                @pl.when((z < self.levels - 1) & (zz <= z))
                def _():
                    self.z_copy(g, zz, 1, False).wait_send()

                @pl.when((z > 0) & (zz >= z))
                def _():
                    self.z_copy(g, zz, 0, False).wait_send()

                return inner

            return lax.fori_loop(0, self.levels, sent, carry)

        lax.fori_loop(0, self.groups, group, 0)


HALF = L // 2
KEYS = 768
HALF_FRAMES = FRAMES // 2
BLOCK = 32


def dot(a, b, dims):
    return lax.dot_general(a, b, (dims, ((), ())), preferred_element_type=jnp.float32)


NN, NT, TN = ((1,), (0,)), ((1,), (1,)), ((0,), (0,))


def flat_panel(ref, mat, side):
    return ref[mat, side].reshape(D, COLS)


def flat_rows(panel, j):
    per = COLS // (2 * panel.shape[2])
    return panel[pl.ds(j * per, per)].reshape(COLS, COLS)


def rows_loop(count, body):
    def run(i, carry):
        body(pl.ds(pl.multiple_of(i * BLOCK, BLOCK), BLOCK), i)
        return carry

    lax.fori_loop(0, count // BLOCK, run, 0)


def loop(count, body):
    def run(i, carry):
        body(i)
        return carry

    lax.fori_loop(0, count, run, 0)


def normed_block(values):
    centre = values - jnp.mean(values, axis=-1, keepdims=True)
    spread = jnp.mean(centre * centre, axis=-1, keepdims=True)
    scaled = lax.rsqrt(spread + 1e-05)
    return centre * scaled, scaled


def panels_row(ref, rows):
    return jnp.concatenate([ref[j, rows, :].astype(jnp.float32) for j in range(4)], axis=1)


def forward_kernel(levels, groups, fast, *refs):
    f32, bf = jnp.float32, jnp.bfloat16
    names = FORWARD_IN + (("pack",) if fast else ("norm_in", "bias_in")) + tuple(n for n, _, _ in FORWARD_OUT) + (
        "wide", "x", "dy", "e", "norm", "bias", "a1", "a2", "a3", "h1", "h2", "qkv", "c1", "q2", "c2", "ek", "ev",
        "lse1", "lse2", "z", "slope", "s", "p", "acc", "part", "got", "packs", "padrow", "outrows",
        "in_sem", "swap_send", "swap_recv", "part_send", "part_recv", "pack_send", "pack_recv", "out_sem",
    )
    r = dict(zip(names, refs))
    gather = Gather(levels, groups, r["shard"], r["wide"], refs[len(names):])
    z, y, x, c = place()
    dp = z * 2 + y
    mate = (dp, x, 1 - c)
    count = levels * 4
    me = dp * 2 + x

    def peer(i):
        return (i // 2, lax.rem(i, 2), c)

    bar = pltpu.get_barrier_semaphore()
    loop(count - 1, lambda k: pl.semaphore_signal(
        bar, inc=1, device_id=peer(lax.rem(me + k + 1, count)), device_id_type=DT))
    pl.semaphore_signal(bar, inc=1, device_id=mate, device_id_type=DT)
    pl.semaphore_wait(bar, count)

    def remote(src, dst, send, recv, dev):
        return pltpu.make_async_remote_copy(src, dst, send, recv, device_id=dev, device_id_type=DT)

    inputs = (("tokens", "x"), ("frames", "e"), ("cotangent", "dy"))

    def swap(k, slot):
        src, dst = inputs[k]
        return remote(r[src], r[dst].at[slot], r["swap_send"].at[k], r["swap_recv"].at[k], mate)

    def local(k):
        src, dst = inputs[k]
        return pltpu.make_async_copy(r[src], r[dst].at[c], r["in_sem"].at[k])

    if fast:
        def pack_copy(k, slot):
            return remote(r["pack"], r["packs"].at[slot], r["pack_send"].at[k], r["pack_recv"].at[slot],
                          peer(lax.rem(me + k + 1, count)))

        loop(count - 1, lambda k: pack_copy(k, me).start())
        own_pack = pltpu.make_async_copy(r["pack"], r["packs"].at[me], r["in_sem"].at[3])
        own_pack.start()
    swap(0, c).start()
    local(0).start()
    gather.begin()
    gather.run(1)
    for k in (1, 2):
        swap(k, c).start()
        local(k).start()

    def arrived(k):
        local(k).wait()
        swap(k, 1 - c).wait_recv()

    outs = {}

    def emit(out, scratch):
        k = len(outs)
        outs[out] = pltpu.make_async_copy(scratch, r[out], r["out_sem"].at[k])
        outs[out].start()

    if fast:
        own_pack.wait()
        loop(count - 1, lambda k: pack_copy(k, lax.rem(me + k + 1, count)).wait_recv())
        for i in range(2 * levels):
            for xx in range(2):
                block = r["packs"][i * 2 + xx]
                if xx == 0:
                    r["norm"][:, i * 128 : (i + 1) * 128] = block
                r["bias"][i * 2 + xx : i * 2 + xx + 1, 0:128] = block[9:10]
                r["bias"][i * 2 + xx : i * 2 + xx + 1, 128:256] = block[10:11]
    else:
        r["norm"][...] = r["norm_in"][...]
        r["bias"][...] = r["bias_in"][...]
    emit("norm_out", r["norm"])

    def norm_row(k):
        return r["norm"][k : k + 1, :]

    def bias_row(k, side):
        return r["bias"][pl.ds(k * 2 + side, 1), :]

    key = lax.broadcasted_iota(jnp.int32, (1, 2 * KEYS), 1)
    real = lax.rem(key, KEYS) < HALF_FRAMES
    r["padrow"][0:1, :] = jnp.where(real, 0.0, -1e30).astype(f32)
    for i in range(3):
        for side in range(2):
            r["qkv"][i, side, L:512, :] = jnp.zeros((512 - L, COLS), bf)

    arrived(0)

    def ln1(half):
        def body(rows, i):
            normed, _ = normed_block(r["x"][half, rows, :].astype(f32))
            out = (normed * norm_row(0) + norm_row(1)).astype(bf)
            r["a1"][pl.ds(pl.multiple_of(half * HALF + i * BLOCK, BLOCK), BLOCK), :] = out

        rows_loop(HALF, body)

    ln1(0)
    ln1(1)
    emit("a1_out", r["a1"])
    emit("x_out", r["x"])

    def project_one(i, side):
        bias = bias_row(0, side) if i == 0 else bias_row(1, side)
        acc = dot(r["a1"][...], flat_panel(r["wide"], i, side), NN)
        if i != 1:
            acc = acc + bias
        r["qkv"][i, side, 0:L, :] = acc.astype(bf)

    gather.need(0)
    for i in range(2):
        loop(2, lambda side: project_one(i, side))
    gather.need(1)
    loop(2, lambda side: project_one(2, side))
    emit("qkv_out", r["qkv"])

    lane = lax.broadcasted_iota(jnp.int32, (1, 128), 1)
    low = lane < HD

    def attend(query, key_parts, values, width, causal, lse, ctx, tick):
        def body(t):
            side, half = t // 2, lax.rem(t, 2)
            lanes = pl.ds(pl.multiple_of(half * 128, 128), 128)
            q = query(side, lanes)
            found = []
            for sub in range(2):
                mine = low if sub == 0 else jnp.logical_not(low)
                qh = jnp.where(mine, q.astype(f32) * 0.125, 0.0).astype(bf)
                for n, part in enumerate(key_parts(side, lanes)):
                    r["s"][:, n * width : (n + 1) * width] = dot(qh, part, NT)
                total = width * len(key_parts(side, lanes))

                def rows_body(rows, i):
                    s = r["s"][rows, 0:total]
                    if causal:
                        row = i * BLOCK + lax.broadcasted_iota(jnp.int32, (BLOCK, total), 0)
                        col = lax.broadcasted_iota(jnp.int32, (BLOCK, total), 1)
                        s = jnp.where(col <= row, s, -1e30)
                    else:
                        s = s + r["padrow"][0:1, 0:total]
                    top = jnp.max(s, axis=-1, keepdims=True)
                    e = jnp.exp(s - top)
                    weight = jnp.sum(e, axis=-1, keepdims=True)
                    r["p"][rows, 0:total] = (e * (1.0 / weight)).astype(bf)
                    lse[rows, :] = jnp.where(lane == t * 2 + sub, top + jnp.log(weight), lse[rows, :])

                rows_loop(L, rows_body)
                acc = None
                for n, part in enumerate(values(side, lanes)):
                    more = dot(r["p"][:, n * width : (n + 1) * width], part, NN)
                    acc = more if acc is None else acc + more
                found.append(acc)
                tick(t * 2 + sub)
            ctx[side, :, lanes] = jnp.where(low, found[0], found[1]).astype(bf)

        loop(4, body)

    attend(
        lambda side, lanes: r["qkv"][0, side, 0:L, lanes],
        lambda side, lanes: [r["qkv"][1, side, :, lanes]],
        lambda side, lanes: [r["qkv"][2, side, :, lanes]],
        512, True, r["lse1"], r["c1"], gather.reserve(8) if levels == 4 else (lambda i: None),
    )
    emit("lse1_out", r["lse1"])
    emit("c1_out", r["c1"])

    def collect(n, ctx, mat):
        def body(j):
            rows = pl.ds(pl.multiple_of(j * COLS, COLS), COLS)
            acc = None
            for side in range(2):
                more = dot(ctx[side], flat_rows(r["wide"].at[mat, side], j), NT)
                acc = more if acc is None else acc + more
            r["part"][n, j] = acc.astype(bf)
            trade(n, j).start()

        loop(4, body)

    def trade(n, j):
        return remote(r["part"].at[n, j], r["got"].at[n, j], r["part_send"].at[n, j], r["part_recv"].at[n, j], mate)

    def traded(n):
        loop(4, lambda j: trade(n, j).wait_recv())

    def residual(n, base, bias_k, out, gain_k, normed_out):
        def body(rows, i):
            v = base(rows, i) + norm_row(bias_k) + (panels_row(r["part"].at[n], rows) + panels_row(r["got"].at[n], rows))
            out[rows, :] = v
            normed, _ = normed_block(v)
            normed_out[rows, :] = (normed * norm_row(gain_k) + norm_row(gain_k + 1)).astype(bf)

        rows_loop(L, body)

    def x_rows(rows, i):
        half = i // (HALF // BLOCK)
        inner = pl.ds(pl.multiple_of((i - half * (HALF // BLOCK)) * BLOCK, BLOCK), BLOCK)
        return r["x"][half, inner, :].astype(f32)

    collect(0, r["c1"], 3)
    traded(0)
    residual(0, x_rows, 6, r["h1"], 2, r["a2"])
    emit("h1_out", r["h1"])
    emit("a2_out", r["a2"])

    gather.need(2)

    def query_two(side):
        acc = dot(r["a2"][...], flat_panel(r["wide"], 4, side), NN) + bias_row(2, side)
        r["q2"][side] = acc.astype(bf)

    loop(2, query_two)
    emit("q2_out", r["q2"])
    arrived(1)
    emit("e_out", r["e"])

    def frame_keys(t):
        side, half = t // 2, lax.rem(t, 2)
        r["ek"][side, half] = dot(r["e"][half], flat_panel(r["wide"], 5, side), NN).astype(bf)

    loop(4, frame_keys)
    emit("ek_out", r["ek"])
    gather.need(3)

    def frame_values(t):
        side, half = t // 2, lax.rem(t, 2)
        acc = dot(r["e"][half], flat_panel(r["wide"], 6, side), NN) + bias_row(3, side)
        r["ev"][side, half] = acc.astype(bf)

    loop(4, frame_values)
    emit("ev_out", r["ev"])
    attend(
        lambda side, lanes: r["q2"][side, :, lanes],
        lambda side, lanes: [r["ek"][side, half, :, lanes] for half in range(2)],
        lambda side, lanes: [r["ev"][side, half, :, lanes] for half in range(2)],
        KEYS, False, r["lse2"], r["c2"], gather.reserve(8) if levels == 4 else (lambda i: None),
    )
    emit("lse2_out", r["lse2"])
    emit("c2_out", r["c2"])
    collect(1, r["c2"], 7)
    traded(1)
    residual(1, lambda rows, i: r["h1"][rows, :], 7, r["h2"], 4, r["a3"])
    emit("h2_out", r["h2"])
    emit("a3_out", r["a3"])
    arrived(2)
    emit("dy_out", r["dy"])

    def hidden(t):
        m, side = t // 2, lax.rem(t, 2)
        u = dot(r["a3"][...], flat_panel(r["wide"], 8 + m, side), NN) + bias_row(4 + m, side)
        half = 0.5 * (1.0 + lax.erf(u * 0.7071067811865476))
        r["z"][t] = (u * half).astype(bf)
        r["slope"][t] = (half + u * jnp.exp(-0.5 * u * u) * 0.3989422804014327).astype(bf)

    def result(t):
        m, side = t // 2, lax.rem(t, 2)

        def tile(j):
            cols = pl.ds(pl.multiple_of(j * COLS, COLS), COLS)
            more = dot(r["z"][t], flat_rows(r["wide"].at[12 + m, side], j), NT)

            @pl.when(t == 0)
            def _():
                r["acc"][:, cols] = more

            @pl.when(t > 0)
            def _():
                r["acc"][:, cols] += more

        loop(4, tile)

    per = groups // 4
    mats = MATS // groups
    for k in range(max(1, groups // 4)):
        gather.need(groups // 2 + k)
        span = 8 // max(1, groups // 4)
        loop(span, lambda t: hidden(k * span + t))
    emit("z_out", r["z"])
    emit("slope_out", r["slope"])
    for k in range(max(1, groups // 4)):
        gather.need(groups * 3 // 4 + k if groups >= 4 else groups - 1)
        span = 8 // max(1, groups // 4)
        loop(span, lambda t: result(k * span + t))

    emit("wide_out", r["wide"])

    for half in range(2):
        @pl.when(c == half)
        def _():
            far = (1 - half) * HALF

            def body(j):
                cols = pl.ds(pl.multiple_of(j * COLS, COLS), COLS)
                r["part"][2, j, 0:HALF, :] = r["acc"][far : far + HALF, cols].astype(bf)

            loop(4, body)

    last = remote(
        r["part"].at[2, :, 0:HALF], r["got"].at[2, :, 0:HALF], r["part_send"].at[2, 0], r["part_recv"].at[2, 0], mate
    )
    last.start()
    last.wait_recv()

    def finish(rows, i):
        here = pl.ds(pl.multiple_of(c * HALF + i * BLOCK, BLOCK), BLOCK)
        own = r["acc"][here, :].astype(bf).astype(f32)
        v = r["h2"][here, :] + norm_row(8) + (own + panels_row(r["got"].at[2], rows))
        r["outrows"][rows, :] = v.astype(bf)

    rows_loop(HALF, finish)
    emit("layer_out", r["outrows"])

    for k in range(3):
        swap(k, c).wait_send()
    if fast:
        loop(count - 1, lambda k: pack_copy(k, me).wait_send())
    for n in range(2):
        loop(4, lambda j: trade(n, j).wait_send())
    last.wait_send()
    gather.drain()
    for copy in outs.values():
        copy.wait()


FORWARD_IN = ("shard", "tokens", "frames", "cotangent")
FORWARD_OUT = (
    ("layer_out", (HALF, D), jnp.bfloat16), ("norm_out", (16, D), jnp.float32),
    ("a1_out", (L, D), jnp.bfloat16), ("x_out", (2, HALF, D), jnp.bfloat16),
    ("qkv_out", (3, 2, 512, COLS), jnp.bfloat16), ("lse1_out", (L, 128), jnp.float32),
    ("c1_out", (2, L, COLS), jnp.bfloat16), ("h1_out", (L, D), jnp.float32), ("a2_out", (L, D), jnp.bfloat16),
    ("q2_out", (2, L, COLS), jnp.bfloat16), ("e_out", (2, KEYS, D), jnp.bfloat16),
    ("ek_out", (2, 2, KEYS, COLS), jnp.bfloat16), ("ev_out", (2, 2, KEYS, COLS), jnp.bfloat16),
    ("lse2_out", (L, 128), jnp.float32), ("c2_out", (2, L, COLS), jnp.bfloat16),
    ("h2_out", (L, D), jnp.float32), ("a3_out", (L, D), jnp.bfloat16), ("dy_out", (2, HALF, D), jnp.bfloat16),
    ("z_out", (8, L, COLS), jnp.bfloat16), ("slope_out", (8, L, COLS), jnp.bfloat16), ("wide_out", None, jnp.bfloat16),
)


def forward(shard, tokens, frames, cotangent, small, shards):
    levels, rows = shards // 2, D // shards
    groups = 8 if levels <= 4 else 4
    fast = len(small) == 1
    f32, bf = jnp.float32, jnp.bfloat16
    sem = pltpu.SemaphoreType.DMA
    vm, hbm = pl.BlockSpec(memory_space=pltpu.VMEM), pl.BlockSpec(memory_space=pl.ANY)
    wide = (MATS, 2, levels, 2, rows, COLS)
    shapes = [(n, wide if s is None else s, t) for n, s, t in FORWARD_OUT]
    peers = shards * 2
    scratch = [
        pltpu.VMEM(wide, bf), pltpu.VMEM((2, HALF, D), bf), pltpu.VMEM((2, HALF, D), bf), pltpu.VMEM((2, KEYS, D), bf),
        pltpu.VMEM((16, D), f32), pltpu.VMEM((16, COLS), f32),
        pltpu.VMEM((L, D), bf), pltpu.VMEM((L, D), bf), pltpu.VMEM((L, D), bf),
        pltpu.VMEM((L, D), f32), pltpu.VMEM((L, D), f32),
        pltpu.VMEM((3, 2, 512, COLS), bf), pltpu.VMEM((2, L, COLS), bf), pltpu.VMEM((2, L, COLS), bf),
        pltpu.VMEM((2, L, COLS), bf), pltpu.VMEM((2, 2, KEYS, COLS), bf), pltpu.VMEM((2, 2, KEYS, COLS), bf),
        pltpu.VMEM((L, 128), f32), pltpu.VMEM((L, 128), f32),
        pltpu.VMEM((8, L, COLS), bf), pltpu.VMEM((8, L, COLS), bf),
        pltpu.VMEM((L, 2 * KEYS), f32), pltpu.VMEM((L, 2 * KEYS), bf), pltpu.VMEM((L, D), f32),
        pltpu.VMEM((3, 4, L, COLS), bf), pltpu.VMEM((3, 4, L, COLS), bf),
        pltpu.VMEM((peers, 16, 128) if fast else (1, 16, 128), f32), pltpu.VMEM((8, 2 * KEYS), f32),
        pltpu.VMEM((HALF, D), bf),
        sem((4,)), sem((3,)), sem((3,)), sem((3, 4)), sem((3, 4)), sem((peers,)), sem((peers,)),
        sem((len(FORWARD_OUT),)),
    ]
    outs = pl.pallas_call(
        partial(forward_kernel, levels, groups, fast),
        out_shape=[jax.ShapeDtypeStruct(s, t) for _, s, t in shapes],
        in_specs=[vm, hbm, hbm, hbm] + [vm] * len(small),
        out_specs=[hbm] * len(shapes),
        scratch_shapes=scratch + Gather.semaphores(levels, groups),
        compiler_params=pltpu.CompilerParams(
            collective_id=0, has_side_effects=True, vmem_limit_bytes=63 * 2**20
        ),
        name="forward",
    )(shard, tokens, frames, cotangent, *small)
    return {n.removesuffix("_out") if n != "layer_out" else n: v for (n, _, _), v in zip(shapes, outs)}


RING = 4


class Scatter:
    def __init__(self, levels, part, own, bufs, sems):
        self.levels, self.part, self.own = levels, part, own
        self.even, self.odd, self.two, self.line = bufs
        self.s1, self.r1, self.s2, self.r2, self.s3, self.r3 = sems
        self.at = place()
        self.sent = self.steps = self.ready = 0

    @staticmethod
    def buffers(levels, rows):
        bf = jnp.bfloat16
        return [
            pltpu.VMEM((2, 2, levels, rows, COLS), bf), pltpu.VMEM((2, levels, 2, rows, COLS), bf),
            pltpu.VMEM((RING, levels, rows, COLS), bf), pltpu.VMEM((RING, levels, rows, COLS), bf),
        ]

    @staticmethod
    def semaphores(levels):
        sem = pltpu.SemaphoreType.DMA
        one = sem((MATS,))
        many = sem((MATS, levels))
        return [one, one, one, one, many, many]

    def first(self, g, even):
        z, y, x, c = self.at
        m = MATS - 1 - g
        if even:
            src, dst, dev = self.part.at[m, :, :, 1 - y], self.even.at[lax.rem(g // 2, 2)], device(z, 1 - y, x, c)
        else:
            src, dst, dev = self.part.at[m, 1 - x], self.odd.at[lax.rem(g // 2, 2)], device(z, y, 1 - x, c)
        return pltpu.make_async_remote_copy(
            src, dst, self.s1.at[g], self.r1.at[g], device_id=dev, device_id_type=DT
        )

    def second(self, g, even):
        z, y, x, c = self.at
        m = MATS - 1 - g
        if even:
            src, dev = self.part.at[m, 1 - x, :, y], device(z, y, 1 - x, c)
        else:
            src, dev = self.part.at[m, x, :, 1 - y], device(z, 1 - y, x, c)
        return pltpu.make_async_remote_copy(
            src, self.two.at[lax.rem(g, RING)], self.s2.at[g], self.r2.at[g], device_id=dev, device_id_type=DT
        )

    def third(self, g, zz, k):
        z, y, x, c = self.at
        return pltpu.make_async_remote_copy(
            self.part.at[MATS - 1 - g, x, zz, y], self.line.at[lax.rem(g, RING), k], self.s3.at[g, zz],
            self.r3.at[g, k], device_id=device(zz, y, x, c), device_id_type=DT,
        )

    def both(self, g, body):
        even = lax.rem(g, 2) == 0

        @pl.when(even)
        def _():
            body(True)

        @pl.when(jnp.logical_not(even))
        def _():
            body(False)

    def send(self, count):
        def body(i):
            self.both(i, lambda even: self.first(i, even).start())

        start = self.sent
        self.sent += count
        loop(count, lambda i: body(start + i))

    def add(self, at, got):
        self.part[at] = (self.part[at].astype(jnp.float32) + got.astype(jnp.float32)).astype(jnp.bfloat16)

    def step_a(self, g):
        z, y, x, c = self.at
        m = MATS - 1 - g

        def run(even):
            self.first(g, even).wait_recv()
            for k in range(2):
                def body(zz):
                    if even:
                        self.add((m, k, zz, y), self.even[lax.rem(g // 2, 2), k, zz])
                    else:
                        self.add((m, x, zz, k), self.odd[lax.rem(g // 2, 2), zz, k])

                loop(self.levels, body)
            self.second(g, even).start()

        self.both(g, run)

    def step_b(self, g):
        z, y, x, c = self.at
        m = MATS - 1 - g

        def run(even):
            self.second(g, even).wait_recv()
            loop(self.levels, lambda zz: self.add((m, x, zz, y), self.two[lax.rem(g, RING), zz]))

        self.both(g, run)
        loop(self.levels - 1, lambda k: self.third(g, lax.rem(z + k + 1, self.levels), z).start())

    def step_c(self, g):
        z, y, x, c = self.at
        m = MATS - 1 - g
        loop(self.levels - 1, lambda k: self.third(g, z, lax.rem(z + k + 1, self.levels)).wait_recv())
        self.own[m] = self.part[m, x, z, y].astype(jnp.float32)

        def body(k):
            @pl.when(k != z)
            def _():
                self.own[m] += self.line[lax.rem(g, RING), k].astype(jnp.float32)

        loop(self.levels, body)

    def step(self, t):
        @pl.when(t < MATS)
        def _():
            self.step_a(t)

        @pl.when((t >= 1) & (t <= MATS))
        def _():
            self.step_b(t - 1)

        @pl.when(t >= 2)
        def _():
            self.step_c(t - 2)

    def turn(self, count):
        start, first = self.steps, self.sent
        self.steps += count
        self.sent = max(first, min(MATS, self.steps + RING - 2))
        assert self.sent <= self.ready

        def body(i):
            t = start + i
            self.step(t)
            g = t + RING - 2

            @pl.when((g >= first) & (g < MATS))
            def _():
                self.both(g, lambda even: self.first(g, even).start())

        return body

    def run(self, count):
        loop(count, self.turn(count))

    def drain(self):
        z, y, x, c = self.at

        def body(g):
            def run(even):
                self.first(g, even).wait_send()
                self.second(g, even).wait_send()

            self.both(g, run)
            loop(self.levels - 1, lambda k: self.third(g, lax.rem(z + k + 1, self.levels), z).wait_send())

        loop(MATS, body)


BACKWARD_IN = (
    "dy", "wide", "slope", "z", "a3", "h2", "norm", "c2", "q2", "lse2", "ek", "ev", "e", "a2", "h1",
    "c1", "qkv", "lse1", "a1", "x",
)


def backward_kernel(levels, fast, *refs):
    f32, bf = jnp.float32, jnp.bfloat16
    given = dict(zip(BACKWARD_IN, refs))
    outs = ("owned_out", "input_out", "frame_out") + (("small_out",) if fast else ("cols_out", "bcols_out"))
    names = outs + (
        "part", "own", "dy", "slope", "z", "left", "h", "norm", "c2", "q2", "lse2", "ek", "ev", "e", "a2",
        "c1", "qkv", "lse1", "x", "dh", "dhb", "dc", "stat", "s", "dp", "p", "ds", "mine", "got", "fsend", "frecv",
        "fout", "cols", "bcols", "small", "smallgot", "smallsum", "in_sem", "trade_send", "trade_recv", "frame_send",
        "frame_recv", "frame_out_sem", "small_send", "small_recv", "out_sem",
    )
    rest = refs[len(BACKWARD_IN):]
    r = dict(zip(names, rest))
    rest = rest[len(names):]
    scatter = Scatter(levels, r["part"], r["own"], rest[:4], rest[4:])
    z, y, x, c = place()
    dp = z * 2 + y
    mate = (dp, x, 1 - c)
    count = levels * 4
    me = dp * 2 + x
    rows_of = D // (levels * 2)
    per = COLS // (2 * rows_of)

    def peer(i):
        return (i // 2, lax.rem(i, 2), c)

    loads = {}

    def load(name, src, dst):
        loads[name] = pltpu.make_async_copy(src, dst, r["in_sem"].at[len(loads)])
        loads[name].start()

    def loaded(*which):
        for name in which:
            loads[name].wait()

    load("dy", given["dy"], r["dy"])
    load("w2", given["wide"].at[12:16], r["part"].at[12:16])
    load("slope", given["slope"], r["slope"])
    load("z", given["z"], r["z"])
    load("w1", given["wide"].at[8:12], r["part"].at[8:12])
    load("a3", given["a3"], r["left"])
    load("h2", given["h2"], r["h"])
    load("w0", given["wide"].at[0:8], r["part"].at[0:8])
    for name in ("norm", "c2", "q2", "lse2", "ek", "ev", "e", "a2", "c1", "qkv", "lse1", "x"):
        load(name, given[name], r[name])

    bar = pltpu.get_barrier_semaphore()
    loop(count - 1, lambda k: pl.semaphore_signal(
        bar, inc=1, device_id=peer(lax.rem(me + k + 1, count)), device_id_type=DT))
    pl.semaphore_signal(bar, inc=1, device_id=mate, device_id_type=DT)
    pl.semaphore_wait(bar, count)

    def remote(src, dst, send, recv, dev):
        return pltpu.make_async_remote_copy(src, dst, send, recv, device_id=dev, device_id_type=DT)

    def trade(n, j):
        return remote(r["mine"].at[n % 2, j], r["got"].at[n % 2, j], r["trade_send"].at[n, j],
                      r["trade_recv"].at[n, j], mate)

    def panel(mat, side):
        return r["part"][mat, side].reshape(D, COLS)

    def grads(lefts, items):
        def body(j):
            cols = pl.ds(pl.multiple_of(j * COLS, COLS), COLS)
            turned = [v.T for v in lefts(cols)]
            for mat, side, rights in items:
                acc = None
                for t, right in zip(turned, rights()):
                    more = dot(t, right, NN)
                    acc = more if acc is None else acc + more
                r["part"][mat, side, pl.ds(j * per, per)] = acc.astype(bf).reshape(per, 2, rows_of, COLS)

        loop(4, body)

    def send_back(n, items):
        if n >= 2:
            loop(4, lambda j: trade(n - 2, j).wait_send())

        def body(j):
            acc = None
            for value, mat, side in items:
                more = dot(value(), flat_rows(r["part"].at[mat, side], j), NT)
                acc = more if acc is None else acc + more
            r["mine"][n % 2, j] = acc.astype(bf)
            trade(n, j).start()

        loop(4, body)

    def fold(v):
        return jnp.sum(v.reshape(BLOCK // 8, 8, D), axis=0)

    def norm_row(k):
        return r["norm"][k : k + 1, :]

    def grow(k, v):
        r["cols"][k * 8 : (k + 1) * 8, :] += fold(v)

    def half_rows(ref, i):
        half = i // (HALF // BLOCK)
        inner = pl.ds(pl.multiple_of((i - half * (HALF // BLOCK)) * BLOCK, BLOCK), BLOCK)
        return ref[half, inner, :].astype(f32)

    def norm_back(n, k, base, incoming, sum_k):
        loop(4, lambda j: trade(n, j).wait_recv())

        def body(rows, i):
            normed, scaled = normed_block(base(rows, i))
            dn = panels_row(r["mine"].at[n % 2], rows) + panels_row(r["got"].at[n % 2], rows)
            inner = dn * norm_row(k)
            back = scaled * (
                inner - jnp.mean(inner, axis=-1, keepdims=True)
                - normed * jnp.mean(inner * normed, axis=-1, keepdims=True)
            )
            came = incoming(rows, i)
            out = came + back
            r["dh"][rows, :] = out
            grow(k, dn * normed)
            grow(k + 1, dn)
            if sum_k is not None:
                r["dhb"][rows, :] = out.astype(bf)
                grow(sum_k, out)
            if n == 0:
                grow(8, came)

        rows_loop(L, body)

    r["cols"][...] = jnp.zeros((72, D), f32)
    loaded("dy", "w2", "slope")

    def hidden_back(t):
        m, side = t // 2, lax.rem(t, 2)
        du = (dot(r["dy"][...].reshape(L, D), panel(12 + m, side), NN) * r["slope"][t].astype(f32)).astype(bf)
        r["slope"][t] = du
        r["bcols"][pl.ds(8 + t, 1), :] = jnp.sum(du.astype(f32), axis=0, keepdims=True)

    loop(8, hidden_back)
    loaded("z")
    grads(
        lambda cols: [r["dy"][:, :, cols].reshape(L, COLS)],
        [(12 + t // 2, t % 2, lambda t=t: [r["z"][t]]) for t in range(8)],
    )
    scatter.send(4)
    loaded("w1")
    send_back(0, [(lambda t=t: r["slope"][t], 8 + t // 2, t % 2) for t in range(8)])
    loaded("a3", "h2", "norm")
    grads(
        lambda cols: [r["left"][:, cols]],
        [(8 + t // 2, t % 2, lambda t=t: [r["slope"][t]]) for t in range(8)],
    )
    scatter.ready = 8
    load("a1", given["a1"], r["left"])
    norm_back(0, 4, lambda rows, i: r["h"][rows, :], lambda rows, i: half_rows(r["dy"], i), 7)
    load("h1", given["h1"], r["h"])
    scatter.run(1)
    loaded("w0")

    def context_back(mat):
        def body(side):
            r["dc"][side] = dot(r["dhb"][...], panel(mat, side), NN).astype(bf)

        loop(2, body)

    def statistics(lse, ctx):
        r["stat"][0:8, :] = lse[...].T[0:8, :]
        for side in range(2):
            both = (r["dc"][side].astype(f32) * ctx[side].astype(f32)).T
            r["stat"][8 + side * 4 : 12 + side * 4, :] = jnp.sum(both.reshape(4, HD, L), axis=1)

    lane = lax.broadcasted_iota(jnp.int32, (1, 128), 1)
    low = lane < HD
    low_row = lax.broadcasted_iota(jnp.int32, (128, 1), 0) < HD

    def attend_back(query, keys, values, parts, width, causal, turn):
        def body(t):
            side, half = t // 2, lax.rem(t, 2)
            lanes = pl.ds(pl.multiple_of(half * 128, 128), 128)
            q = query[(side, slice(0, L), lanes)].astype(f32) * 0.125
            dc = r["dc"][side, :, lanes].astype(f32)
            back = None
            for n in range(parts):
                at = (side, n, slice(None), lanes) if parts > 1 else (side, slice(0, L), lanes)
                k, v = keys[at], values[at]
                flat = k.T
                dk = dv = None
                for sub in range(2):
                    mine = low if sub == 0 else jnp.logical_not(low)
                    mine_row = low_row if sub == 0 else jnp.logical_not(low_row)
                    qh = jnp.where(mine, q, 0.0).astype(bf)
                    dm = jnp.where(mine, dc, 0.0).astype(bf)
                    kt = jnp.where(mine_row, flat.astype(f32), 0.0).astype(bf)
                    r["s"][0:width, :] = dot(k, qh, NT)
                    r["dp"][0:width, :] = dot(v, dm, NT)
                    lse = r["stat"][pl.ds(t * 2 + sub, 1), :]
                    delta = r["stat"][pl.ds(8 + t * 2 + sub, 1), :]

                    def rows_body(rows, i):
                        key = i * BLOCK + lax.broadcasted_iota(jnp.int32, (BLOCK, L), 0)
                        if causal:
                            keep = lax.broadcasted_iota(jnp.int32, (BLOCK, L), 1) >= key
                        else:
                            keep = key < HALF_FRAMES
                        p = jnp.where(keep, jnp.exp(jnp.where(keep, r["s"][rows, :], -1e30) - lse), 0.0)
                        r["p"][rows, :] = p.astype(bf)
                        r["ds"][rows, :] = (p * (r["dp"][rows, :] - delta)).astype(bf)

                    rows_loop(width, rows_body)
                    p, ds = r["p"][0:width, :], r["ds"][0:width, :]
                    dv = dot(p, dm, NN) if dv is None else dv + dot(p, dm, NN)
                    dk = dot(ds, qh, NN) if dk is None else dk + dot(ds, qh, NN)
                    more = dot(kt, ds, NN)
                    back = more if back is None else back + more
                keys[at] = dk.astype(bf)
                values[at] = dv.astype(bf)
            query[(side, slice(0, L), lanes)] = (back.T * 0.125).astype(bf)
            turn(t)

        loop(4, body)

    def column(k, ref, at):
        def body(side):
            r["bcols"][pl.ds(k * 2 + side, 1), :] = jnp.sum(ref[at(side)].astype(f32), axis=0, keepdims=True)

        loop(2, body)

    context_back(7)
    loaded("c2", "lse2")
    statistics(r["lse2"], r["c2"])
    grads(
        lambda cols: [r["dhb"][:, cols]], [(7, side, lambda side=side: [r["c2"][side]]) for side in range(2)]
    )
    scatter.ready = 9
    scatter.run(1)
    loaded("q2", "ek", "ev")
    attend_back(r["q2"], r["ek"], r["ev"], 2, KEYS, False, scatter.turn(4))

    loaded("e", "a2")

    def frame_share(half, j):
        acc = None
        for mat, ref in ((5, r["ek"]), (6, r["ev"])):
            for side in range(2):
                more = dot(ref[side, half], flat_rows(r["part"].at[mat, side], j), NT)
                acc = more if acc is None else acc + more
        return acc

    def frame_trade(j):
        return remote(r["fsend"].at[j], r["frecv"].at[j], r["frame_send"].at[j], r["frame_recv"].at[j], mate)

    def frame_store(j):
        cols = pl.ds(pl.multiple_of(j * COLS, COLS), COLS)
        return pltpu.make_async_copy(r["fout"].at[lax.rem(j, 2)], r["frame_out"].at[:, cols], r["frame_out_sem"].at[j])

    def frame_far(j):
        r["fsend"][j] = frame_share(1 - c, j).astype(bf)
        frame_trade(j).start()

    def frame_near(j):
        @pl.when(j >= 2)
        def _():
            frame_store(j - 2).wait()

        frame_trade(j).wait_recv()
        r["fout"][lax.rem(j, 2)] = frame_share(c, j) + r["frecv"][j].astype(f32)
        frame_store(j).start()

    loop(4, frame_far)
    send_back(1, [(lambda side=side: r["q2"][side], 4, side) for side in range(2)])
    loop(4, frame_near)
    scatter.run(1)
    grads(
        lambda cols: [r["e"][n, :, cols] for n in range(2)],
        [(5 + i, side, lambda ref=ref, side=side: [ref[side, n] for n in range(2)])
         for i, ref in ((1, r["ev"]), (0, r["ek"])) for side in range(2)],
    )
    scatter.ready = 11
    scatter.run(1)
    column(2, r["q2"], lambda side: (side,))

    def value_column(side):
        total = sum(jnp.sum(r["ev"][side, n].astype(f32), axis=0, keepdims=True) for n in range(2))
        r["bcols"][pl.ds(6 + side, 1), :] = total

    loop(2, value_column)
    grads(lambda cols: [r["a2"][:, cols]], [(4, side, lambda side=side: [r["q2"][side]]) for side in range(2)])
    scatter.ready = 12
    loaded("h1")
    norm_back(1, 2, lambda rows, i: r["h"][rows, :], lambda rows, i: r["dh"][rows, :], 6)
    scatter.run(1)
    context_back(3)
    loaded("c1", "lse1")
    statistics(r["lse1"], r["c1"])
    grads(
        lambda cols: [r["dhb"][:, cols]], [(3, side, lambda side=side: [r["c1"][side]]) for side in range(2)]
    )
    scatter.ready = 13
    scatter.run(1)
    loaded("qkv")
    q_ref, k_ref, v_ref = (r["qkv"].at[i] for i in range(3))
    attend_back(q_ref, k_ref, v_ref, 1, L, True, lambda t: None)
    send_back(2, [(lambda i=i, side=side: r["qkv"][i, side, 0:L, :], i, side) for i in range(3) for side in range(2)])
    loaded("a1")
    grads(
        lambda cols: [r["left"][:, cols]],
        [(i, side, lambda i=i, side=side: [r["qkv"][i, side, 0:L, :]]) for i in (2, 1, 0) for side in range(2)],
    )
    scatter.ready = 16
    scatter.run(1)
    column(0, q_ref, lambda side: (side, slice(0, L)))
    column(1, v_ref, lambda side: (side, slice(0, L)))
    loaded("x")
    norm_back(2, 0, lambda rows, i: half_rows(r["x"], i), lambda rows, i: r["dh"][rows, :], None)
    own_rows = pl.ds(pl.multiple_of(c * HALF, HALF), HALF)
    input_copy = pltpu.make_async_copy(r["dh"].at[own_rows], r["input_out"], r["out_sem"].at[0])
    input_copy.start()

    sums = jnp.concatenate([jnp.sum(r["cols"][k * 8 : k * 8 + 8, :], axis=0, keepdims=True) for k in range(9)], axis=0)
    if fast:
        r["small"][...] = jnp.zeros(r["small"].shape, f32)
        for i in range(2 * levels):
            for xx in range(2):
                k = i * 2 + xx
                r["small"][k, 0:9, :] = sums[:, i * 128 : (i + 1) * 128]
                r["small"][k, 9:10, :] = r["bcols"][k : k + 1, 0:128]
                r["small"][k, 10:11, :] = r["bcols"][k : k + 1, 128:256]

        def small_copy(k, slot):
            i = lax.rem(me + k + 1, count)
            return remote(r["small"].at[i], r["smallgot"].at[slot], r["small_send"].at[k], r["small_recv"].at[slot],
                          peer(i))

        loop(count - 1, lambda k: small_copy(k, me).start())
        r["smallgot"][me] = r["small"][me]
    else:
        r["smallsum"][0:9, :] = sums
    while scatter.steps < MATS + 2:
        scatter.run(min(4, MATS + 2 - scatter.steps))
    owned_copy = pltpu.make_async_copy(r["own"], r["owned_out"], r["out_sem"].at[1])
    owned_copy.start()
    if fast:
        loop(count - 1, lambda k: small_copy(k, lax.rem(me + k + 1, count)).wait_recv())
        total = r["smallgot"][0]
        for k in range(1, 4 * levels):
            total = total + r["smallgot"][k]
        r["smallsum"][...] = total
        small_store = pltpu.make_async_copy(r["smallsum"], r["small_out"], r["out_sem"].at[2])
        small_store.start()
        loop(count - 1, lambda k: small_copy(k, me).wait_send())
        small_store.wait()
    else:
        first_store = pltpu.make_async_copy(r["smallsum"], r["cols_out"], r["out_sem"].at[2])
        second_store = pltpu.make_async_copy(r["bcols"], r["bcols_out"], r["out_sem"].at[3])
        first_store.start()
        second_store.start()
        first_store.wait()
        second_store.wait()
    for n in (1, 2):
        loop(4, lambda j: trade(n, j).wait_send())
    loop(4, lambda j: frame_trade(j).wait_send())
    for j in (2, 3):
        frame_store(j).wait()
    scatter.drain()
    input_copy.wait()
    owned_copy.wait()


def backward(kept, shards):
    levels, rows = shards // 2, D // shards
    fast = rows == 128
    f32, bf = jnp.float32, jnp.bfloat16
    sem = pltpu.SemaphoreType.DMA
    hbm = pl.BlockSpec(memory_space=pl.ANY)
    peers = shards * 2
    shapes = [((MATS, rows, COLS), f32), ((HALF, D), f32), ((KEYS, D), f32)]
    shapes += [((16, 128), f32)] if fast else [((16, D), f32), ((16, COLS), f32)]
    small = (peers, 16, 128) if fast else (1, 16, 128)
    vm = pltpu.VMEM
    scratch = [
        vm((MATS, 2, levels, 2, rows, COLS), bf), vm((MATS, rows, COLS), f32), vm((2, HALF, D), bf),
        vm((8, L, COLS), bf), vm((8, L, COLS), bf), vm((L, D), bf), vm((L, D), f32), vm((16, D), f32),
        vm((2, L, COLS), bf), vm((2, L, COLS), bf), vm((L, 128), f32), vm((2, 2, KEYS, COLS), bf),
        vm((2, 2, KEYS, COLS), bf), vm((2, KEYS, D), bf), vm((L, D), bf),
        vm((2, L, COLS), bf), vm((3, 2, 512, COLS), bf), vm((L, 128), f32), vm((2, HALF, D), bf),
        vm((L, D), f32), vm((L, D), bf), vm((2, L, COLS), bf), vm((16, L), f32),
        vm((KEYS, L), f32), vm((KEYS, L), f32), vm((KEYS, L), bf), vm((KEYS, L), bf),
        vm((2, 4, L, COLS), bf), vm((2, 4, L, COLS), bf), vm((4, KEYS, COLS), bf), vm((4, KEYS, COLS), bf),
        vm((2, KEYS, COLS), f32), vm((72, D), f32), vm((16, COLS), f32), vm(small, f32), vm(small, f32),
        vm((16, 128) if fast else (16, D), f32),
        sem((24,)), sem((3, 4)), sem((3, 4)), sem((4,)), sem((4,)), sem((4,)), sem((peers,)), sem((peers,)), sem((4,)),
    ]
    return pl.pallas_call(
        partial(backward_kernel, levels, fast),
        out_shape=[jax.ShapeDtypeStruct(s, t) for s, t in shapes],
        in_specs=[hbm] * len(BACKWARD_IN),
        out_specs=[hbm] * len(shapes),
        scratch_shapes=scratch + Scatter.buffers(levels, rows) + Scatter.semaphores(levels),
        compiler_params=pltpu.CompilerParams(
            collective_id=1, has_side_effects=True, vmem_limit_bytes=63 * 2**20
        ),
        name="backward",
    )(*[kept[n] for n in BACKWARD_IN])


def small_kernel(shards, every, scatter, src, out, own_sem, send_sem, recv_sem):
    dp, x, c = (lax.axis_index(a) for a in AXES)
    cores = 2 if every else 1
    count = shards * 2 * cores
    me = (dp * 2 + x) * cores + (c if every else 0)

    def peer(i):
        if every:
            return (i // 4, lax.rem(i // 2, 2), lax.rem(i, 2))
        return (i // 2, lax.rem(i, 2), c)

    bar = pltpu.get_barrier_semaphore()

    def greet(k, carry):
        pl.semaphore_signal(bar, inc=1, device_id=peer(lax.rem(me + k, count)), device_id_type=DT)
        return carry

    lax.fori_loop(1, count, greet, 0)
    pl.semaphore_wait(bar, count - 1)

    def copy(k):
        i = lax.rem(me + k, count)
        return pltpu.make_async_remote_copy(
            src.at[i] if scatter else src, out.at[me], send_sem.at[k], recv_sem.at[me],
            device_id=peer(i), device_id_type=DT,
        )

    def send(k, carry):
        copy(k).start()
        return carry

    own = pltpu.make_async_copy(src.at[me] if scatter else src, out.at[me], own_sem)
    own.start()
    lax.fori_loop(1, count, send, 0)
    own.wait()

    def finish(k, carry):
        i = lax.rem(me + k, count)
        pltpu.make_async_remote_copy(
            src.at[i] if scatter else src, out.at[i], send_sem.at[k], recv_sem.at[i],
            device_id=peer(i), device_id_type=DT,
        ).wait_recv()
        copy(k).wait_send()
        return carry

    lax.fori_loop(1, count, finish, 0)


def small_exchange(src, shards, every, scatter, call_id):
    count = shards * 2 * (2 if every else 1)
    shape = src.shape[1:] if scatter else src.shape
    sem = pltpu.SemaphoreType.DMA
    vm = pl.BlockSpec(memory_space=pltpu.VMEM)
    return pl.pallas_call(
        partial(small_kernel, shards, every, scatter),
        out_shape=jax.ShapeDtypeStruct((count, *shape), src.dtype),
        in_specs=[vm],
        out_specs=vm,
        scratch_shapes=[sem, sem((count,)), sem((count,))],
        compiler_params=pltpu.CompilerParams(collective_id=call_id, has_side_effects=True),
        name=f"small_exchange_{call_id}",
    )(src)


def adapt(weight, gradient, moment, second, token_total):
    scaled_grad = gradient / token_total
    new_moment = 0.5 * moment + 0.5 * scaled_grad
    new_second = 0.5 * second + 0.5 * scaled_grad * scaled_grad
    direction = new_moment / (jnp.sqrt(new_second) + 1e-06) + 0.01 * weight
    return (new_moment, new_second, direction)


def shards_fn(
    tokens, frames, cotangent, attention_weights, dense_weights, unit_bias, norm_bias,
    attention_mean, dense_mean, unit_mean, norm_mean,
    attention_square, dense_square, unit_square, norm_square,
):
    f32, bf = jnp.float32, jnp.bfloat16
    shards = lax.axis_size("dp")
    rows = D // shards
    c = lax.axis_index("core")
    unit_cols = unit_bias.shape[1]
    column_rows = (lax.axis_index("dp") * unit_cols + jnp.arange(unit_cols, dtype=jnp.int32)) // HD
    row_pick = (column_rows[:, None] == jnp.arange(8, dtype=jnp.int32)[None, :]).astype(f32)
    leader = ((lax.axis_index("side") == 0) & (c == 0)).astype(f32)

    def square_rows(attn_part, dense_part, unit_part, norm_part):
        unit_sums = jnp.sum(jnp.sum(unit_part * unit_part, axis=0)[:, None] * row_pick, axis=0)
        return jnp.concatenate(
            [
                jnp.sum(attn_part * attn_part, axis=(2, 3)).reshape(8),
                jnp.sum(dense_part * dense_part, axis=(1, 2, 3)),
                unit_sums,
                jnp.sum(norm_part * norm_part, axis=1) * leader,
            ]
        )

    own_attn = attention_weights.astype(f32)
    own_dense = dense_weights.astype(f32)
    own_unit = unit_bias.astype(f32)
    own_norm = norm_bias.astype(f32)

    if rows == 128:
        pack = jnp.concatenate([norm_bias.astype(f32), unit_bias.astype(f32).reshape(2, 128)])
        small = (jnp.pad(pack, ((0, 5), (0, 0))),)
    else:
        pack = jnp.concatenate([norm_bias.reshape(-1), unit_bias.reshape(-1)])
        pack = jnp.pad(pack, (0, 2048 - pack.shape[0])).reshape(16, 128)
        packs = small_exchange(pack, shards, False, False, 2).reshape(shards, 2, 2048)
        norm_rows = packs[:, 0, : 9 * rows].reshape(shards, 9, rows).transpose(1, 0, 2).reshape(9, D).astype(f32)
        unit_all = packs[:, :, 9 * rows : 9 * rows + 4 * unit_cols].reshape(shards, 2, 4, unit_cols)
        bias_rows = (
            unit_all.transpose(1, 2, 0, 3).reshape(2, 4, 8, HD).transpose(2, 0, 1, 3).reshape(16, COLS).astype(f32)
        )
        small = (jnp.pad(norm_rows, ((0, 7), (0, 0))), bias_rows)

    shard = jnp.concatenate(
        [attention_weights.reshape(8, rows, COLS), dense_weights.transpose(0, 2, 1, 3).reshape(8, rows, COLS)]
    )
    kept = forward(shard, tokens, jnp.pad(frames, ((0, KEYS - HALF_FRAMES), (0, 0))), cotangent, small, shards)
    layer_out = kept["layer_out"]
    owned, input_gradient, frame_gradient, *small_grads = backward(kept, shards)
    frame_gradient = frame_gradient[:HALF_FRAMES]
    attention_owned = owned[:8].reshape(2, 4, rows, COLS)
    dense_owned = owned[8:].reshape(2, 4, rows, COLS).transpose(0, 2, 1, 3)

    if rows == 128:
        norm_owned = small_grads[0][:9]
        unit_owned = small_grads[0][9:11].reshape(4, unit_cols)
    else:
        norm_parts = small_grads[0][:9].reshape(9, shards, rows).transpose(1, 0, 2).reshape(shards, 1, 9 * rows)
        unit_parts = small_grads[1].reshape(8, 2, 4, HD).transpose(1, 2, 0, 3).reshape(2, 4, shards, unit_cols)
        unit_parts = unit_parts.transpose(2, 0, 1, 3).reshape(shards, 2, 4 * unit_cols)
        small = jnp.concatenate([jnp.broadcast_to(norm_parts, (shards, 2, 9 * rows)), unit_parts], axis=2)
        small = jnp.pad(small, ((0, 0), (0, 0), (0, 2048 - small.shape[2]))).reshape(shards * 2, 16, 128)
        small = jnp.sum(small_exchange(small, shards, False, True, 13), axis=0).reshape(2048)
        norm_owned = small[: 9 * rows].reshape(9, rows)
        unit_owned = small[9 * rows : 9 * rows + 4 * unit_cols].reshape(4, unit_cols)

    token_total = float(tokens.shape[0] * shards * 4)
    attn_moment, attn_second, attn_dir = adapt(
        own_attn, attention_owned, attention_mean, attention_square, token_total
    )
    dense_moment, dense_second, dense_dir = adapt(
        own_dense, dense_owned, dense_mean, dense_square, token_total
    )
    unit_moment, unit_second, unit_dir = adapt(
        own_unit, unit_owned, unit_mean, unit_square, token_total
    )
    norm_moment, norm_second, norm_dir = adapt(
        own_norm, norm_owned, norm_mean, norm_square, token_total
    )
    sums = jnp.concatenate(
        [
            square_rows(own_attn, own_dense, own_unit, own_norm),
            square_rows(attn_dir, dense_dir, unit_dir, norm_dir),
        ]
    )
    sums = jnp.pad(sums, (0, 1024 - 54)).reshape(8, 128)
    sums = jnp.sum(small_exchange(sums, shards, True, False, 14), axis=0).reshape(1024)
    weight_norms = jnp.sqrt(sums[:27])
    step_norms = jnp.sqrt(sums[27:54])
    trust = weight_norms / step_norms
    attention_step = -learning_rate * trust[0:8].reshape(2, 4, 1, 1) * attn_dir
    dense_step = -learning_rate * trust[8:10].reshape(2, 1, 1, 1) * dense_dir
    unit_factor = jnp.sum(row_pick * trust[10:18][None, :], axis=1)
    unit_step = -learning_rate * unit_factor[None, :] * unit_dir
    norm_step = -learning_rate * trust[18:27][:, None] * norm_dir
    return (
        layer_out, input_gradient, frame_gradient,
        attention_owned, dense_owned, unit_owned, norm_owned,
        attn_moment, dense_moment, unit_moment, norm_moment,
        attn_second, dense_second, unit_second, norm_second,
        attention_step, dense_step, unit_step, norm_step,
        weight_norms, step_norms,
    )


def solution(mesh):
    shards = mesh.shape["dp"]
    inner = Mesh(mesh.devices.reshape(shards, 2, 2), AXES)
    tensor = ("side", "core")
    rows = P(("dp", *tensor), None)
    state = (P(None, None, "dp", tensor), P(None, "dp", None, tensor), P(tensor, "dp"), P(None, "dp"))
    return jax.shard_map(
        shards_fn,
        mesh=inner,
        in_specs=(rows, rows, rows) + state * 3,
        out_specs=(rows, rows, rows) + state * 4 + (P(), P()),
        check_vma=False,
    )
```

```python
from functools import partial
from typing import NamedTuple

import jax
import jax.numpy as jnp
from jax import lax
from jax.experimental import pallas as pl
from jax.experimental.pallas import tpu as pltpu
from jax.sharding import Mesh, PartitionSpec as P

D = 1024
HEADS = 16
HD = 64
L = 448
FRAMES = 1500
MATS = 16
COLS = 256

learning_rate = 0.3
DT = pl.DeviceIdType.MESH
AXES = ("dp", "side", "core")


def place():
    dp = lax.axis_index("dp")
    return dp // 2, lax.rem(dp, 2), lax.axis_index("side"), lax.axis_index("core")


def device(z, y, x, c):
    return (z * 2 + y, x, c)


def greet_neighbours(levels):
    z, y, x, c = place()
    bar = pltpu.get_barrier_semaphore()
    pl.semaphore_signal(bar, inc=1, device_id=device(z, y, 1 - x, c), device_id_type=DT)
    pl.semaphore_signal(bar, inc=1, device_id=device(z, 1 - y, x, c), device_id_type=DT)

    @pl.when(z > 0)
    def _():
        pl.semaphore_signal(bar, inc=1, device_id=device(z - 1, y, x, c), device_id_type=DT)

    @pl.when(z < levels - 1)
    def _():
        pl.semaphore_signal(bar, inc=1, device_id=device(z + 1, y, x, c), device_id_type=DT)

    pl.semaphore_wait(
        bar, 2 + jnp.where(z > 0, 1, 0) + jnp.where(z < levels - 1, 1, 0)
    )


class Gather:
    def __init__(self, levels, groups, shard, wide, sems):
        self.levels, self.groups, self.size = levels, groups, MATS // groups
        self.shard, self.wide = shard, wide
        self.own, self.zs, self.zr, self.xs, self.xr, self.ys, self.yr = sems
        self.at = place()
        self.done = 0
        self.total = (groups + LAG) * levels

    @staticmethod
    def semaphores(levels, groups):
        sem = pltpu.SemaphoreType.DMA
        one, pair = sem((groups, levels)), sem((groups, levels, 2))
        return [sem, pair, one, pair, pair, pair, pair]

    def block(self, g, xx, zz, yy):
        return self.wide.at[pl.ds(g * self.size, self.size), xx, zz, yy]

    def mine(self, g):
        return self.shard.at[pl.ds(g * self.size, self.size)]

    def z_copy(self, g, zz, up, own=False):
        z, y, x, c = self.at
        return pltpu.make_async_remote_copy(
            self.mine(g) if own else self.block(g, x, zz, y), self.block(g, x, zz, y), self.zs.at[g, zz, up],
            self.zr.at[g, zz], device_id=device(z + 1 if up else z - 1, y, x, c), device_id_type=DT,
        )

    def x_copy(self, g, zz, yy, own=False):
        z, y, x, c = self.at
        return pltpu.make_async_remote_copy(
            self.mine(g) if own else self.block(g, x, zz, yy), self.block(g, x, zz, yy), self.xs.at[g, zz, yy],
            self.xr.at[g, zz, yy], device_id=device(z, y, 1 - x, c), device_id_type=DT,
        )

    def y_copy(self, g, zz, xx, own=False):
        z, y, x, c = self.at
        return pltpu.make_async_remote_copy(
            self.mine(g) if own else self.block(g, xx, zz, y), self.block(g, xx, zz, y), self.ys.at[g, zz, xx],
            self.yr.at[g, zz, xx], device_id=device(z, 1 - y, x, c), device_id_type=DT,
        )

    def z_send(self, g):
        z = self.at[0]
        for up in (1, 0):
            @pl.when(z < self.levels - 1 if up else z > 0)
            def _():
                self.z_copy(g, z, up, True).start()

    def begin(self):
        z, y, x, c = self.at
        for g in range(min(Z_AHEAD, self.groups)):
            self.z_send(g)
        self.local = pltpu.make_async_copy(self.shard, self.wide.at[:, x, z, y], self.own)
        self.local.start()

    def first(self, g, d):
        z, y, x, c = self.at

        @pl.when(d == 0)
        def _():
            @pl.when(g + Z_AHEAD < self.groups)
            def _():
                self.z_send(g + Z_AHEAD)

            self.x_copy(g, z, y, True).start()
            self.y_copy(g, z, x, True).start()

        for up in (1, 0):
            zz = z - d if up else z + d

            @pl.when((d > 0) & (zz >= 0 if up else zz < self.levels))
            def _():
                self.z_copy(g, zz, up).wait_recv()

                @pl.when(z < self.levels - 1 if up else z > 0)
                def _():
                    self.z_copy(g, zz, up).start()

                self.x_copy(g, zz, y).start()
                self.y_copy(g, zz, x).start()

    def second(self, g, d):
        z, y, x, c = self.at
        for up in (1, 0):
            zz = z - d if up else z + d
            here = zz >= 0 if up else (zz < self.levels) & (d > 0)
            even = lax.rem(zz + self.levels, 2) == 0

            @pl.when(here & even)
            def _():
                self.x_copy(g, zz, y).wait_recv()
                self.y_copy(g, zz, 1 - x).start()

            @pl.when(here & jnp.logical_not(even))
            def _():
                self.y_copy(g, zz, x).wait_recv()
                self.x_copy(g, zz, 1 - y).start()

    def tick(self, t):
        g, d = t // self.levels, lax.rem(t, self.levels)

        @pl.when((g >= LAG) & (g < self.groups + LAG))
        def _():
            self.second(g - LAG, d)

        @pl.when(g < self.groups)
        def _():
            self.first(g, d)

    def run(self, count):
        count = max(0, min(count, self.total - self.done))
        start = self.done
        self.done += count
        if count:
            loop(count, lambda i: self.tick(start + i))

    def turn(self, count):
        start = self.done
        self.done = min(self.total, self.done + count)
        return lambda i: self.tick(start + i)

    def need(self, mat):
        g = mat // self.size
        self.run((g + 1 + LAG) * self.levels - self.done)
        z, y, x, c = self.at

        def body(zz):
            @pl.when(lax.rem(zz, 2) == 0)
            def _():
                self.y_copy(g, zz, x).wait_recv()
                self.y_copy(g, zz, 1 - x).wait_recv()

            @pl.when(lax.rem(zz, 2) == 1)
            def _():
                self.x_copy(g, zz, y).wait_recv()
                self.x_copy(g, zz, 1 - y).wait_recv()

        if mat % self.size == 0:
            loop(self.levels, body)
        if mat == 0:
            self.local.wait()

    def drain(self):
        z, y, x, c = self.at

        def group(g):
            def sent(zz):
                self.x_copy(g, zz, y).wait_send()
                self.y_copy(g, zz, x).wait_send()

                @pl.when(lax.rem(zz, 2) == 0)
                def _():
                    self.y_copy(g, zz, 1 - x).wait_send()

                @pl.when(lax.rem(zz, 2) == 1)
                def _():
                    self.x_copy(g, zz, 1 - y).wait_send()

            loop(self.levels, sent)

            def relayed(zz):
                @pl.when((z < self.levels - 1) & (zz <= z))
                def _():
                    self.z_copy(g, zz, 1).wait_send()

                @pl.when((z > 0) & (zz >= z))
                def _():
                    self.z_copy(g, zz, 0).wait_send()

            loop(self.levels, relayed)

        loop(self.groups, group)


LAG = 2
Z_AHEAD = 1
GROUPS = 8
HALF = L // 2
KEYS = 768
HALF_FRAMES = FRAMES // 2
BLOCK = 32
SOFT_TURNS = 14
NORM_TURNS = 7
BACK_TURNS = 12


def dot(a, b, dims):
    return lax.dot_general(a, b, (dims, ((), ())), preferred_element_type=jnp.float32)


NN, NT, TN = ((1,), (0,)), ((1,), (1,)), ((0,), (0,))


def flat_panel(ref, mat, side):
    return ref[mat, side].reshape(D, COLS)


def flat_rows(panel, j):
    per = COLS // (2 * panel.shape[2])
    return panel[pl.ds(j * per, per)].reshape(COLS, COLS)


def rows_loop(count, body, turns=1):
    def run(k, carry):
        for u in range(turns):
            i = k * turns + u
            body(pl.ds(pl.multiple_of(i * BLOCK, BLOCK), BLOCK), i)
        return carry

    lax.fori_loop(0, count // (BLOCK * turns), run, 0)


def loop(count, body):
    def run(i, carry):
        body(i)
        return carry

    lax.fori_loop(0, count, run, 0)


def normed_block(values):
    centre = values - jnp.mean(values, axis=-1, keepdims=True)
    spread = jnp.mean(centre * centre, axis=-1, keepdims=True)
    scaled = lax.rsqrt(spread + 1e-05)
    return centre * scaled, scaled


def panels_row(ref, rows):
    return jnp.concatenate([ref[j, rows, :].astype(jnp.float32) for j in range(4)], axis=1)


def forward_kernel(levels, groups, fast, *refs):
    f32, bf = jnp.float32, jnp.bfloat16
    width = len(ForwardRefs._fields)
    r = ForwardRefs(*refs[:width])
    gather = Gather(levels, groups, r.shard, r.wide, refs[width:])
    z, y, x, c = place()
    dp = z * 2 + y
    mate = (dp, x, 1 - c)
    count = levels * 4
    me = dp * 2 + x

    def peer(i):
        return (i // 2, lax.rem(i, 2), c)

    bar = pltpu.get_barrier_semaphore()
    loop(count - 1, lambda k: pl.semaphore_signal(
        bar, inc=1, device_id=peer(lax.rem(me + k + 1, count)), device_id_type=DT))
    pl.semaphore_signal(bar, inc=1, device_id=mate, device_id_type=DT)
    pl.semaphore_wait(bar, count)

    def remote(src, dst, send, recv, dev):
        return pltpu.make_async_remote_copy(src, dst, send, recv, device_id=dev, device_id_type=DT)

    inputs = ((r.tokens, r.x), (r.frames, r.e), (r.cotangent, r.dy))

    def swap(k, slot):
        src, dst = inputs[k]
        return remote(src, dst.at[slot], r.swap_send.at[k], r.swap_recv.at[k], mate)

    def local(k):
        src, dst = inputs[k]
        return pltpu.make_async_copy(src, dst.at[c], r.in_sem.at[k])

    if fast:
        def pack_copy(k, slot):
            return remote(r.pack, r.packs.at[slot], r.pack_send.at[k], r.pack_recv.at[slot],
                          peer(lax.rem(me + k + 1, count)))

        loop(count - 1, lambda k: pack_copy(k, me).start())
        own_pack = pltpu.make_async_copy(r.pack, r.packs.at[me], r.in_sem.at[3])
        own_pack.start()
    swap(0, c).start()
    local(0).start()
    gather.begin()
    gather.run(1)
    for k in (1, 2):
        swap(k, c).start()
        local(k).start()

    def arrived(k):
        local(k).wait()
        swap(k, 1 - c).wait_recv()

    outs = []

    def emit(out, scratch):
        outs.append(pltpu.make_async_copy(scratch, out, r.out_sem.at[len(outs)]))
        outs[-1].start()

    if fast:
        own_pack.wait()
        loop(count - 1, lambda k: pack_copy(k, lax.rem(me + k + 1, count)).wait_recv())
        for i in range(2 * levels):
            for xx in range(2):
                block = r.packs[i * 2 + xx]
                if xx == 0:
                    r.norm[:, i * 128 : (i + 1) * 128] = block
                r.bias[i * 2 + xx : i * 2 + xx + 1, 0:128] = block[9:10]
                r.bias[i * 2 + xx : i * 2 + xx + 1, 128:256] = block[10:11]
    else:
        r.norm[...] = r.norm_in[...]
        r.bias[...] = r.bias_in[...]
    emit(r.norm_out, r.norm)

    def norm_row(k):
        return r.norm[k : k + 1, :]

    def bias_row(k, side):
        return r.bias[pl.ds(k * 2 + side, 1), :]

    key = lax.broadcasted_iota(jnp.int32, (1, 2 * KEYS), 1)
    real = lax.rem(key, KEYS) < HALF_FRAMES
    r.padrow[0:1, :] = jnp.where(real, 0.0, -1e30).astype(f32)
    for i in range(3):
        for side in range(2):
            r.qkv[i, side, L:512, :] = jnp.zeros((512 - L, COLS), bf)

    arrived(0)

    def ln1(half):
        def body(rows, i):
            normed, _ = normed_block(r.x[half, rows, :].astype(f32))
            out = (normed * norm_row(0) + norm_row(1)).astype(bf)
            r.a1[pl.ds(pl.multiple_of(half * HALF + i * BLOCK, BLOCK), BLOCK), :] = out

        rows_loop(HALF, body, NORM_TURNS if NORM_TURNS in (1, 7) else 1)

    ln1(0)
    ln1(1)
    emit(r.a1_out, r.a1)
    emit(r.x_out, r.x)

    def project_one(i, side):
        bias = bias_row(0, side) if i == 0 else bias_row(1, side)
        acc = dot(r.a1[...], flat_panel(r.wide, i, side), NN)
        if i != 1:
            acc = acc + bias
        r.qkv[i, side, 0:L, :] = acc.astype(bf)

    for i in range(3):
        gather.need(i)
        loop(2, lambda side: project_one(i, side))
    emit(r.qkv_out, r.qkv)

    lane = lax.broadcasted_iota(jnp.int32, (1, 128), 1)
    low = lane < HD

    def attend(query, key_parts, values, width, causal, lse, ctx, per_head, tick):
        def body(t):
            side, half = t // 2, lax.rem(t, 2)
            lanes = pl.ds(pl.multiple_of(half * 128, 128), 128)
            q = query(side, lanes)
            found = []
            for sub in range(2):
                mine = low if sub == 0 else jnp.logical_not(low)
                qh = jnp.where(mine, q.astype(f32) * 0.125, 0.0).astype(bf)
                for n, part in enumerate(key_parts(side, lanes)):
                    r.s[:, n * width : (n + 1) * width] = dot(qh, part, NT)
                total = width * len(key_parts(side, lanes))

                def rows_body(rows, i):
                    s = r.s[rows, 0:total]
                    if causal:
                        row = i * BLOCK + lax.broadcasted_iota(jnp.int32, (BLOCK, total), 0)
                        col = lax.broadcasted_iota(jnp.int32, (BLOCK, total), 1)
                        s = jnp.where(col <= row, s, -1e30)
                    else:
                        s = s + r.padrow[0:1, 0:total]
                    top = jnp.max(s, axis=-1, keepdims=True)
                    e = jnp.exp(s - top)
                    weight = jnp.sum(e, axis=-1, keepdims=True)
                    r.p[rows, 0:total] = (e * (1.0 / weight)).astype(bf)
                    lse[rows, :] = jnp.where(lane == t * 2 + sub, top + jnp.log(weight), lse[rows, :])

                rows_loop(L, rows_body, SOFT_TURNS)
                for i in range(per_head):
                    tick((t * 2 + sub) * per_head + i)
                acc = None
                for n, part in enumerate(values(side, lanes)):
                    more = dot(r.p[:, n * width : (n + 1) * width], part, NN)
                    acc = more if acc is None else acc + more
                found.append(acc)
            ctx[side, :, lanes] = jnp.where(low, found[0], found[1]).astype(bf)

        loop(4, body)

    attend(
        lambda side, lanes: r.qkv[0, side, 0:L, lanes],
        lambda side, lanes: [r.qkv[1, side, :, lanes]],
        lambda side, lanes: [r.qkv[2, side, :, lanes]],
        512, True, r.lse1, r.c1, 1, gather.turn(8),
    )
    emit(r.lse1_out, r.lse1)
    emit(r.c1_out, r.c1)

    def collect(n, ctx, mat):
        def body(j):
            rows = pl.ds(pl.multiple_of(j * COLS, COLS), COLS)
            acc = None
            for side in range(2):
                more = dot(ctx[side], flat_rows(r.wide.at[mat, side], j), NT)
                acc = more if acc is None else acc + more
            r.part[n, j] = acc.astype(bf)
            trade(n, j).start()

        loop(4, body)

    def trade(n, j):
        return remote(r.part.at[n, j], r.got.at[n, j], r.part_send.at[n, j], r.part_recv.at[n, j], mate)

    def traded(n):
        loop(4, lambda j: trade(n, j).wait_recv())

    def residual(n, base, bias_k, out, gain_k, normed_out):
        def body(rows, i):
            v = base(rows, i) + norm_row(bias_k) + (panels_row(r.part.at[n], rows) + panels_row(r.got.at[n], rows))
            out[rows, :] = v
            normed, _ = normed_block(v)
            normed_out[rows, :] = (normed * norm_row(gain_k) + norm_row(gain_k + 1)).astype(bf)

        rows_loop(L, body, NORM_TURNS)

    def x_rows(rows, i):
        half = i // (HALF // BLOCK)
        inner = pl.ds(pl.multiple_of((i - half * (HALF // BLOCK)) * BLOCK, BLOCK), BLOCK)
        return r.x[half, inner, :].astype(f32)

    gather.need(3)
    collect(0, r.c1, 3)
    gather.run(1)
    traded(0)
    residual(0, x_rows, 6, r.h1, 2, r.a2)
    emit(r.h1_out, r.h1)
    emit(r.a2_out, r.a2)

    gather.need(4)

    def query_two(side):
        acc = dot(r.a2[...], flat_panel(r.wide, 4, side), NN) + bias_row(2, side)
        r.q2[side] = acc.astype(bf)

    loop(2, query_two)
    emit(r.q2_out, r.q2)
    arrived(1)
    emit(r.e_out, r.e)

    gather.need(5)

    def frame_keys(t):
        side, half = t // 2, lax.rem(t, 2)
        r.ek[side, half] = dot(r.e[half], flat_panel(r.wide, 5, side), NN).astype(bf)

    loop(4, frame_keys)
    emit(r.ek_out, r.ek)
    gather.need(6)

    def frame_values(t):
        side, half = t // 2, lax.rem(t, 2)
        acc = dot(r.e[half], flat_panel(r.wide, 6, side), NN) + bias_row(3, side)
        r.ev[side, half] = acc.astype(bf)

    loop(4, frame_values)
    emit(r.ev_out, r.ev)
    attend(
        lambda side, lanes: r.q2[side, :, lanes],
        lambda side, lanes: [r.ek[side, half, :, lanes] for half in range(2)],
        lambda side, lanes: [r.ev[side, half, :, lanes] for half in range(2)],
        KEYS, False, r.lse2, r.c2, 2, gather.turn(16),
    )
    emit(r.lse2_out, r.lse2)
    emit(r.c2_out, r.c2)
    gather.need(7)
    collect(1, r.c2, 7)
    gather.run(1)
    traded(1)
    residual(1, lambda rows, i: r.h1[rows, :], 7, r.h2, 4, r.a3)
    emit(r.h2_out, r.h2)
    emit(r.a3_out, r.a3)
    arrived(2)
    emit(r.dy_out, r.dy)

    def hidden(t):
        m, side = t // 2, lax.rem(t, 2)
        u = dot(r.a3[...], flat_panel(r.wide, 8 + m, side), NN) + bias_row(4 + m, side)
        half = 0.5 * (1.0 + lax.erf(u * 0.7071067811865476))
        r.z[t] = (u * half).astype(bf)
        r.slope[t] = (half + u * jnp.exp(-0.5 * u * u) * 0.3989422804014327).astype(bf)

    def result(k):
        def tile(j):
            cols = pl.ds(pl.multiple_of(j * COLS, COLS), COLS)
            acc = None
            for t in range(4 * k, 4 * k + 4):
                more = dot(r.z[t], flat_rows(r.wide.at[12 + t // 2, t % 2], j), NT)
                acc = more if acc is None else acc + more
            if k == 0:
                r.acc[:, cols] = acc
            else:
                r.acc[:, cols] += acc

        loop(4, tile)

    for m in range(4):
        gather.need(8 + m)
        loop(2, lambda side: hidden(2 * m + side))
    emit(r.z_out, r.z)
    emit(r.slope_out, r.slope)
    for k in range(2):
        gather.need(12 + 2 * k)
        gather.need(13 + 2 * k)
        result(k)

    emit(r.wide_out, r.wide)

    for half in range(2):
        @pl.when(c == half)
        def _():
            far = (1 - half) * HALF

            def body(j):
                cols = pl.ds(pl.multiple_of(j * COLS, COLS), COLS)
                r.part[2, j, 0:HALF, :] = r.acc[far : far + HALF, cols].astype(bf)

            loop(4, body)

    last = remote(
        r.part.at[2, :, 0:HALF], r.got.at[2, :, 0:HALF], r.part_send.at[2, 0], r.part_recv.at[2, 0], mate
    )
    last.start()
    last.wait_recv()

    def finish(rows, i):
        here = pl.ds(pl.multiple_of(c * HALF + i * BLOCK, BLOCK), BLOCK)
        own = r.acc[here, :].astype(bf).astype(f32)
        v = r.h2[here, :] + norm_row(8) + (own + panels_row(r.got.at[2], rows))
        r.outrows[rows, :] = v.astype(bf)

    rows_loop(HALF, finish)
    emit(r.layer_out, r.outrows)

    for k in range(3):
        swap(k, c).wait_send()
    if fast:
        loop(count - 1, lambda k: pack_copy(k, me).wait_send())
    for n in range(2):
        loop(4, lambda j: trade(n, j).wait_send())
    last.wait_send()
    gather.drain()
    for copy in outs:
        copy.wait()


class ForwardRefs(NamedTuple):
    shard: object
    tokens: object
    frames: object
    cotangent: object
    pack: object
    norm_in: object
    bias_in: object
    layer_out: object
    norm_out: object
    a1_out: object
    x_out: object
    qkv_out: object
    lse1_out: object
    c1_out: object
    h1_out: object
    a2_out: object
    q2_out: object
    e_out: object
    ek_out: object
    ev_out: object
    lse2_out: object
    c2_out: object
    h2_out: object
    a3_out: object
    dy_out: object
    z_out: object
    slope_out: object
    wide_out: object
    wide: object
    x: object
    dy: object
    e: object
    norm: object
    bias: object
    a1: object
    a2: object
    a3: object
    h1: object
    h2: object
    qkv: object
    c1: object
    q2: object
    c2: object
    ek: object
    ev: object
    lse1: object
    lse2: object
    z: object
    slope: object
    s: object
    p: object
    acc: object
    part: object
    got: object
    packs: object
    padrow: object
    outrows: object
    in_sem: object
    swap_send: object
    swap_recv: object
    part_send: object
    part_recv: object
    pack_send: object
    pack_recv: object
    out_sem: object


class Kept(NamedTuple):
    layer_out: object
    norm: object
    a1: object
    x: object
    qkv: object
    lse1: object
    c1: object
    h1: object
    a2: object
    q2: object
    e: object
    ek: object
    ev: object
    lse2: object
    c2: object
    h2: object
    a3: object
    dy: object
    z: object
    slope: object
    wide: object


def forward(shard, tokens, frames, cotangent, small, shards):
    levels, rows = shards // 2, D // shards
    groups = GROUPS if levels <= 4 else 4
    fast = rows == 128
    f32, bf = jnp.float32, jnp.bfloat16
    sem = pltpu.SemaphoreType.DMA
    vm, hbm = pl.BlockSpec(memory_space=pltpu.VMEM), pl.BlockSpec(memory_space=pl.ANY)
    wide = (MATS, 2, levels, 2, rows, COLS)
    shapes = [
        ((HALF, D), bf),
        ((16, D), f32),
        ((L, D), bf),
        ((2, HALF, D), bf),
        ((3, 2, 512, COLS), bf),
        ((L, 128), f32),
        ((2, L, COLS), bf),
        ((L, D), f32),
        ((L, D), bf),
        ((2, L, COLS), bf),
        ((2, KEYS, D), bf),
        ((2, 2, KEYS, COLS), bf),
        ((2, 2, KEYS, COLS), bf),
        ((L, 128), f32),
        ((2, L, COLS), bf),
        ((L, D), f32),
        ((L, D), bf),
        ((2, HALF, D), bf),
        ((8, L, COLS), bf),
        ((8, L, COLS), bf),
        (wide, bf),
    ]
    peers = shards * 2
    scratch = [
        pltpu.VMEM(wide, bf), pltpu.VMEM((2, HALF, D), bf), pltpu.VMEM((2, HALF, D), bf), pltpu.VMEM((2, KEYS, D), bf),
        pltpu.VMEM((16, D), f32), pltpu.VMEM((16, COLS), f32),
        pltpu.VMEM((L, D), bf), pltpu.VMEM((L, D), bf), pltpu.VMEM((L, D), bf),
        pltpu.VMEM((L, D), f32), pltpu.VMEM((L, D), f32),
        pltpu.VMEM((3, 2, 512, COLS), bf), pltpu.VMEM((2, L, COLS), bf), pltpu.VMEM((2, L, COLS), bf),
        pltpu.VMEM((2, L, COLS), bf), pltpu.VMEM((2, 2, KEYS, COLS), bf), pltpu.VMEM((2, 2, KEYS, COLS), bf),
        pltpu.VMEM((L, 128), f32), pltpu.VMEM((L, 128), f32),
        pltpu.VMEM((8, L, COLS), bf), pltpu.VMEM((8, L, COLS), bf),
        pltpu.VMEM((L, 2 * KEYS), f32), pltpu.VMEM((L, 2 * KEYS), bf), pltpu.VMEM((L, D), f32),
        pltpu.VMEM((3, 4, L, COLS), bf), pltpu.VMEM((3, 4, L, COLS), bf),
        pltpu.VMEM((peers, 16, 128) if fast else (1, 16, 128), f32), pltpu.VMEM((8, 2 * KEYS), f32),
        pltpu.VMEM((HALF, D), bf),
        sem((4,)), sem((3,)), sem((3,)), sem((3, 4)), sem((3, 4)), sem((peers,)), sem((peers,)),
        sem((len(shapes),)),
    ]
    outs = pl.pallas_call(
        partial(forward_kernel, levels, groups, fast),
        out_shape=[jax.ShapeDtypeStruct(s, t) for s, t in shapes],
        in_specs=[vm, hbm, hbm, hbm, vm, vm, vm],
        out_specs=[hbm] * len(shapes),
        scratch_shapes=scratch + Gather.semaphores(levels, groups),
        compiler_params=pltpu.CompilerParams(
            collective_id=0, has_side_effects=True, vmem_limit_bytes=63 * 2**20
        ),
        name="forward",
    )(shard, tokens, frames, cotangent, *small)
    return Kept(*outs)


RING = 4


class Scatter:
    def __init__(self, levels, part, own, bufs, sems):
        self.levels, self.part, self.own = levels, part, own
        self.one_y, self.one_x, self.two_x, self.two_y, self.line = bufs
        self.s1, self.r1, self.s2, self.r2, self.s3, self.r3 = sems
        self.at = place()
        self.sent = self.steps = self.ready = 0

    @staticmethod
    def buffers(levels, rows):
        bf, half = jnp.bfloat16, levels // 2
        return [
            pltpu.VMEM((RING, 2, half, rows, COLS), bf), pltpu.VMEM((RING, half, 2, rows, COLS), bf),
            pltpu.VMEM((RING, half, rows, COLS), bf), pltpu.VMEM((RING, half, rows, COLS), bf),
            pltpu.VMEM((RING, levels, rows, COLS), bf),
        ]

    @staticmethod
    def semaphores(levels):
        sem = pltpu.SemaphoreType.DMA
        two = sem((MATS, 2))
        many = sem((MATS, levels))
        return [two, two, two, two, many, many]

    def to_x(self, src, dst, send, recv):
        z, y, x, c = self.at
        return pltpu.make_async_remote_copy(src, dst, send, recv, device_id=device(z, y, 1 - x, c), device_id_type=DT)

    def to_y(self, src, dst, send, recv):
        z, y, x, c = self.at
        return pltpu.make_async_remote_copy(src, dst, send, recv, device_id=device(z, 1 - y, x, c), device_id_type=DT)

    def first(self, g):
        z, y, x, c = self.at
        m, slot = MATS - 1 - g, lax.rem(g, RING)
        return (
            self.to_y(self.part.at[m, :, :, 0, 1 - y], self.one_y.at[slot], self.s1.at[g, 0], self.r1.at[g, 0]),
            self.to_x(self.part.at[m, 1 - x, :, 1], self.one_x.at[slot], self.s1.at[g, 1], self.r1.at[g, 1]),
        )

    def second(self, g):
        z, y, x, c = self.at
        m, slot = MATS - 1 - g, lax.rem(g, RING)
        return (
            self.to_x(self.part.at[m, 1 - x, :, 0, y], self.two_x.at[slot], self.s2.at[g, 0], self.r2.at[g, 0]),
            self.to_y(self.part.at[m, x, :, 1, 1 - y], self.two_y.at[slot], self.s2.at[g, 1], self.r2.at[g, 1]),
        )

    def third(self, g, zz, k):
        z, y, x, c = self.at
        return pltpu.make_async_remote_copy(
            self.part.at[MATS - 1 - g, x, zz // 2, lax.rem(zz, 2), y], self.line.at[lax.rem(g, RING), k],
            self.s3.at[g, zz], self.r3.at[g, k], device_id=device(zz, y, x, c), device_id_type=DT,
        )

    def send(self, count):
        def body(i):
            for copy in self.first(i):
                copy.start()

        start = self.sent
        self.sent += count
        loop(count, lambda i: body(start + i))

    def add(self, at, got):
        self.part[at] = (self.part[at].astype(jnp.float32) + got.astype(jnp.float32)).astype(jnp.bfloat16)

    def step_a(self, g):
        z, y, x, c = self.at
        m, slot = MATS - 1 - g, lax.rem(g, RING)
        along_y, along_x = self.first(g)
        then_x, then_y = self.second(g)
        along_y.wait_recv()
        for k in range(2):
            loop(self.levels // 2, lambda h: self.add((m, k, h, 0, y), self.one_y[slot, k, h]))
        then_x.start()
        along_x.wait_recv()
        for k in range(2):
            loop(self.levels // 2, lambda h: self.add((m, x, h, 1, k), self.one_x[slot, h, k]))
        then_y.start()

    def step_b(self, g):
        z, y, x, c = self.at
        m, slot = MATS - 1 - g, lax.rem(g, RING)
        then_x, then_y = self.second(g)
        then_x.wait_recv()
        loop(self.levels // 2, lambda h: self.add((m, x, h, 0, y), self.two_x[slot, h]))
        then_y.wait_recv()
        loop(self.levels // 2, lambda h: self.add((m, x, h, 1, y), self.two_y[slot, h]))
        loop(self.levels - 1, lambda k: self.third(g, lax.rem(z + k + 1, self.levels), z).start())

    def step_c(self, g):
        z, y, x, c = self.at
        m = MATS - 1 - g
        loop(self.levels - 1, lambda k: self.third(g, z, lax.rem(z + k + 1, self.levels)).wait_recv())
        self.own[m] = self.part[m, x, z // 2, lax.rem(z, 2), y].astype(jnp.float32)

        def body(k):
            @pl.when(k != z)
            def _():
                self.own[m] += self.line[lax.rem(g, RING), k].astype(jnp.float32)

        loop(self.levels, body)

    def step(self, t):
        @pl.when(t < MATS)
        def _():
            self.step_a(t)

        @pl.when((t >= 1) & (t <= MATS))
        def _():
            self.step_b(t - 1)

        @pl.when(t >= 2)
        def _():
            self.step_c(t - 2)

    def turn(self, count):
        start, first = self.steps, self.sent
        self.steps += count
        self.sent = max(first, min(MATS, self.steps + RING - 2))
        assert self.sent <= self.ready

        def body(i):
            t = start + i
            self.step(t)
            g = t + RING - 2

            @pl.when((g >= first) & (g < MATS))
            def _():
                for copy in self.first(g):
                    copy.start()

        return body

    def run(self, count):
        loop(count, self.turn(count))

    def drain(self):
        z, y, x, c = self.at

        def body(g):
            for copy in (*self.first(g), *self.second(g)):
                copy.wait_send()
            loop(self.levels - 1, lambda k: self.third(g, lax.rem(z + k + 1, self.levels), z).wait_send())

        loop(MATS, body)


class BackwardIn(NamedTuple):
    dy: object
    wide: object
    slope: object
    z: object
    a3: object
    h2: object
    norm: object
    c2: object
    q2: object
    lse2: object
    ek: object
    ev: object
    e: object
    a2: object
    h1: object
    c1: object
    qkv: object
    lse1: object
    a1: object
    x: object


class BackwardRefs(NamedTuple):
    owned_out: object
    input_out: object
    frame_out: object
    small_out: object
    bcols_out: object
    part: object
    own: object
    dy: object
    slope: object
    z: object
    left: object
    h: object
    norm: object
    c2: object
    q2: object
    lse2: object
    ek: object
    ev: object
    e: object
    a2: object
    c1: object
    qkv: object
    lse1: object
    x: object
    dh: object
    dhb: object
    dc: object
    stat: object
    s: object
    dp: object
    p: object
    ds: object
    mine: object
    got: object
    fsend: object
    frecv: object
    fout: object
    cols: object
    bcols: object
    small: object
    smallgot: object
    smallsum: object
    in_sem: object
    trade_send: object
    trade_recv: object
    frame_send: object
    frame_recv: object
    frame_out_sem: object
    small_send: object
    small_recv: object
    out_sem: object


def backward_kernel(levels, fast, *refs):
    f32, bf = jnp.float32, jnp.bfloat16
    at, width = len(BackwardIn._fields), len(BackwardRefs._fields)
    given = BackwardIn(*refs[:at])
    r = BackwardRefs(*refs[at : at + width])
    rest = refs[at + width :]
    scatter = Scatter(levels, r.part, r.own, rest[:5], rest[5:])
    z, y, x, c = place()
    dp = z * 2 + y
    mate = (dp, x, 1 - c)
    count = levels * 4
    me = dp * 2 + x
    rows_of = D // (levels * 2)
    per = COLS // (2 * rows_of)

    def peer(i):
        return (i // 2, lax.rem(i, 2), c)

    loads = []

    def load(src, dst):
        loads.append(pltpu.make_async_copy(src, dst, r.in_sem.at[len(loads)]))
        loads[-1].start()
        return loads[-1]

    def loaded(*which):
        for copy in which:
            copy.wait()

    get_dy = load(given.dy, r.dy)
    get_w2 = load(given.wide.at[12:16], r.part.at[12:16])
    get_slope = load(given.slope, r.slope)
    get_z = load(given.z, r.z)
    get_w1 = load(given.wide.at[8:12], r.part.at[8:12])
    get_a3 = load(given.a3, r.left)
    get_h2 = load(given.h2, r.h)
    get_w0 = load(given.wide.at[0:8], r.part.at[0:8])
    get_norm = load(given.norm, r.norm)
    get_c2 = load(given.c2, r.c2)
    get_q2 = load(given.q2, r.q2)
    get_lse2 = load(given.lse2, r.lse2)
    get_ek = load(given.ek, r.ek)
    get_ev = load(given.ev, r.ev)
    get_e = load(given.e, r.e)
    get_a2 = load(given.a2, r.a2)
    get_c1 = load(given.c1, r.c1)
    get_qkv = load(given.qkv, r.qkv)
    get_lse1 = load(given.lse1, r.lse1)
    get_x = load(given.x, r.x)

    bar = pltpu.get_barrier_semaphore()
    loop(count - 1, lambda k: pl.semaphore_signal(
        bar, inc=1, device_id=peer(lax.rem(me + k + 1, count)), device_id_type=DT))
    pl.semaphore_signal(bar, inc=1, device_id=mate, device_id_type=DT)
    pl.semaphore_wait(bar, count)

    def remote(src, dst, send, recv, dev):
        return pltpu.make_async_remote_copy(src, dst, send, recv, device_id=dev, device_id_type=DT)

    def trade(n, j):
        return remote(r.mine.at[n % 2, j], r.got.at[n % 2, j], r.trade_send.at[n, j],
                      r.trade_recv.at[n, j], mate)

    def panel(mat, side):
        return r.part[mat, side].reshape(D, COLS)

    def part_rows(mat, side, j):
        if per == 1:
            return r.part[mat, side, j // 2, lax.rem(j, 2)].reshape(COLS, COLS)
        return r.part[mat, side, pl.ds(j * (per // 2), per // 2)].reshape(COLS, COLS)

    def grads(lefts, items):
        def body(j):
            cols = pl.ds(pl.multiple_of(j * COLS, COLS), COLS)
            turned = [v.T for v in lefts(cols)]
            for mat, side, rights in items:
                acc = None
                for t, right in zip(turned, rights()):
                    more = dot(t, right, NN)
                    acc = more if acc is None else acc + more
                if per == 1:
                    r.part[mat, side, j // 2, lax.rem(j, 2)] = acc.astype(bf).reshape(2, rows_of, COLS)
                else:
                    blocks = pl.ds(j * (per // 2), per // 2)
                    r.part[mat, side, blocks] = acc.astype(bf).reshape(per // 2, 2, 2, rows_of, COLS)

        loop(4, body)

    def send_back(n, items):
        if n >= 2:
            loop(4, lambda j: trade(n - 2, j).wait_send())

        def body(j):
            acc = None
            for value, mat, side in items:
                more = dot(value(), part_rows(mat, side, j), NT)
                acc = more if acc is None else acc + more
            r.mine[n % 2, j] = acc.astype(bf)
            trade(n, j).start()

        loop(4, body)

    def fold(v):
        return jnp.sum(v.reshape(BLOCK // 8, 8, D), axis=0)

    def norm_row(k):
        return r.norm[k : k + 1, :]

    def grow(k, v):
        r.cols[k * 8 : (k + 1) * 8, :] += fold(v)

    def half_rows(ref, i):
        half = i // (HALF // BLOCK)
        inner = pl.ds(pl.multiple_of((i - half * (HALF // BLOCK)) * BLOCK, BLOCK), BLOCK)
        return ref[half, inner, :].astype(f32)

    def norm_back(n, k, base, incoming, sum_k):
        loop(4, lambda j: trade(n, j).wait_recv())

        def body(rows, i):
            normed, scaled = normed_block(base(rows, i))
            dn = panels_row(r.mine.at[n % 2], rows) + panels_row(r.got.at[n % 2], rows)
            inner = dn * norm_row(k)
            back = scaled * (
                inner - jnp.mean(inner, axis=-1, keepdims=True)
                - normed * jnp.mean(inner * normed, axis=-1, keepdims=True)
            )
            came = incoming(rows, i)
            out = came + back
            r.dh[rows, :] = out
            grow(k, dn * normed)
            grow(k + 1, dn)
            if sum_k is not None:
                r.dhb[rows, :] = out.astype(bf)
                grow(sum_k, out)
            if n == 0:
                grow(8, came)

        rows_loop(L, body, NORM_TURNS)

    r.cols[...] = jnp.zeros((72, D), f32)
    loaded(get_dy, get_w2, get_slope)

    def hidden_back(t):
        m, side = t // 2, lax.rem(t, 2)
        du = (dot(r.dy[...].reshape(L, D), panel(12 + m, side), NN) * r.slope[t].astype(f32)).astype(bf)
        r.slope[t] = du
        r.bcols[pl.ds(8 + t, 1), :] = jnp.sum(du.astype(f32), axis=0, keepdims=True)

    loop(8, hidden_back)
    loaded(get_z)
    grads(
        lambda cols: [r.dy[:, :, cols].reshape(L, COLS)],
        [(12 + t // 2, t % 2, lambda t=t: [r.z[t]]) for t in range(8)],
    )
    scatter.send(4)
    loaded(get_w1)
    send_back(0, [(lambda t=t: r.slope[t], 8 + t // 2, t % 2) for t in range(8)])
    loaded(get_a3, get_h2, get_norm)
    grads(
        lambda cols: [r.left[:, cols]],
        [(8 + t // 2, t % 2, lambda t=t: [r.slope[t]]) for t in range(8)],
    )
    scatter.ready = 8
    get_a1 = load(given.a1, r.left)
    norm_back(0, 4, lambda rows, i: r.h[rows, :], lambda rows, i: half_rows(r.dy, i), 7)
    get_h1 = load(given.h1, r.h)
    scatter.run(1)
    loaded(get_w0)

    def context_back(mat):
        def body(side):
            r.dc[side] = dot(r.dhb[...], panel(mat, side), NN).astype(bf)

        loop(2, body)

    def statistics(lse, ctx):
        r.stat[0:8, :] = lse[...].T[0:8, :]
        for side in range(2):
            both = (r.dc[side].astype(f32) * ctx[side].astype(f32)).T
            r.stat[8 + side * 4 : 12 + side * 4, :] = jnp.sum(both.reshape(4, HD, L), axis=1)

    lane = lax.broadcasted_iota(jnp.int32, (1, 128), 1)
    low = lane < HD
    low_row = lax.broadcasted_iota(jnp.int32, (128, 1), 0) < HD

    def attend_back(query, keys, values, parts, width, causal, turn):
        def body(t):
            side, half = t // 2, lax.rem(t, 2)
            lanes = pl.ds(pl.multiple_of(half * 128, 128), 128)
            q = query[(side, slice(0, L), lanes)].astype(f32) * 0.125
            dc = r.dc[side, :, lanes].astype(f32)
            back = None
            for n in range(parts):
                at = (side, n, slice(None), lanes) if parts > 1 else (side, slice(0, L), lanes)
                k, v = keys[at], values[at]
                flat = k.T
                dk = dv = None
                for sub in range(2):
                    mine = low if sub == 0 else jnp.logical_not(low)
                    mine_row = low_row if sub == 0 else jnp.logical_not(low_row)
                    qh = jnp.where(mine, q, 0.0).astype(bf)
                    dm = jnp.where(mine, dc, 0.0).astype(bf)
                    kt = jnp.where(mine_row, flat.astype(f32), 0.0).astype(bf)
                    r.s[0:width, :] = dot(k, qh, NT)
                    r.dp[0:width, :] = dot(v, dm, NT)
                    lse = r.stat[pl.ds(t * 2 + sub, 1), :]
                    delta = r.stat[pl.ds(8 + t * 2 + sub, 1), :]

                    def rows_body(rows, i):
                        key = i * BLOCK + lax.broadcasted_iota(jnp.int32, (BLOCK, L), 0)
                        if causal:
                            keep = lax.broadcasted_iota(jnp.int32, (BLOCK, L), 1) >= key
                        else:
                            keep = key < HALF_FRAMES
                        p = jnp.where(keep, jnp.exp(jnp.where(keep, r.s[rows, :], -1e30) - lse), 0.0)
                        r.p[rows, :] = p.astype(bf)
                        r.ds[rows, :] = (p * (r.dp[rows, :] - delta)).astype(bf)

                    rows_loop(width, rows_body, 14 if causal else BACK_TURNS)
                    p, ds = r.p[0:width, :], r.ds[0:width, :]
                    dv = dot(p, dm, NN) if dv is None else dv + dot(p, dm, NN)
                    dk = dot(ds, qh, NN) if dk is None else dk + dot(ds, qh, NN)
                    more = dot(kt, ds, NN)
                    back = more if back is None else back + more
                keys[at] = dk.astype(bf)
                values[at] = dv.astype(bf)
            query[(side, slice(0, L), lanes)] = (back.T * 0.125).astype(bf)
            turn(t)

        loop(4, body)

    def column(k, ref, at):
        def body(side):
            r.bcols[pl.ds(k * 2 + side, 1), :] = jnp.sum(ref[at(side)].astype(f32), axis=0, keepdims=True)

        loop(2, body)

    context_back(7)
    loaded(get_c2, get_lse2)
    statistics(r.lse2, r.c2)
    grads(
        lambda cols: [r.dhb[:, cols]], [(7, side, lambda side=side: [r.c2[side]]) for side in range(2)]
    )
    scatter.ready = 9
    scatter.run(1)
    loaded(get_q2, get_ek, get_ev)
    attend_back(r.q2, r.ek, r.ev, 2, KEYS, False, scatter.turn(4))

    loaded(get_e, get_a2)

    def frame_share(half, j):
        acc = None
        for mat, ref in ((5, r.ek), (6, r.ev)):
            for side in range(2):
                more = dot(ref[side, half], part_rows(mat, side, j), NT)
                acc = more if acc is None else acc + more
        return acc

    def frame_trade(j):
        return remote(r.fsend.at[j], r.frecv.at[j], r.frame_send.at[j], r.frame_recv.at[j], mate)

    def frame_store(j):
        cols = pl.ds(pl.multiple_of(j * COLS, COLS), COLS)
        return pltpu.make_async_copy(r.fout.at[lax.rem(j, 2)], r.frame_out.at[:, cols], r.frame_out_sem.at[j])

    def frame_far(j):
        r.fsend[j] = frame_share(1 - c, j).astype(bf)
        frame_trade(j).start()

    def frame_near(j):
        @pl.when(j >= 2)
        def _():
            frame_store(j - 2).wait()

        frame_trade(j).wait_recv()
        r.fout[lax.rem(j, 2)] = frame_share(c, j) + r.frecv[j].astype(f32)
        frame_store(j).start()

    loop(4, frame_far)
    send_back(1, [(lambda side=side: r.q2[side], 4, side) for side in range(2)])
    loop(4, frame_near)
    scatter.run(1)
    grads(
        lambda cols: [r.e[n, :, cols] for n in range(2)],
        [(5 + i, side, lambda ref=ref, side=side: [ref[side, n] for n in range(2)])
         for i, ref in ((1, r.ev), (0, r.ek)) for side in range(2)],
    )
    scatter.ready = 11
    scatter.run(1)
    column(2, r.q2, lambda side: (side,))

    def value_column(side):
        total = sum(jnp.sum(r.ev[side, n].astype(f32), axis=0, keepdims=True) for n in range(2))
        r.bcols[pl.ds(6 + side, 1), :] = total

    loop(2, value_column)
    grads(lambda cols: [r.a2[:, cols]], [(4, side, lambda side=side: [r.q2[side]]) for side in range(2)])
    scatter.ready = 12
    loaded(get_h1)
    norm_back(1, 2, lambda rows, i: r.h[rows, :], lambda rows, i: r.dh[rows, :], 6)
    scatter.run(1)
    context_back(3)
    loaded(get_c1, get_lse1)
    statistics(r.lse1, r.c1)
    grads(
        lambda cols: [r.dhb[:, cols]], [(3, side, lambda side=side: [r.c1[side]]) for side in range(2)]
    )
    scatter.ready = 13
    scatter.run(1)
    loaded(get_qkv)
    q_ref, k_ref, v_ref = (r.qkv.at[i] for i in range(3))
    attend_back(q_ref, k_ref, v_ref, 1, L, True, lambda t: None)
    send_back(2, [(lambda i=i, side=side: r.qkv[i, side, 0:L, :], i, side) for i in range(3) for side in range(2)])
    loaded(get_a1)
    grads(
        lambda cols: [r.left[:, cols]],
        [(i, side, lambda i=i, side=side: [r.qkv[i, side, 0:L, :]]) for i in (2, 1, 0) for side in range(2)],
    )
    scatter.ready = 16
    scatter.run(1)
    column(0, q_ref, lambda side: (side, slice(0, L)))
    column(1, v_ref, lambda side: (side, slice(0, L)))
    loaded(get_x)
    norm_back(2, 0, lambda rows, i: half_rows(r.x, i), lambda rows, i: r.dh[rows, :], None)
    own_rows = pl.ds(pl.multiple_of(c * HALF, HALF), HALF)
    input_copy = pltpu.make_async_copy(r.dh.at[own_rows], r.input_out, r.out_sem.at[0])
    input_copy.start()

    sums = jnp.concatenate([jnp.sum(r.cols[k * 8 : k * 8 + 8, :], axis=0, keepdims=True) for k in range(9)], axis=0)
    if fast:
        r.small[...] = jnp.zeros(r.small.shape, f32)
        for i in range(2 * levels):
            for xx in range(2):
                k = i * 2 + xx
                r.small[k, 0:9, :] = sums[:, i * 128 : (i + 1) * 128]
                r.small[k, 9:10, :] = r.bcols[k : k + 1, 0:128]
                r.small[k, 10:11, :] = r.bcols[k : k + 1, 128:256]

        def small_copy(k, slot):
            i = lax.rem(me + k + 1, count)
            return remote(r.small.at[i], r.smallgot.at[slot], r.small_send.at[k], r.small_recv.at[slot],
                          peer(i))

        loop(count - 1, lambda k: small_copy(k, me).start())
        r.smallgot[me] = r.small[me]
    else:
        r.smallsum[0:9, :] = sums
    while scatter.steps < MATS + 2:
        scatter.run(min(4, MATS + 2 - scatter.steps))
    owned_copy = pltpu.make_async_copy(r.own, r.owned_out, r.out_sem.at[1])
    owned_copy.start()
    if fast:
        loop(count - 1, lambda k: small_copy(k, lax.rem(me + k + 1, count)).wait_recv())
        total = r.smallgot[0]
        for k in range(1, 4 * levels):
            total = total + r.smallgot[k]
        r.smallsum[...] = total
        loop(count - 1, lambda k: small_copy(k, me).wait_send())
    small_store = pltpu.make_async_copy(r.smallsum, r.small_out, r.out_sem.at[2])
    bcols_store = pltpu.make_async_copy(r.bcols, r.bcols_out, r.out_sem.at[3])
    small_store.start()
    bcols_store.start()
    small_store.wait()
    bcols_store.wait()
    for n in (1, 2):
        loop(4, lambda j: trade(n, j).wait_send())
    loop(4, lambda j: frame_trade(j).wait_send())
    for j in (2, 3):
        frame_store(j).wait()
    scatter.drain()
    input_copy.wait()
    owned_copy.wait()


def backward(kept, shards):
    levels, rows = shards // 2, D // shards
    fast = rows == 128
    f32, bf = jnp.float32, jnp.bfloat16
    sem = pltpu.SemaphoreType.DMA
    hbm = pl.BlockSpec(memory_space=pl.ANY)
    peers = shards * 2
    shapes = [((MATS, rows, COLS), f32), ((HALF, D), f32), ((KEYS, D), f32)]
    shapes += [((16, 128) if fast else (16, D), f32), ((16, COLS), f32)]
    small = (peers, 16, 128) if fast else (1, 16, 128)
    vm = pltpu.VMEM
    scratch = [
        vm((MATS, 2, levels // 2, 2, 2, rows, COLS), bf), vm((MATS, rows, COLS), f32), vm((2, HALF, D), bf),
        vm((8, L, COLS), bf), vm((8, L, COLS), bf), vm((L, D), bf), vm((L, D), f32), vm((16, D), f32),
        vm((2, L, COLS), bf), vm((2, L, COLS), bf), vm((L, 128), f32), vm((2, 2, KEYS, COLS), bf),
        vm((2, 2, KEYS, COLS), bf), vm((2, KEYS, D), bf), vm((L, D), bf),
        vm((2, L, COLS), bf), vm((3, 2, 512, COLS), bf), vm((L, 128), f32), vm((2, HALF, D), bf),
        vm((L, D), f32), vm((L, D), bf), vm((2, L, COLS), bf), vm((16, L), f32),
        vm((KEYS, L), f32), vm((KEYS, L), f32), vm((KEYS, L), bf), vm((KEYS, L), bf),
        vm((2, 4, L, COLS), bf), vm((2, 4, L, COLS), bf), vm((4, KEYS, COLS), bf), vm((4, KEYS, COLS), bf),
        vm((2, KEYS, COLS), f32), vm((72, D), f32), vm((16, COLS), f32), vm(small, f32), vm(small, f32),
        vm((16, 128) if fast else (16, D), f32),
        sem((24,)), sem((3, 4)), sem((3, 4)), sem((4,)), sem((4,)), sem((4,)), sem((peers,)), sem((peers,)), sem((4,)),
    ]
    return pl.pallas_call(
        partial(backward_kernel, levels, fast),
        out_shape=[jax.ShapeDtypeStruct(s, t) for s, t in shapes],
        in_specs=[hbm] * len(BackwardIn._fields),
        out_specs=[hbm] * len(shapes),
        scratch_shapes=scratch + Scatter.buffers(levels, rows) + Scatter.semaphores(levels),
        compiler_params=pltpu.CompilerParams(
            collective_id=1, has_side_effects=True, vmem_limit_bytes=63 * 2**20
        ),
        name="backward",
    )(
        kept.dy, kept.wide.reshape(MATS, 2, levels // 2, 2, 2, rows, COLS), kept.slope, kept.z, kept.a3, kept.h2, kept.norm, kept.c2, kept.q2, kept.lse2,
        kept.ek, kept.ev, kept.e, kept.a2, kept.h1, kept.c1, kept.qkv, kept.lse1, kept.a1, kept.x,
    )


def small_kernel(shards, every, scatter, src, out, own_sem, send_sem, recv_sem):
    dp, x, c = (lax.axis_index(a) for a in AXES)
    cores = 2 if every else 1
    count = shards * 2 * cores
    me = (dp * 2 + x) * cores + (c if every else 0)

    def peer(i):
        if every:
            return (i // 4, lax.rem(i // 2, 2), lax.rem(i, 2))
        return (i // 2, lax.rem(i, 2), c)

    bar = pltpu.get_barrier_semaphore()

    def greet(k, carry):
        pl.semaphore_signal(bar, inc=1, device_id=peer(lax.rem(me + k, count)), device_id_type=DT)
        return carry

    lax.fori_loop(1, count, greet, 0)
    pl.semaphore_wait(bar, count - 1)

    def copy(k):
        i = lax.rem(me + k, count)
        return pltpu.make_async_remote_copy(
            src.at[i] if scatter else src, out.at[me], send_sem.at[k], recv_sem.at[me],
            device_id=peer(i), device_id_type=DT,
        )

    def send(k, carry):
        copy(k).start()
        return carry

    own = pltpu.make_async_copy(src.at[me] if scatter else src, out.at[me], own_sem)
    own.start()
    lax.fori_loop(1, count, send, 0)
    own.wait()

    def finish(k, carry):
        i = lax.rem(me + k, count)
        pltpu.make_async_remote_copy(
            src.at[i] if scatter else src, out.at[i], send_sem.at[k], recv_sem.at[i],
            device_id=peer(i), device_id_type=DT,
        ).wait_recv()
        copy(k).wait_send()
        return carry

    lax.fori_loop(1, count, finish, 0)


def small_exchange(src, shards, every, scatter, call_id):
    count = shards * 2 * (2 if every else 1)
    shape = src.shape[1:] if scatter else src.shape
    sem = pltpu.SemaphoreType.DMA
    vm = pl.BlockSpec(memory_space=pltpu.VMEM)
    return pl.pallas_call(
        partial(small_kernel, shards, every, scatter),
        out_shape=jax.ShapeDtypeStruct((count, *shape), src.dtype),
        in_specs=[vm],
        out_specs=vm,
        scratch_shapes=[sem, sem((count,)), sem((count,))],
        compiler_params=pltpu.CompilerParams(collective_id=call_id, has_side_effects=True),
        name=f"small_exchange_{call_id}",
    )(src)


def adapt(weight, gradient, moment, second, token_total):
    scaled_grad = gradient / token_total
    new_moment = 0.5 * moment + 0.5 * scaled_grad
    new_second = 0.5 * second + 0.5 * scaled_grad * scaled_grad
    direction = new_moment / (jnp.sqrt(new_second) + 1e-06) + 0.01 * weight
    return (new_moment, new_second, direction)


def shards_fn(
    tokens, frames, cotangent, attention_weights, dense_weights, unit_bias, norm_bias,
    attention_mean, dense_mean, unit_mean, norm_mean,
    attention_square, dense_square, unit_square, norm_square,
):
    f32, bf = jnp.float32, jnp.bfloat16
    shards = lax.axis_size("dp")
    rows = D // shards
    c = lax.axis_index("core")
    unit_cols = unit_bias.shape[1]
    column_rows = (lax.axis_index("dp") * unit_cols + jnp.arange(unit_cols, dtype=jnp.int32)) // HD
    row_pick = (column_rows[:, None] == jnp.arange(8, dtype=jnp.int32)[None, :]).astype(f32)
    leader = ((lax.axis_index("side") == 0) & (c == 0)).astype(f32)

    def square_rows(attn_part, dense_part, unit_part, norm_part):
        unit_sums = jnp.sum(jnp.sum(unit_part * unit_part, axis=0)[:, None] * row_pick, axis=0)
        return jnp.concatenate(
            [
                jnp.sum(attn_part * attn_part, axis=(2, 3)).reshape(8),
                jnp.sum(dense_part * dense_part, axis=(1, 2, 3)),
                unit_sums,
                jnp.sum(norm_part * norm_part, axis=1) * leader,
            ]
        )

    own_attn = attention_weights.astype(f32)
    own_dense = dense_weights.astype(f32)
    own_unit = unit_bias.astype(f32)
    own_norm = norm_bias.astype(f32)

    if rows == 128:
        pack = jnp.concatenate([norm_bias.astype(f32), unit_bias.astype(f32).reshape(2, 128)])
        small = (jnp.pad(pack, ((0, 5), (0, 0))), jnp.zeros((8, 128), f32), jnp.zeros((8, 128), f32))
    else:
        pack = jnp.concatenate([norm_bias.reshape(-1), unit_bias.reshape(-1)])
        pack = jnp.pad(pack, (0, 2048 - pack.shape[0])).reshape(16, 128)
        packs = small_exchange(pack, shards, False, False, 2).reshape(shards, 2, 2048)
        norm_rows = packs[:, 0, : 9 * rows].reshape(shards, 9, rows).transpose(1, 0, 2).reshape(9, D).astype(f32)
        unit_all = packs[:, :, 9 * rows : 9 * rows + 4 * unit_cols].reshape(shards, 2, 4, unit_cols)
        bias_rows = (
            unit_all.transpose(1, 2, 0, 3).reshape(2, 4, 8, HD).transpose(2, 0, 1, 3).reshape(16, COLS).astype(f32)
        )
        small = (jnp.zeros((16, 128), f32), jnp.pad(norm_rows, ((0, 7), (0, 0))), bias_rows)

    shard = jnp.concatenate(
        [attention_weights.reshape(8, rows, COLS), dense_weights.transpose(0, 2, 1, 3).reshape(8, rows, COLS)]
    )
    kept = forward(shard, tokens, jnp.pad(frames, ((0, KEYS - HALF_FRAMES), (0, 0))), cotangent, small, shards)
    layer_out = kept.layer_out
    owned, input_gradient, frame_gradient, *small_grads = backward(kept, shards)
    frame_gradient = frame_gradient[:HALF_FRAMES]
    attention_owned = owned[:8].reshape(2, 4, rows, COLS)
    dense_owned = owned[8:].reshape(2, 4, rows, COLS).transpose(0, 2, 1, 3)

    if rows == 128:
        norm_owned = small_grads[0][:9]
        unit_owned = small_grads[0][9:11].reshape(4, unit_cols)
    else:
        norm_parts = small_grads[0][:9].reshape(9, shards, rows).transpose(1, 0, 2).reshape(shards, 1, 9 * rows)
        unit_parts = small_grads[1].reshape(8, 2, 4, HD).transpose(1, 2, 0, 3).reshape(2, 4, shards, unit_cols)
        unit_parts = unit_parts.transpose(2, 0, 1, 3).reshape(shards, 2, 4 * unit_cols)
        small = jnp.concatenate([jnp.broadcast_to(norm_parts, (shards, 2, 9 * rows)), unit_parts], axis=2)
        small = jnp.pad(small, ((0, 0), (0, 0), (0, 2048 - small.shape[2]))).reshape(shards * 2, 16, 128)
        small = jnp.sum(small_exchange(small, shards, False, True, 13), axis=0).reshape(2048)
        norm_owned = small[: 9 * rows].reshape(9, rows)
        unit_owned = small[9 * rows : 9 * rows + 4 * unit_cols].reshape(4, unit_cols)

    token_total = float(tokens.shape[0] * shards * 4)
    attn_moment, attn_second, attn_dir = adapt(
        own_attn, attention_owned, attention_mean, attention_square, token_total
    )
    dense_moment, dense_second, dense_dir = adapt(
        own_dense, dense_owned, dense_mean, dense_square, token_total
    )
    unit_moment, unit_second, unit_dir = adapt(
        own_unit, unit_owned, unit_mean, unit_square, token_total
    )
    norm_moment, norm_second, norm_dir = adapt(
        own_norm, norm_owned, norm_mean, norm_square, token_total
    )
    sums = jnp.concatenate(
        [
            square_rows(own_attn, own_dense, own_unit, own_norm),
            square_rows(attn_dir, dense_dir, unit_dir, norm_dir),
        ]
    )
    sums = jnp.pad(sums, (0, 1024 - 54)).reshape(8, 128)
    sums = jnp.sum(small_exchange(sums, shards, True, False, 14), axis=0).reshape(1024)
    weight_norms = jnp.sqrt(sums[:27])
    step_norms = jnp.sqrt(sums[27:54])
    trust = weight_norms / step_norms
    attention_step = -learning_rate * trust[0:8].reshape(2, 4, 1, 1) * attn_dir
    dense_step = -learning_rate * trust[8:10].reshape(2, 1, 1, 1) * dense_dir
    unit_factor = jnp.sum(row_pick * trust[10:18][None, :], axis=1)
    unit_step = -learning_rate * unit_factor[None, :] * unit_dir
    norm_step = -learning_rate * trust[18:27][:, None] * norm_dir
    return (
        layer_out, input_gradient, frame_gradient,
        attention_owned, dense_owned, unit_owned, norm_owned,
        attn_moment, dense_moment, unit_moment, norm_moment,
        attn_second, dense_second, unit_second, norm_second,
        attention_step, dense_step, unit_step, norm_step,
        weight_norms, step_norms,
    )


def solution(mesh):
    shards = mesh.shape["dp"]
    inner = Mesh(mesh.devices.reshape(shards, 2, 2), AXES)
    tensor = ("side", "core")
    rows = P(("dp", *tensor), None)
    state = (P(None, None, "dp", tensor), P(None, "dp", None, tensor), P(tensor, "dp"), P(None, "dp"))
    return jax.shard_map(
        shards_fn,
        mesh=inner,
        in_specs=(rows, rows, rows) + state * 3,
        out_specs=(rows, rows, rows) + state * 4 + (P(), P()),
        check_vma=False,
    )
```

```python
from functools import partial
from typing import NamedTuple

import jax
import jax.numpy as jnp
from jax import lax
from jax.experimental import pallas as pl
from jax.experimental.pallas import tpu as pltpu
from jax.sharding import Mesh, PartitionSpec as P

D = 1024
HEADS = 16
HD = 64
L = 448
FRAMES = 1500
MATS = 16
COLS = 256

learning_rate = 0.3
DT = pl.DeviceIdType.MESH
AXES = ("dp", "side", "core")


def place():
    dp = lax.axis_index("dp")
    return dp // 2, lax.rem(dp, 2), lax.axis_index("side"), lax.axis_index("core")


def device(z, y, x, c):
    return (z * 2 + y, x, c)


def greet_neighbours(levels):
    z, y, x, c = place()
    bar = pltpu.get_barrier_semaphore()
    pl.semaphore_signal(bar, inc=1, device_id=device(z, y, 1 - x, c), device_id_type=DT)
    pl.semaphore_signal(bar, inc=1, device_id=device(z, 1 - y, x, c), device_id_type=DT)

    @pl.when(z > 0)
    def _():
        pl.semaphore_signal(bar, inc=1, device_id=device(z - 1, y, x, c), device_id_type=DT)

    @pl.when(z < levels - 1)
    def _():
        pl.semaphore_signal(bar, inc=1, device_id=device(z + 1, y, x, c), device_id_type=DT)

    pl.semaphore_wait(
        bar, 2 + jnp.where(z > 0, 1, 0) + jnp.where(z < levels - 1, 1, 0)
    )


class Gather:
    def __init__(self, levels, groups, shard, wide, sems):
        self.levels, self.groups, self.size = levels, groups, MATS // groups
        self.shard, self.wide = shard, wide
        self.own, self.zs, self.zr, self.xs, self.xr, self.ys, self.yr = sems
        self.at = place()
        self.done = 0
        self.total = (groups + LAG) * levels

    @staticmethod
    def semaphores(levels, groups):
        sem = pltpu.SemaphoreType.DMA
        one, pair = sem((groups, levels)), sem((groups, levels, 2))
        return [sem, pair, one, pair, pair, pair, pair]

    def block(self, g, xx, zz, yy):
        return self.wide.at[pl.ds(g * self.size, self.size), xx, zz, yy]

    def mine(self, g):
        return self.shard.at[pl.ds(g * self.size, self.size)]

    def z_copy(self, g, zz, up, own=False):
        z, y, x, c = self.at
        return pltpu.make_async_remote_copy(
            self.mine(g) if own else self.block(g, x, zz, y), self.block(g, x, zz, y), self.zs.at[g, zz, up],
            self.zr.at[g, zz], device_id=device(z + 1 if up else z - 1, y, x, c), device_id_type=DT,
        )

    def x_copy(self, g, zz, yy, own=False):
        z, y, x, c = self.at
        return pltpu.make_async_remote_copy(
            self.mine(g) if own else self.block(g, x, zz, yy), self.block(g, x, zz, yy), self.xs.at[g, zz, yy],
            self.xr.at[g, zz, yy], device_id=device(z, y, 1 - x, c), device_id_type=DT,
        )

    def y_copy(self, g, zz, xx, own=False):
        z, y, x, c = self.at
        return pltpu.make_async_remote_copy(
            self.mine(g) if own else self.block(g, xx, zz, y), self.block(g, xx, zz, y), self.ys.at[g, zz, xx],
            self.yr.at[g, zz, xx], device_id=device(z, 1 - y, x, c), device_id_type=DT,
        )

    def z_send(self, g):
        z = self.at[0]
        for up in (1, 0):
            @pl.when(z < self.levels - 1 if up else z > 0)
            def _():
                self.z_copy(g, z, up, True).start()

    def begin(self):
        z, y, x, c = self.at
        for g in range(min(Z_AHEAD, self.groups)):
            self.z_send(g)
        self.local = pltpu.make_async_copy(self.shard, self.wide.at[:, x, z, y], self.own)
        self.local.start()

    def first(self, g, d):
        z, y, x, c = self.at

        @pl.when(d == 0)
        def _():
            @pl.when(g + Z_AHEAD < self.groups)
            def _():
                self.z_send(g + Z_AHEAD)

            self.x_copy(g, z, y, True).start()
            self.y_copy(g, z, x, True).start()

        for up in (1, 0):
            zz = z - d if up else z + d

            @pl.when((d > 0) & (zz >= 0 if up else zz < self.levels))
            def _():
                self.z_copy(g, zz, up).wait_recv()

                @pl.when(z < self.levels - 1 if up else z > 0)
                def _():
                    self.z_copy(g, zz, up).start()

                self.x_copy(g, zz, y).start()
                self.y_copy(g, zz, x).start()

    def second(self, g, d):
        z, y, x, c = self.at
        for up in (1, 0):
            zz = z - d if up else z + d
            here = zz >= 0 if up else (zz < self.levels) & (d > 0)
            even = lax.rem(zz + self.levels, 2) == 0

            @pl.when(here & even)
            def _():
                self.x_copy(g, zz, y).wait_recv()
                self.y_copy(g, zz, 1 - x).start()

            @pl.when(here & jnp.logical_not(even))
            def _():
                self.y_copy(g, zz, x).wait_recv()
                self.x_copy(g, zz, 1 - y).start()

    def tick(self, t):
        g, d = t // self.levels, lax.rem(t, self.levels)

        @pl.when((g >= LAG) & (g < self.groups + LAG))
        def _():
            self.second(g - LAG, d)

        @pl.when(g < self.groups)
        def _():
            self.first(g, d)

    def run(self, count):
        count = max(0, min(count, self.total - self.done))
        start = self.done
        self.done += count
        if count:
            loop(count, lambda i: self.tick(start + i))

    def turn(self, count):
        start = self.done
        self.done = min(self.total, self.done + count)
        return lambda i: self.tick(start + i)

    def need(self, mat):
        g = mat // self.size
        self.run((g + 1 + LAG) * self.levels - self.done)
        z, y, x, c = self.at

        def body(zz):
            @pl.when(lax.rem(zz, 2) == 0)
            def _():
                self.y_copy(g, zz, x).wait_recv()
                self.y_copy(g, zz, 1 - x).wait_recv()

            @pl.when(lax.rem(zz, 2) == 1)
            def _():
                self.x_copy(g, zz, y).wait_recv()
                self.x_copy(g, zz, 1 - y).wait_recv()

        if mat % self.size == 0:
            loop(self.levels, body)
        if mat == 0:
            self.local.wait()

    def drain(self):
        z, y, x, c = self.at

        def group(g):
            def sent(zz):
                self.x_copy(g, zz, y).wait_send()
                self.y_copy(g, zz, x).wait_send()

                @pl.when(lax.rem(zz, 2) == 0)
                def _():
                    self.y_copy(g, zz, 1 - x).wait_send()

                @pl.when(lax.rem(zz, 2) == 1)
                def _():
                    self.x_copy(g, zz, 1 - y).wait_send()

            loop(self.levels, sent)

            def relayed(zz):
                @pl.when((z < self.levels - 1) & (zz <= z))
                def _():
                    self.z_copy(g, zz, 1).wait_send()

                @pl.when((z > 0) & (zz >= z))
                def _():
                    self.z_copy(g, zz, 0).wait_send()

            loop(self.levels, relayed)

        loop(self.groups, group)


LAG = 2
Z_AHEAD = 1
GROUPS = 8
HALF = L // 2
KEYS = 768
HALF_FRAMES = FRAMES // 2
BLOCK = 32
SOFT_TURNS = 14
NORM_TURNS = 7
BACK_TURNS = 12


def dot(a, b, dims):
    return lax.dot_general(a, b, (dims, ((), ())), preferred_element_type=jnp.float32)


NN, NT, TN = ((1,), (0,)), ((1,), (1,)), ((0,), (0,))


def flat_panel(ref, mat, side):
    return ref[mat, side].reshape(D, COLS)


def flat_rows(panel, j):
    per = COLS // (2 * panel.shape[2])
    return panel[pl.ds(j * per, per)].reshape(COLS, COLS)


def rows_loop(count, body, turns=1):
    def run(k, carry):
        for u in range(turns):
            i = k * turns + u
            body(pl.ds(pl.multiple_of(i * BLOCK, BLOCK), BLOCK), i)
        return carry

    lax.fori_loop(0, count // (BLOCK * turns), run, 0)


def loop(count, body):
    def run(i, carry):
        body(i)
        return carry

    lax.fori_loop(0, count, run, 0)


def normed_block(values):
    centre = values - jnp.mean(values, axis=-1, keepdims=True)
    spread = jnp.mean(centre * centre, axis=-1, keepdims=True)
    scaled = lax.rsqrt(spread + 1e-05)
    return centre * scaled, scaled


def panels_row(ref, rows):
    return jnp.concatenate([ref[j, rows, :].astype(jnp.float32) for j in range(4)], axis=1)


def forward_kernel(levels, groups, fast, *refs):
    f32, bf = jnp.float32, jnp.bfloat16
    width = len(ForwardRefs._fields)
    r = ForwardRefs(*refs[:width])
    gather = Gather(levels, groups, r.shard, r.wide, refs[width:])
    z, y, x, c = place()
    dp = z * 2 + y
    mate = (dp, x, 1 - c)
    count = levels * 4
    me = dp * 2 + x

    def peer(i):
        return (i // 2, lax.rem(i, 2), c)

    bar = pltpu.get_barrier_semaphore()
    loop(count - 1, lambda k: pl.semaphore_signal(
        bar, inc=1, device_id=peer(lax.rem(me + k + 1, count)), device_id_type=DT))
    pl.semaphore_signal(bar, inc=1, device_id=mate, device_id_type=DT)
    pl.semaphore_wait(bar, count)

    def remote(src, dst, send, recv, dev):
        return pltpu.make_async_remote_copy(src, dst, send, recv, device_id=dev, device_id_type=DT)

    inputs = ((r.tokens, r.x), (r.frames, r.e), (r.cotangent, r.dy))

    def swap(k, slot):
        src, dst = inputs[k]
        return remote(src, dst.at[slot], r.swap_send.at[k], r.swap_recv.at[k], mate)

    def local(k):
        src, dst = inputs[k]
        return pltpu.make_async_copy(src, dst.at[c], r.in_sem.at[k])

    if fast:
        def pack_copy(k, slot):
            return remote(r.pack, r.packs.at[slot], r.pack_send.at[k], r.pack_recv.at[slot],
                          peer(lax.rem(me + k + 1, count)))

        loop(count - 1, lambda k: pack_copy(k, me).start())
        own_pack = pltpu.make_async_copy(r.pack, r.packs.at[me], r.in_sem.at[3])
        own_pack.start()
    swap(0, c).start()
    local(0).start()
    gather.begin()
    gather.run(1)
    for k in (1, 2):
        swap(k, c).start()
        local(k).start()

    def arrived(k):
        local(k).wait()
        swap(k, 1 - c).wait_recv()

    outs = []

    def emit(out, scratch):
        outs.append(pltpu.make_async_copy(scratch, out, r.out_sem.at[len(outs)]))
        outs[-1].start()

    if fast:
        own_pack.wait()
        loop(count - 1, lambda k: pack_copy(k, lax.rem(me + k + 1, count)).wait_recv())
        for i in range(2 * levels):
            for xx in range(2):
                block = r.packs[i * 2 + xx]
                if xx == 0:
                    r.norm[:, i * 128 : (i + 1) * 128] = block
                r.bias[i * 2 + xx : i * 2 + xx + 1, 0:128] = block[9:10]
                r.bias[i * 2 + xx : i * 2 + xx + 1, 128:256] = block[10:11]
    else:
        r.norm[...] = r.norm_in[...]
        r.bias[...] = r.bias_in[...]
    emit(r.norm_out, r.norm)

    def norm_row(k):
        return r.norm[k : k + 1, :]

    def bias_row(k, side):
        return r.bias[pl.ds(k * 2 + side, 1), :]

    key = lax.broadcasted_iota(jnp.int32, (1, 2 * KEYS), 1)
    real = lax.rem(key, KEYS) < HALF_FRAMES
    r.padrow[0:1, :] = jnp.where(real, 0.0, -1e30).astype(f32)
    for i in range(3):
        for side in range(2):
            r.qkv[i, side, L:512, :] = jnp.zeros((512 - L, COLS), bf)

    arrived(0)

    def ln1(half):
        def body(rows, i):
            normed, _ = normed_block(r.x[half, rows, :].astype(f32))
            out = (normed * norm_row(0) + norm_row(1)).astype(bf)
            r.a1[pl.ds(pl.multiple_of(half * HALF + i * BLOCK, BLOCK), BLOCK), :] = out

        rows_loop(HALF, body, NORM_TURNS if NORM_TURNS in (1, 7) else 1)

    ln1(0)
    ln1(1)
    emit(r.a1_out, r.a1)
    emit(r.x_out, r.x)

    def project_one(i, side):
        bias = bias_row(0, side) if i == 0 else bias_row(1, side)
        acc = dot(r.a1[...], flat_panel(r.wide, i, side), NN)
        if i != 1:
            acc = acc + bias
        r.qkv[i, side, 0:L, :] = acc.astype(bf)

    for i in range(3):
        gather.need(i)
        loop(2, lambda side: project_one(i, side))
    emit(r.qkv_out, r.qkv)

    lane = lax.broadcasted_iota(jnp.int32, (1, 128), 1)
    low = lane < HD

    def attend(query, key_parts, values, width, causal, lse, ctx, per_head, tick):
        def body(t):
            side, half = t // 2, lax.rem(t, 2)
            lanes = pl.ds(pl.multiple_of(half * 128, 128), 128)
            q = query(side, lanes)
            found = []
            for sub in range(2):
                mine = low if sub == 0 else jnp.logical_not(low)
                qh = jnp.where(mine, q.astype(f32) * 0.125, 0.0).astype(bf)
                for n, part in enumerate(key_parts(side, lanes)):
                    r.s[:, n * width : (n + 1) * width] = dot(qh, part, NT)
                total = width * len(key_parts(side, lanes))

                def rows_body(rows, i):
                    s = r.s[rows, 0:total]
                    if causal:
                        row = i * BLOCK + lax.broadcasted_iota(jnp.int32, (BLOCK, total), 0)
                        col = lax.broadcasted_iota(jnp.int32, (BLOCK, total), 1)
                        s = jnp.where(col <= row, s, -1e30)
                    else:
                        s = s + r.padrow[0:1, 0:total]
                    top = jnp.max(s, axis=-1, keepdims=True)
                    e = jnp.exp(s - top)
                    weight = jnp.sum(e, axis=-1, keepdims=True)
                    r.p[rows, 0:total] = (e * (1.0 / weight)).astype(bf)
                    lse[rows, :] = jnp.where(lane == t * 2 + sub, top + jnp.log(weight), lse[rows, :])

                rows_loop(L, rows_body, SOFT_TURNS)
                for i in range(per_head):
                    tick((t * 2 + sub) * per_head + i)
                acc = None
                for n, part in enumerate(values(side, lanes)):
                    more = dot(r.p[:, n * width : (n + 1) * width], part, NN)
                    acc = more if acc is None else acc + more
                found.append(acc)
            ctx[side, :, lanes] = jnp.where(low, found[0], found[1]).astype(bf)

        loop(4, body)

    attend(
        lambda side, lanes: r.qkv[0, side, 0:L, lanes],
        lambda side, lanes: [r.qkv[1, side, :, lanes]],
        lambda side, lanes: [r.qkv[2, side, :, lanes]],
        512, True, r.lse1, r.c1, 1, gather.turn(8),
    )
    emit(r.lse1_out, r.lse1)
    emit(r.c1_out, r.c1)

    def collect(n, ctx, mat):
        def body(j):
            rows = pl.ds(pl.multiple_of(j * COLS, COLS), COLS)
            acc = None
            for side in range(2):
                more = dot(ctx[side], flat_rows(r.wide.at[mat, side], j), NT)
                acc = more if acc is None else acc + more
            r.part[n, j] = acc.astype(bf)
            trade(n, j).start()

        loop(4, body)

    def trade(n, j):
        return remote(r.part.at[n, j], r.got.at[n, j], r.part_send.at[n, j], r.part_recv.at[n, j], mate)

    def traded(n):
        loop(4, lambda j: trade(n, j).wait_recv())

    def residual(n, base, bias_k, out, gain_k, normed_out):
        def body(rows, i):
            v = base(rows, i) + norm_row(bias_k) + (panels_row(r.part.at[n], rows) + panels_row(r.got.at[n], rows))
            out[rows, :] = v
            normed, _ = normed_block(v)
            normed_out[rows, :] = (normed * norm_row(gain_k) + norm_row(gain_k + 1)).astype(bf)

        rows_loop(L, body, NORM_TURNS)

    def x_rows(rows, i):
        half = i // (HALF // BLOCK)
        inner = pl.ds(pl.multiple_of((i - half * (HALF // BLOCK)) * BLOCK, BLOCK), BLOCK)
        return r.x[half, inner, :].astype(f32)

    gather.need(3)
    collect(0, r.c1, 3)
    gather.run(1)
    traded(0)
    residual(0, x_rows, 6, r.h1, 2, r.a2)
    emit(r.h1_out, r.h1)
    emit(r.a2_out, r.a2)

    gather.need(4)

    def query_two(side):
        acc = dot(r.a2[...], flat_panel(r.wide, 4, side), NN) + bias_row(2, side)
        r.q2[side] = acc.astype(bf)

    loop(2, query_two)
    emit(r.q2_out, r.q2)
    arrived(1)
    emit(r.e_out, r.e)

    gather.need(5)

    def frame_keys(t):
        side, half = t // 2, lax.rem(t, 2)
        r.ek[side, half] = dot(r.e[half], flat_panel(r.wide, 5, side), NN).astype(bf)

    loop(4, frame_keys)
    emit(r.ek_out, r.ek)
    gather.need(6)

    def frame_values(t):
        side, half = t // 2, lax.rem(t, 2)
        acc = dot(r.e[half], flat_panel(r.wide, 6, side), NN) + bias_row(3, side)
        r.ev[side, half] = acc.astype(bf)

    loop(4, frame_values)
    emit(r.ev_out, r.ev)
    attend(
        lambda side, lanes: r.q2[side, :, lanes],
        lambda side, lanes: [r.ek[side, half, :, lanes] for half in range(2)],
        lambda side, lanes: [r.ev[side, half, :, lanes] for half in range(2)],
        KEYS, False, r.lse2, r.c2, 2, gather.turn(16),
    )
    emit(r.lse2_out, r.lse2)
    emit(r.c2_out, r.c2)
    gather.need(7)
    collect(1, r.c2, 7)
    gather.run(1)
    traded(1)
    residual(1, lambda rows, i: r.h1[rows, :], 7, r.h2, 4, r.a3)
    emit(r.h2_out, r.h2)
    emit(r.a3_out, r.a3)
    arrived(2)
    emit(r.dy_out, r.dy)

    def hidden(t):
        m, side = t // 2, lax.rem(t, 2)
        u = dot(r.a3[...], flat_panel(r.wide, 8 + m, side), NN) + bias_row(4 + m, side)
        half = 0.5 * (1.0 + lax.erf(u * 0.7071067811865476))
        r.z[t] = (u * half).astype(bf)
        r.slope[t] = (half + u * jnp.exp(-0.5 * u * u) * 0.3989422804014327).astype(bf)

    def result(k):
        def tile(j):
            cols = pl.ds(pl.multiple_of(j * COLS, COLS), COLS)
            acc = None
            for t in range(4 * k, 4 * k + 4):
                more = dot(r.z[t], flat_rows(r.wide.at[12 + t // 2, t % 2], j), NT)
                acc = more if acc is None else acc + more
            if k == 0:
                r.acc[:, cols] = acc
            else:
                r.acc[:, cols] += acc

        loop(4, tile)

    for m in range(4):
        gather.need(8 + m)
        loop(2, lambda side: hidden(2 * m + side))
    emit(r.z_out, r.z)
    emit(r.slope_out, r.slope)
    for k in range(2):
        gather.need(12 + 2 * k)
        gather.need(13 + 2 * k)
        result(k)

    emit(r.wide_out, r.wide)

    for half in range(2):
        @pl.when(c == half)
        def _():
            far = (1 - half) * HALF

            def body(j):
                cols = pl.ds(pl.multiple_of(j * COLS, COLS), COLS)
                r.part[2, j, 0:HALF, :] = r.acc[far : far + HALF, cols].astype(bf)

            loop(4, body)

    last = remote(
        r.part.at[2, :, 0:HALF], r.got.at[2, :, 0:HALF], r.part_send.at[2, 0], r.part_recv.at[2, 0], mate
    )
    last.start()
    last.wait_recv()

    def finish(rows, i):
        here = pl.ds(pl.multiple_of(c * HALF + i * BLOCK, BLOCK), BLOCK)
        own = r.acc[here, :].astype(bf).astype(f32)
        v = r.h2[here, :] + norm_row(8) + (own + panels_row(r.got.at[2], rows))
        r.outrows[rows, :] = v.astype(bf)

    rows_loop(HALF, finish)
    emit(r.layer_out, r.outrows)

    for k in range(3):
        swap(k, c).wait_send()
    if fast:
        loop(count - 1, lambda k: pack_copy(k, me).wait_send())
    for n in range(2):
        loop(4, lambda j: trade(n, j).wait_send())
    last.wait_send()
    gather.drain()
    for copy in outs:
        copy.wait()


class ForwardRefs(NamedTuple):
    shard: object
    tokens: object
    frames: object
    cotangent: object
    pack: object
    norm_in: object
    bias_in: object
    layer_out: object
    norm_out: object
    a1_out: object
    x_out: object
    qkv_out: object
    lse1_out: object
    c1_out: object
    h1_out: object
    a2_out: object
    q2_out: object
    e_out: object
    ek_out: object
    ev_out: object
    lse2_out: object
    c2_out: object
    h2_out: object
    a3_out: object
    dy_out: object
    z_out: object
    slope_out: object
    wide_out: object
    wide: object
    x: object
    dy: object
    e: object
    norm: object
    bias: object
    a1: object
    a2: object
    a3: object
    h1: object
    h2: object
    qkv: object
    c1: object
    q2: object
    c2: object
    ek: object
    ev: object
    lse1: object
    lse2: object
    z: object
    slope: object
    s: object
    p: object
    acc: object
    part: object
    got: object
    packs: object
    padrow: object
    outrows: object
    in_sem: object
    swap_send: object
    swap_recv: object
    part_send: object
    part_recv: object
    pack_send: object
    pack_recv: object
    out_sem: object


class Kept(NamedTuple):
    layer_out: object
    norm: object
    a1: object
    x: object
    qkv: object
    lse1: object
    c1: object
    h1: object
    a2: object
    q2: object
    e: object
    ek: object
    ev: object
    lse2: object
    c2: object
    h2: object
    a3: object
    dy: object
    z: object
    slope: object
    wide: object


def forward(shard, tokens, frames, cotangent, small, shards):
    levels, rows = shards // 2, D // shards
    groups = GROUPS if levels <= 4 else 4
    fast = rows == 128
    f32, bf = jnp.float32, jnp.bfloat16
    sem = pltpu.SemaphoreType.DMA
    vm, hbm = pl.BlockSpec(memory_space=pltpu.VMEM), pl.BlockSpec(memory_space=pl.ANY)
    wide = (MATS, 2, levels, 2, rows, COLS)
    shapes = [
        ((HALF, D), bf),
        ((16, D), f32),
        ((L, D), bf),
        ((2, HALF, D), bf),
        ((3, 2, 512, COLS), bf),
        ((L, 128), f32),
        ((2, L, COLS), bf),
        ((L, D), f32),
        ((L, D), bf),
        ((2, L, COLS), bf),
        ((2, KEYS, D), bf),
        ((2, 2, KEYS, COLS), bf),
        ((2, 2, KEYS, COLS), bf),
        ((L, 128), f32),
        ((2, L, COLS), bf),
        ((L, D), f32),
        ((L, D), bf),
        ((2, HALF, D), bf),
        ((8, L, COLS), bf),
        ((8, L, COLS), bf),
        (wide, bf),
    ]
    peers = shards * 2
    scratch = [
        pltpu.VMEM(wide, bf), pltpu.VMEM((2, HALF, D), bf), pltpu.VMEM((2, HALF, D), bf), pltpu.VMEM((2, KEYS, D), bf),
        pltpu.VMEM((16, D), f32), pltpu.VMEM((16, COLS), f32),
        pltpu.VMEM((L, D), bf), pltpu.VMEM((L, D), bf), pltpu.VMEM((L, D), bf),
        pltpu.VMEM((L, D), f32), pltpu.VMEM((L, D), f32),
        pltpu.VMEM((3, 2, 512, COLS), bf), pltpu.VMEM((2, L, COLS), bf), pltpu.VMEM((2, L, COLS), bf),
        pltpu.VMEM((2, L, COLS), bf), pltpu.VMEM((2, 2, KEYS, COLS), bf), pltpu.VMEM((2, 2, KEYS, COLS), bf),
        pltpu.VMEM((L, 128), f32), pltpu.VMEM((L, 128), f32),
        pltpu.VMEM((8, L, COLS), bf), pltpu.VMEM((8, L, COLS), bf),
        pltpu.VMEM((L, 2 * KEYS), f32), pltpu.VMEM((L, 2 * KEYS), bf), pltpu.VMEM((L, D), f32),
        pltpu.VMEM((3, 4, L, COLS), bf), pltpu.VMEM((3, 4, L, COLS), bf),
        pltpu.VMEM((peers, 16, 128) if fast else (1, 16, 128), f32), pltpu.VMEM((8, 2 * KEYS), f32),
        pltpu.VMEM((HALF, D), bf),
        sem((4,)), sem((3,)), sem((3,)), sem((3, 4)), sem((3, 4)), sem((peers,)), sem((peers,)),
        sem((len(shapes),)),
    ]
    outs = pl.pallas_call(
        partial(forward_kernel, levels, groups, fast),
        out_shape=[jax.ShapeDtypeStruct(s, t) for s, t in shapes],
        in_specs=[vm, hbm, hbm, hbm, vm, vm, vm],
        out_specs=[hbm] * len(shapes),
        scratch_shapes=scratch + Gather.semaphores(levels, groups),
        compiler_params=pltpu.CompilerParams(
            collective_id=0, has_side_effects=True, vmem_limit_bytes=63 * 2**20
        ),
        name="forward",
    )(shard, tokens, frames, cotangent, *small)
    return Kept(*outs)


RING = 4


class Scatter:
    def __init__(self, levels, part, own, bufs, sems):
        self.levels, self.part, self.own = levels, part, own
        self.one_y, self.one_x, self.two_x, self.two_y, self.line = bufs
        self.s1, self.r1, self.s2, self.r2, self.s3, self.r3 = sems
        self.at = place()
        self.sent = self.steps = self.ready = 0

    @staticmethod
    def buffers(levels, rows):
        bf, half = jnp.bfloat16, levels // 2
        return [
            pltpu.VMEM((RING, 2, half, rows, COLS), bf), pltpu.VMEM((RING, half, 2, rows, COLS), bf),
            pltpu.VMEM((RING, half, rows, COLS), bf), pltpu.VMEM((RING, half, rows, COLS), bf),
            pltpu.VMEM((RING, levels, rows, COLS), bf),
        ]

    @staticmethod
    def semaphores(levels):
        sem = pltpu.SemaphoreType.DMA
        two = sem((MATS, 2))
        many = sem((MATS, levels))
        return [two, two, two, two, many, many]

    def to_x(self, src, dst, send, recv):
        z, y, x, c = self.at
        return pltpu.make_async_remote_copy(src, dst, send, recv, device_id=device(z, y, 1 - x, c), device_id_type=DT)

    def to_y(self, src, dst, send, recv):
        z, y, x, c = self.at
        return pltpu.make_async_remote_copy(src, dst, send, recv, device_id=device(z, 1 - y, x, c), device_id_type=DT)

    def first(self, g):
        z, y, x, c = self.at
        m, slot = MATS - 1 - g, lax.rem(g, RING)
        return (
            self.to_y(self.part.at[m, :, :, 0, 1 - y], self.one_y.at[slot], self.s1.at[g, 0], self.r1.at[g, 0]),
            self.to_x(self.part.at[m, 1 - x, :, 1], self.one_x.at[slot], self.s1.at[g, 1], self.r1.at[g, 1]),
        )

    def second(self, g):
        z, y, x, c = self.at
        m, slot = MATS - 1 - g, lax.rem(g, RING)
        return (
            self.to_x(self.part.at[m, 1 - x, :, 0, y], self.two_x.at[slot], self.s2.at[g, 0], self.r2.at[g, 0]),
            self.to_y(self.part.at[m, x, :, 1, 1 - y], self.two_y.at[slot], self.s2.at[g, 1], self.r2.at[g, 1]),
        )

    def third(self, g, zz, k):
        z, y, x, c = self.at
        return pltpu.make_async_remote_copy(
            self.part.at[MATS - 1 - g, x, zz // 2, lax.rem(zz, 2), y], self.line.at[lax.rem(g, RING), k],
            self.s3.at[g, zz], self.r3.at[g, k], device_id=device(zz, y, x, c), device_id_type=DT,
        )

    def send(self, count):
        def body(i):
            for copy in self.first(i):
                copy.start()

        start = self.sent
        self.sent += count
        loop(count, lambda i: body(start + i))

    def add(self, at, got):
        self.part[at] = (self.part[at].astype(jnp.float32) + got.astype(jnp.float32)).astype(jnp.bfloat16)

    def step_a(self, g):
        z, y, x, c = self.at
        m, slot = MATS - 1 - g, lax.rem(g, RING)
        along_y, along_x = self.first(g)
        then_x, then_y = self.second(g)
        along_y.wait_recv()
        for k in range(2):
            loop(self.levels // 2, lambda h: self.add((m, k, h, 0, y), self.one_y[slot, k, h]))
        then_x.start()
        along_x.wait_recv()
        for k in range(2):
            loop(self.levels // 2, lambda h: self.add((m, x, h, 1, k), self.one_x[slot, h, k]))
        then_y.start()

    def step_b(self, g):
        z, y, x, c = self.at
        m, slot = MATS - 1 - g, lax.rem(g, RING)
        then_x, then_y = self.second(g)
        then_x.wait_recv()
        loop(self.levels // 2, lambda h: self.add((m, x, h, 0, y), self.two_x[slot, h]))
        then_y.wait_recv()
        loop(self.levels // 2, lambda h: self.add((m, x, h, 1, y), self.two_y[slot, h]))
        loop(self.levels - 1, lambda k: self.third(g, lax.rem(z + k + 1, self.levels), z).start())

    def step_c(self, g):
        z, y, x, c = self.at
        m = MATS - 1 - g
        loop(self.levels - 1, lambda k: self.third(g, z, lax.rem(z + k + 1, self.levels)).wait_recv())
        self.own[m] = self.part[m, x, z // 2, lax.rem(z, 2), y].astype(jnp.float32)

        def body(k):
            @pl.when(k != z)
            def _():
                self.own[m] += self.line[lax.rem(g, RING), k].astype(jnp.float32)

        loop(self.levels, body)

    def step(self, t):
        @pl.when(t < MATS)
        def _():
            self.step_a(t)

        @pl.when((t >= 1) & (t <= MATS))
        def _():
            self.step_b(t - 1)

        @pl.when(t >= 2)
        def _():
            self.step_c(t - 2)

    def turn(self, count):
        start, first = self.steps, self.sent
        self.steps += count
        self.sent = max(first, min(MATS, self.steps + RING - 2))
        assert self.sent <= self.ready

        def body(i):
            t = start + i
            self.step(t)
            g = t + RING - 2

            @pl.when((g >= first) & (g < MATS))
            def _():
                for copy in self.first(g):
                    copy.start()

        return body

    def run(self, count):
        loop(count, self.turn(count))

    def drain(self):
        z, y, x, c = self.at

        def body(g):
            for copy in (*self.first(g), *self.second(g)):
                copy.wait_send()
            loop(self.levels - 1, lambda k: self.third(g, lax.rem(z + k + 1, self.levels), z).wait_send())

        loop(MATS, body)


class BackwardIn(NamedTuple):
    dy: object
    wide: object
    slope: object
    z: object
    a3: object
    h2: object
    norm: object
    c2: object
    q2: object
    lse2: object
    ek: object
    ev: object
    e: object
    a2: object
    h1: object
    c1: object
    qkv: object
    lse1: object
    a1: object
    x: object
    mean_attn: object
    mean_dense: object
    square_attn: object
    square_dense: object
    shard: object
    pack: object
    pack_mean: object
    pack_square: object


class BackwardOut(NamedTuple):
    owned_attn: object
    owned_dense: object
    input_out: object
    frame_out: object
    small_out: object
    bcols_out: object
    mean_attn: object
    mean_dense: object
    square_attn: object
    square_dense: object
    step_attn: object
    step_dense: object
    small_mean: object
    small_square: object
    small_step: object
    norms: object


class BackwardRefs(NamedTuple):
    owned_attn: object
    owned_dense: object
    input_out: object
    frame_out: object
    small_out: object
    bcols_out: object
    mean_attn: object
    mean_dense: object
    square_attn: object
    square_dense: object
    step_attn: object
    step_dense: object
    small_mean: object
    small_square: object
    small_step: object
    norms: object
    part: object
    own: object
    dy: object
    slope: object
    z: object
    left: object
    h: object
    norm: object
    c2: object
    q2: object
    lse2: object
    ek: object
    ev: object
    e: object
    a2: object
    c1: object
    qkv: object
    lse1: object
    x: object
    dh: object
    dhb: object
    dc: object
    stat: object
    s: object
    dp: object
    p: object
    ds: object
    mine: object
    got: object
    fsend: object
    frecv: object
    fout: object
    cols: object
    bcols: object
    small: object
    smallgot: object
    smallsum: object
    in_sem: object
    trade_send: object
    trade_recv: object
    frame_send: object
    frame_recv: object
    frame_out_sem: object
    small_send: object
    small_recv: object
    out_sem: object
    moments: object
    held: object
    squares: object
    sums: object
    sumsgot: object
    sumspair: object
    load_sem: object
    store_sem: object
    step_sem: object
    pair_sem: object
    sums_send: object
    sums_recv: object


def backward_kernel(levels, fast, token_total, *refs):
    f32, bf = jnp.float32, jnp.bfloat16
    at, width = len(BackwardIn._fields), len(BackwardRefs._fields)
    given = BackwardIn(*refs[:at])
    r = BackwardRefs(*refs[at : at + width])
    rest = refs[at + width :]
    scatter = Scatter(levels, r.part, r.own, rest[:5], rest[5:])
    z, y, x, c = place()
    dp = z * 2 + y
    mate = (dp, x, 1 - c)
    count = levels * 4
    me = dp * 2 + x
    rows_of = D // (levels * 2)
    per = COLS // (2 * rows_of)

    def peer(i):
        return (i // 2, lax.rem(i, 2), c)

    loads = []

    def load(src, dst):
        loads.append(pltpu.make_async_copy(src, dst, r.in_sem.at[len(loads)]))
        loads[-1].start()
        return loads[-1]

    def loaded(*which):
        for copy in which:
            copy.wait()

    get_dy = load(given.dy, r.dy)
    get_w2 = load(given.wide.at[12:16], r.part.at[12:16])
    get_slope = load(given.slope, r.slope)
    get_z = load(given.z, r.z)
    get_w1 = load(given.wide.at[8:12], r.part.at[8:12])
    get_a3 = load(given.a3, r.left)
    get_h2 = load(given.h2, r.h)
    get_w0 = load(given.wide.at[0:8], r.part.at[0:8])
    get_norm = load(given.norm, r.norm)
    get_c2 = load(given.c2, r.c2)
    get_q2 = load(given.q2, r.q2)
    get_lse2 = load(given.lse2, r.lse2)
    get_ek = load(given.ek, r.ek)
    get_ev = load(given.ev, r.ev)
    get_e = load(given.e, r.e)
    get_a2 = load(given.a2, r.a2)
    get_c1 = load(given.c1, r.c1)
    get_qkv = load(given.qkv, r.qkv)
    get_lse1 = load(given.lse1, r.lse1)
    get_x = load(given.x, r.x)

    bar = pltpu.get_barrier_semaphore()
    loop(count - 1, lambda k: pl.semaphore_signal(
        bar, inc=1, device_id=peer(lax.rem(me + k + 1, count)), device_id_type=DT))
    pl.semaphore_signal(bar, inc=1, device_id=mate, device_id_type=DT)
    pl.semaphore_wait(bar, count)

    def remote(src, dst, send, recv, dev):
        return pltpu.make_async_remote_copy(src, dst, send, recv, device_id=dev, device_id_type=DT)

    def trade(n, j):
        return remote(r.mine.at[n % 2, j], r.got.at[n % 2, j], r.trade_send.at[n, j],
                      r.trade_recv.at[n, j], mate)

    def panel(mat, side):
        return r.part[mat, side].reshape(D, COLS)

    def part_rows(mat, side, j):
        if per == 1:
            return r.part[mat, side, j // 2, lax.rem(j, 2)].reshape(COLS, COLS)
        return r.part[mat, side, pl.ds(j * (per // 2), per // 2)].reshape(COLS, COLS)

    def grads(lefts, items):
        def body(j):
            cols = pl.ds(pl.multiple_of(j * COLS, COLS), COLS)
            turned = [v.T for v in lefts(cols)]
            for mat, side, rights in items:
                acc = None
                for t, right in zip(turned, rights()):
                    more = dot(t, right, NN)
                    acc = more if acc is None else acc + more
                if per == 1:
                    r.part[mat, side, j // 2, lax.rem(j, 2)] = acc.astype(bf).reshape(2, rows_of, COLS)
                else:
                    blocks = pl.ds(j * (per // 2), per // 2)
                    r.part[mat, side, blocks] = acc.astype(bf).reshape(per // 2, 2, 2, rows_of, COLS)

        loop(4, body)

    def send_back(n, items):
        if n >= 2:
            loop(4, lambda j: trade(n - 2, j).wait_send())

        def body(j):
            acc = None
            for value, mat, side in items:
                more = dot(value(), part_rows(mat, side, j), NT)
                acc = more if acc is None else acc + more
            r.mine[n % 2, j] = acc.astype(bf)
            trade(n, j).start()

        loop(4, body)

    def fold(v):
        return jnp.sum(v.reshape(BLOCK // 8, 8, D), axis=0)

    def norm_row(k):
        return r.norm[k : k + 1, :]

    def grow(k, v):
        r.cols[k * 8 : (k + 1) * 8, :] += fold(v)

    def half_rows(ref, i):
        half = i // (HALF // BLOCK)
        inner = pl.ds(pl.multiple_of((i - half * (HALF // BLOCK)) * BLOCK, BLOCK), BLOCK)
        return ref[half, inner, :].astype(f32)

    def norm_back(n, k, base, incoming, sum_k):
        loop(4, lambda j: trade(n, j).wait_recv())

        def body(rows, i):
            normed, scaled = normed_block(base(rows, i))
            dn = panels_row(r.mine.at[n % 2], rows) + panels_row(r.got.at[n % 2], rows)
            inner = dn * norm_row(k)
            back = scaled * (
                inner - jnp.mean(inner, axis=-1, keepdims=True)
                - normed * jnp.mean(inner * normed, axis=-1, keepdims=True)
            )
            came = incoming(rows, i)
            out = came + back
            r.dh[rows, :] = out
            grow(k, dn * normed)
            grow(k + 1, dn)
            if sum_k is not None:
                r.dhb[rows, :] = out.astype(bf)
                grow(sum_k, out)
            if n == 0:
                grow(8, came)

        rows_loop(L, body, NORM_TURNS)

    r.cols[...] = jnp.zeros((72, D), f32)
    loaded(get_dy, get_w2, get_slope)

    def hidden_back(t):
        m, side = t // 2, lax.rem(t, 2)
        du = (dot(r.dy[...].reshape(L, D), panel(12 + m, side), NN) * r.slope[t].astype(f32)).astype(bf)
        r.slope[t] = du
        r.bcols[pl.ds(8 + t, 1), :] = jnp.sum(du.astype(f32), axis=0, keepdims=True)

    loop(8, hidden_back)
    loaded(get_z)
    grads(
        lambda cols: [r.dy[:, :, cols].reshape(L, COLS)],
        [(12 + t // 2, t % 2, lambda t=t: [r.z[t]]) for t in range(8)],
    )
    scatter.send(4)
    loaded(get_w1)
    send_back(0, [(lambda t=t: r.slope[t], 8 + t // 2, t % 2) for t in range(8)])
    loaded(get_a3, get_h2, get_norm)
    grads(
        lambda cols: [r.left[:, cols]],
        [(8 + t // 2, t % 2, lambda t=t: [r.slope[t]]) for t in range(8)],
    )
    scatter.ready = 8
    get_a1 = load(given.a1, r.left)
    norm_back(0, 4, lambda rows, i: r.h[rows, :], lambda rows, i: half_rows(r.dy, i), 7)
    get_h1 = load(given.h1, r.h)
    scatter.run(1)
    loaded(get_w0)

    def context_back(mat):
        def body(side):
            r.dc[side] = dot(r.dhb[...], panel(mat, side), NN).astype(bf)

        loop(2, body)

    def statistics(lse, ctx):
        r.stat[0:8, :] = lse[...].T[0:8, :]
        for side in range(2):
            both = (r.dc[side].astype(f32) * ctx[side].astype(f32)).T
            r.stat[8 + side * 4 : 12 + side * 4, :] = jnp.sum(both.reshape(4, HD, L), axis=1)

    lane = lax.broadcasted_iota(jnp.int32, (1, 128), 1)
    low = lane < HD
    low_row = lax.broadcasted_iota(jnp.int32, (128, 1), 0) < HD

    def attend_back(query, keys, values, parts, width, causal, turn):
        def body(t):
            side, half = t // 2, lax.rem(t, 2)
            lanes = pl.ds(pl.multiple_of(half * 128, 128), 128)
            q = query[(side, slice(0, L), lanes)].astype(f32) * 0.125
            dc = r.dc[side, :, lanes].astype(f32)
            back = None
            for n in range(parts):
                at = (side, n, slice(None), lanes) if parts > 1 else (side, slice(0, L), lanes)
                k, v = keys[at], values[at]
                flat = k.T
                dk = dv = None
                for sub in range(2):
                    mine = low if sub == 0 else jnp.logical_not(low)
                    mine_row = low_row if sub == 0 else jnp.logical_not(low_row)
                    qh = jnp.where(mine, q, 0.0).astype(bf)
                    dm = jnp.where(mine, dc, 0.0).astype(bf)
                    kt = jnp.where(mine_row, flat.astype(f32), 0.0).astype(bf)
                    r.s[0:width, :] = dot(k, qh, NT)
                    r.dp[0:width, :] = dot(v, dm, NT)
                    lse = r.stat[pl.ds(t * 2 + sub, 1), :]
                    delta = r.stat[pl.ds(8 + t * 2 + sub, 1), :]

                    def rows_body(rows, i):
                        key = i * BLOCK + lax.broadcasted_iota(jnp.int32, (BLOCK, L), 0)
                        if causal:
                            keep = lax.broadcasted_iota(jnp.int32, (BLOCK, L), 1) >= key
                        else:
                            keep = key < HALF_FRAMES
                        p = jnp.where(keep, jnp.exp(jnp.where(keep, r.s[rows, :], -1e30) - lse), 0.0)
                        r.p[rows, :] = p.astype(bf)
                        r.ds[rows, :] = (p * (r.dp[rows, :] - delta)).astype(bf)

                    rows_loop(width, rows_body, 14 if causal else BACK_TURNS)
                    p, ds = r.p[0:width, :], r.ds[0:width, :]
                    dv = dot(p, dm, NN) if dv is None else dv + dot(p, dm, NN)
                    dk = dot(ds, qh, NN) if dk is None else dk + dot(ds, qh, NN)
                    more = dot(kt, ds, NN)
                    back = more if back is None else back + more
                keys[at] = dk.astype(bf)
                values[at] = dv.astype(bf)
            query[(side, slice(0, L), lanes)] = (back.T * 0.125).astype(bf)
            turn(t)

        loop(4, body)

    def column(k, ref, at):
        def body(side):
            r.bcols[pl.ds(k * 2 + side, 1), :] = jnp.sum(ref[at(side)].astype(f32), axis=0, keepdims=True)

        loop(2, body)

    context_back(7)
    loaded(get_c2, get_lse2)
    statistics(r.lse2, r.c2)
    grads(
        lambda cols: [r.dhb[:, cols]], [(7, side, lambda side=side: [r.c2[side]]) for side in range(2)]
    )
    scatter.ready = 9
    scatter.run(1)
    loaded(get_q2, get_ek, get_ev)
    attend_back(r.q2, r.ek, r.ev, 2, KEYS, False, scatter.turn(4))

    loaded(get_e, get_a2)

    def frame_share(half, j):
        acc = None
        for mat, ref in ((5, r.ek), (6, r.ev)):
            for side in range(2):
                more = dot(ref[side, half], part_rows(mat, side, j), NT)
                acc = more if acc is None else acc + more
        return acc

    def frame_trade(j):
        return remote(r.fsend.at[j], r.frecv.at[j], r.frame_send.at[j], r.frame_recv.at[j], mate)

    def frame_store(j):
        cols = pl.ds(pl.multiple_of(j * COLS, COLS), COLS)
        return pltpu.make_async_copy(r.fout.at[lax.rem(j, 2)], r.frame_out.at[:, cols], r.frame_out_sem.at[j])

    def frame_far(j):
        r.fsend[j] = frame_share(1 - c, j).astype(bf)
        frame_trade(j).start()

    def frame_near(j):
        @pl.when(j >= 2)
        def _():
            frame_store(j - 2).wait()

        frame_trade(j).wait_recv()
        r.fout[lax.rem(j, 2)] = (frame_share(c, j) + r.frecv[j].astype(f32))[0:HALF_FRAMES]
        frame_store(j).start()

    loop(4, frame_far)
    send_back(1, [(lambda side=side: r.q2[side], 4, side) for side in range(2)])
    loop(4, frame_near)
    scatter.run(1)
    grads(
        lambda cols: [r.e[n, :, cols] for n in range(2)],
        [(5 + i, side, lambda ref=ref, side=side: [ref[side, n] for n in range(2)])
         for i, ref in ((1, r.ev), (0, r.ek)) for side in range(2)],
    )
    scatter.ready = 11
    scatter.run(1)
    column(2, r.q2, lambda side: (side,))

    def value_column(side):
        total = sum(jnp.sum(r.ev[side, n].astype(f32), axis=0, keepdims=True) for n in range(2))
        r.bcols[pl.ds(6 + side, 1), :] = total

    loop(2, value_column)
    grads(lambda cols: [r.a2[:, cols]], [(4, side, lambda side=side: [r.q2[side]]) for side in range(2)])
    scatter.ready = 12
    loaded(get_h1)
    norm_back(1, 2, lambda rows, i: r.h[rows, :], lambda rows, i: r.dh[rows, :], 6)
    scatter.run(1)
    context_back(3)
    loaded(get_c1, get_lse1)
    statistics(r.lse1, r.c1)
    grads(
        lambda cols: [r.dhb[:, cols]], [(3, side, lambda side=side: [r.c1[side]]) for side in range(2)]
    )
    scatter.ready = 13
    scatter.run(1)
    loaded(get_qkv)
    q_ref, k_ref, v_ref = (r.qkv.at[i] for i in range(3))
    attend_back(q_ref, k_ref, v_ref, 1, L, True, lambda t: None)
    send_back(2, [(lambda i=i, side=side: r.qkv[i, side, 0:L, :], i, side) for i in range(3) for side in range(2)])
    loaded(get_a1)
    grads(
        lambda cols: [r.left[:, cols]],
        [(i, side, lambda i=i, side=side: [r.qkv[i, side, 0:L, :]]) for i in (2, 1, 0) for side in range(2)],
    )
    scatter.ready = 16
    scatter.run(1)
    column(0, q_ref, lambda side: (side, slice(0, L)))
    column(1, v_ref, lambda side: (side, slice(0, L)))
    loaded(get_x)
    norm_back(2, 0, lambda rows, i: half_rows(r.x, i), lambda rows, i: r.dh[rows, :], None)
    own_rows = pl.ds(pl.multiple_of(c * HALF, HALF), HALF)
    input_copy = pltpu.make_async_copy(r.dh.at[own_rows], r.input_out, r.out_sem.at[0])
    input_copy.start()

    sums = jnp.concatenate([jnp.sum(r.cols[k * 8 : k * 8 + 8, :], axis=0, keepdims=True) for k in range(9)], axis=0)
    if fast:
        r.small[...] = jnp.zeros(r.small.shape, f32)
        for i in range(2 * levels):
            for xx in range(2):
                k = i * 2 + xx
                r.small[k, 0:9, :] = sums[:, i * 128 : (i + 1) * 128]
                r.small[k, 9:10, :] = r.bcols[k : k + 1, 0:128]
                r.small[k, 10:11, :] = r.bcols[k : k + 1, 128:256]

        def small_copy(k, slot):
            i = lax.rem(me + k + 1, count)
            return remote(r.small.at[i], r.smallgot.at[slot], r.small_send.at[k], r.small_recv.at[slot],
                          peer(i))

        loop(count - 1, lambda k: small_copy(k, me).start())
        r.smallgot[me] = r.small[me]
    else:
        r.smallsum[0:9, :] = sums

    def either(m, attn, dense, action):
        @pl.when(m < 8)
        def _():
            action(attn())

        @pl.when(m >= 8)
        def _():
            action(dense())

    def moment_loads(g, action):
        m, slot = MATS - 1 - g, lax.rem(g, 2)
        for k, (attn, dense) in enumerate(
            ((given.mean_attn, given.mean_dense), (given.square_attn, given.square_dense))
        ):
            def copy(src, at):
                return pltpu.make_async_copy(src.at[at], r.moments.at[slot, k], r.load_sem.at[slot, k])

            either(m, lambda: copy(attn, m), lambda: copy(dense, m - 8), action)
        action(pltpu.make_async_copy(given.shard.at[m], r.held.at[slot], r.load_sem.at[slot, 2]))

    def moment_stores(g, action):
        m, slot = MATS - 1 - g, lax.rem(g, 2)
        for k, (attn, dense) in enumerate(((r.mean_attn, r.mean_dense), (r.square_attn, r.square_dense))):
            def copy(dst, at):
                return pltpu.make_async_copy(r.moments.at[slot, k], dst.at[at], r.store_sem.at[slot, k])

            either(m, lambda: copy(attn, m), lambda: copy(dense, m - 8), action)

    def begin(copy):
        copy.start()

    def end(copy):
        copy.wait()

    def whole_store(m, attn, dense, action):
        def copy(dst, at):
            return pltpu.make_async_copy(r.own.at[m], dst.at[at], r.step_sem.at[m])

        either(m, lambda: copy(attn, m), lambda: copy(dense, m - 8), action)

    def adapted(gradient, moment, second, weight):
        scaled = gradient / token_total
        moment = 0.5 * moment + 0.5 * scaled
        second = 0.5 * second + 0.5 * scaled * scaled
        return moment, second, moment / (jnp.sqrt(second) + 1e-06) + 0.01 * weight

    def update(g):
        m, slot = MATS - 1 - g, lax.rem(g, 2)
        whole_store(m, r.owned_attn, r.owned_dense, begin)
        moment_loads(g, end)

        @pl.when(g >= 1)
        def _():
            moment_stores(g - 1, end)

        @pl.when(g + 1 < MATS)
        def _():
            moment_loads(g + 1, begin)

        whole_store(m, r.owned_attn, r.owned_dense, end)
        r.squares[pl.ds(m, 1), :] = jnp.zeros((1, COLS), f32)
        r.squares[pl.ds(MATS + m, 1), :] = jnp.zeros((1, COLS), f32)

        def block(rows, i):
            weight = r.held[slot, rows, :].astype(f32)
            moment, second, direction = adapted(
                r.own[m, rows, :], r.moments[slot, 0, rows, :], r.moments[slot, 1, rows, :], weight
            )
            r.moments[slot, 0, rows, :] = moment
            r.moments[slot, 1, rows, :] = second
            r.own[m, rows, :] = direction
            r.squares[pl.ds(m, 1), :] += jnp.sum(direction * direction, axis=0, keepdims=True)
            r.squares[pl.ds(MATS + m, 1), :] += jnp.sum(weight * weight, axis=0, keepdims=True)

        rows_loop(rows_of, block, 2)
        moment_stores(g, begin)

    if fast:
        moment_loads(0, begin)
        updated = scatter.steps - 2
        loop(updated, update)
        left = MATS + 2 - scatter.steps
        final = scatter.turn(left)

        def last_turn(i):
            final(i)
            update(updated + i)

        loop(left, last_turn)
    else:
        scatter.run(MATS + 2 - scatter.steps)
        for k, dst in enumerate((r.owned_attn, r.owned_dense)):
            copy = pltpu.make_async_copy(r.own.at[8 * k : 8 * k + 8], dst, r.step_sem.at[k])
            copy.start()
            copy.wait()
    if fast:
        loop(count - 1, lambda k: small_copy(k, lax.rem(me + k + 1, count)).wait_recv())
        total = r.smallgot[0]
        for k in range(1, 4 * levels):
            total = total + r.smallgot[k]
        r.smallsum[...] = total
        moment, second, direction = adapted(total, given.pack_mean[...], given.pack_square[...], given.pack[...])
        r.small_mean[...] = moment
        r.small_square[...] = second
        lanes = lax.broadcasted_iota(jnp.int32, (1, 128), 1)
        wide_lane = lax.broadcasted_iota(jnp.int32, (16, 128), 1)
        row = lax.broadcasted_iota(jnp.int32, (16, 128), 0)
        place_of = jnp.where(row < 9, 18 + row, jnp.where(row < 11, 10 + dp, 127))
        counted = jnp.where(row < 9, jnp.where((x == 0) & (c == 0), 1.0, 0.0), 1.0)

        def spread(first_row, small):
            line = jnp.zeros((1, 128), f32)
            for m in range(MATS):
                k = first_row + m
                one = jnp.sum(r.squares[k : k + 1, :], axis=1, keepdims=True)
                line = line + jnp.where(lanes == (m if m < 8 else 8 + (m - 8) // 4), one, 0.0)
            per_row = jnp.sum(small * small * counted, axis=1, keepdims=True)
            return line + jnp.sum(jnp.where(wide_lane == place_of, per_row, 0.0), axis=0, keepdims=True)

        r.sums[0, 0:1, :] = spread(MATS, given.pack[...])
        r.sums[0, 1:2, :] = spread(0, direction)
        pair = remote(r.sums.at[0], r.sumspair, r.pair_sem.at[0], r.pair_sem.at[1], mate)
        pair.start()
        pair.wait_recv()
        r.sums[1] = r.sums[0] + r.sumspair[...]

        def sums_copy(k, slot):
            return remote(r.sums.at[1], r.sumsgot.at[slot], r.sums_send.at[k], r.sums_recv.at[slot],
                          peer(lax.rem(me + k + 1, count)))

        loop(count - 1, lambda k: sums_copy(k, me).start())
        r.sumsgot[me] = r.sums[1]
        loop(count - 1, lambda k: sums_copy(k, lax.rem(me + k + 1, count)).wait_recv())
        all_sums = r.sumsgot[0]
        for k in range(1, 4 * levels):
            all_sums = all_sums + r.sumsgot[k]
        norms = jnp.sqrt(all_sums)
        r.norms[...] = norms
        trust = norms[0:1] / norms[1:2]

        def scale(m):
            at = jnp.where(m < 8, m, 8 + (m - 8) // 4)
            factor = -learning_rate * jnp.sum(jnp.where(lanes == at, trust, 0.0), axis=1, keepdims=True)
            r.own[m] = r.own[m] * factor
            whole_store(m, r.step_attn, r.step_dense, begin)

        loop(MATS, scale)
        small_factor = jnp.sum(jnp.where(wide_lane == place_of, trust, 0.0), axis=1, keepdims=True)
        r.small_step[...] = jnp.where(row < 11, -learning_rate * small_factor * direction, 0.0)
        pair.wait_send()
        loop(count - 1, lambda k: small_copy(k, me).wait_send())
        loop(count - 1, lambda k: sums_copy(k, me).wait_send())
        moment_stores(MATS - 1, end)
    small_store = pltpu.make_async_copy(r.smallsum, r.small_out, r.out_sem.at[2])
    bcols_store = pltpu.make_async_copy(r.bcols, r.bcols_out, r.out_sem.at[3])
    small_store.start()
    bcols_store.start()
    small_store.wait()
    bcols_store.wait()
    for n in (1, 2):
        loop(4, lambda j: trade(n, j).wait_send())
    loop(4, lambda j: frame_trade(j).wait_send())
    for j in (2, 3):
        frame_store(j).wait()
    scatter.drain()
    input_copy.wait()
    if fast:
        loop(MATS, lambda m: whole_store(m, r.step_attn, r.step_dense, end))


def backward(kept, state, token_total, shards):
    levels, rows = shards // 2, D // shards
    fast = rows == 128
    f32, bf = jnp.float32, jnp.bfloat16
    sem = pltpu.SemaphoreType.DMA
    hbm = pl.BlockSpec(memory_space=pl.ANY)
    peers = shards * 2
    half = ((8, rows, COLS), f32)
    shapes = [half, half, ((HALF, D), f32), ((HALF_FRAMES, D), f32)]
    shapes += [((16, 128) if fast else (16, D), f32), ((16, COLS), f32)]
    shapes += [half] * 6 + [((16, 128), f32)] * 3 + [((8, 128), f32)]
    small = (peers, 16, 128) if fast else (1, 16, 128)
    vm = pltpu.VMEM
    inside = pl.BlockSpec(memory_space=pltpu.VMEM)
    scratch = [
        vm((MATS, 2, levels // 2, 2, 2, rows, COLS), bf), vm((MATS, rows, COLS), f32), vm((2, HALF, D), bf),
        vm((8, L, COLS), bf), vm((8, L, COLS), bf), vm((L, D), bf), vm((L, D), f32), vm((16, D), f32),
        vm((2, L, COLS), bf), vm((2, L, COLS), bf), vm((L, 128), f32), vm((2, 2, KEYS, COLS), bf),
        vm((2, 2, KEYS, COLS), bf), vm((2, KEYS, D), bf), vm((L, D), bf),
        vm((2, L, COLS), bf), vm((3, 2, 512, COLS), bf), vm((L, 128), f32), vm((2, HALF, D), bf),
        vm((L, D), f32), vm((L, D), bf), vm((2, L, COLS), bf), vm((16, L), f32),
        vm((KEYS, L), f32), vm((KEYS, L), f32), vm((KEYS, L), bf), vm((KEYS, L), bf),
        vm((2, 4, L, COLS), bf), vm((2, 4, L, COLS), bf), vm((4, KEYS, COLS), bf), vm((4, KEYS, COLS), bf),
        vm((2, HALF_FRAMES, COLS), f32), vm((72, D), f32), vm((16, COLS), f32), vm(small, f32), vm(small, f32),
        vm((16, 128) if fast else (16, D), f32),
        sem((24,)), sem((3, 4)), sem((3, 4)), sem((4,)), sem((4,)), sem((4,)), sem((peers,)), sem((peers,)), sem((4,)),
        vm((2, 2, rows, COLS), f32), vm((2, rows, COLS), bf), vm((2 * MATS, COLS), f32), vm((2, 8, 128), f32),
        vm((peers if fast else 1, 8, 128), f32), vm((8, 128), f32), sem((2, 3)), sem((2, 2)), sem((MATS,)), sem((2,)),
        sem((peers,)), sem((peers,)),
    ]
    return pl.pallas_call(
        partial(backward_kernel, levels, fast, token_total),
        out_shape=[jax.ShapeDtypeStruct(s, t) for s, t in shapes],
        in_specs=[hbm] * (len(BackwardIn._fields) - 3) + [inside] * 3,
        out_specs=[hbm] * (len(shapes) - 4) + [inside] * 4,
        scratch_shapes=scratch + Scatter.buffers(levels, rows) + Scatter.semaphores(levels),
        compiler_params=pltpu.CompilerParams(
            collective_id=1, has_side_effects=True, vmem_limit_bytes=63 * 2**20
        ),
        name="backward",
    )(
        kept.dy, kept.wide.reshape(MATS, 2, levels // 2, 2, 2, rows, COLS), kept.slope, kept.z, kept.a3, kept.h2, kept.norm, kept.c2, kept.q2, kept.lse2,
        kept.ek, kept.ev, kept.e, kept.a2, kept.h1, kept.c1, kept.qkv, kept.lse1, kept.a1, kept.x, *state,
    )


def small_kernel(shards, every, scatter, src, out, own_sem, send_sem, recv_sem):
    dp, x, c = (lax.axis_index(a) for a in AXES)
    cores = 2 if every else 1
    count = shards * 2 * cores
    me = (dp * 2 + x) * cores + (c if every else 0)

    def peer(i):
        if every:
            return (i // 4, lax.rem(i // 2, 2), lax.rem(i, 2))
        return (i // 2, lax.rem(i, 2), c)

    bar = pltpu.get_barrier_semaphore()

    def greet(k, carry):
        pl.semaphore_signal(bar, inc=1, device_id=peer(lax.rem(me + k, count)), device_id_type=DT)
        return carry

    lax.fori_loop(1, count, greet, 0)
    pl.semaphore_wait(bar, count - 1)

    def copy(k):
        i = lax.rem(me + k, count)
        return pltpu.make_async_remote_copy(
            src.at[i] if scatter else src, out.at[me], send_sem.at[k], recv_sem.at[me],
            device_id=peer(i), device_id_type=DT,
        )

    def send(k, carry):
        copy(k).start()
        return carry

    own = pltpu.make_async_copy(src.at[me] if scatter else src, out.at[me], own_sem)
    own.start()
    lax.fori_loop(1, count, send, 0)
    own.wait()

    def finish(k, carry):
        i = lax.rem(me + k, count)
        pltpu.make_async_remote_copy(
            src.at[i] if scatter else src, out.at[i], send_sem.at[k], recv_sem.at[i],
            device_id=peer(i), device_id_type=DT,
        ).wait_recv()
        copy(k).wait_send()
        return carry

    lax.fori_loop(1, count, finish, 0)


def small_exchange(src, shards, every, scatter, call_id):
    count = shards * 2 * (2 if every else 1)
    shape = src.shape[1:] if scatter else src.shape
    sem = pltpu.SemaphoreType.DMA
    vm = pl.BlockSpec(memory_space=pltpu.VMEM)
    return pl.pallas_call(
        partial(small_kernel, shards, every, scatter),
        out_shape=jax.ShapeDtypeStruct((count, *shape), src.dtype),
        in_specs=[vm],
        out_specs=vm,
        scratch_shapes=[sem, sem((count,)), sem((count,))],
        compiler_params=pltpu.CompilerParams(collective_id=call_id, has_side_effects=True),
        name=f"small_exchange_{call_id}",
    )(src)


def adapt(weight, gradient, moment, second, token_total):
    scaled_grad = gradient / token_total
    new_moment = 0.5 * moment + 0.5 * scaled_grad
    new_second = 0.5 * second + 0.5 * scaled_grad * scaled_grad
    direction = new_moment / (jnp.sqrt(new_second) + 1e-06) + 0.01 * weight
    return (new_moment, new_second, direction)


def shards_fn(
    tokens, frames, cotangent, attention_weights, dense_weights, unit_bias, norm_bias,
    attention_mean, dense_mean, unit_mean, norm_mean,
    attention_square, dense_square, unit_square, norm_square,
):
    f32, bf = jnp.float32, jnp.bfloat16
    shards = lax.axis_size("dp")
    rows = D // shards
    c = lax.axis_index("core")
    unit_cols = unit_bias.shape[1]
    column_rows = (lax.axis_index("dp") * unit_cols + jnp.arange(unit_cols, dtype=jnp.int32)) // HD
    row_pick = (column_rows[:, None] == jnp.arange(8, dtype=jnp.int32)[None, :]).astype(f32)
    leader = ((lax.axis_index("side") == 0) & (c == 0)).astype(f32)

    def square_rows(attn_part, dense_part, unit_part, norm_part):
        unit_sums = jnp.sum(jnp.sum(unit_part * unit_part, axis=0)[:, None] * row_pick, axis=0)
        return jnp.concatenate(
            [
                jnp.sum(attn_part * attn_part, axis=(2, 3)).reshape(8),
                jnp.sum(dense_part * dense_part, axis=(1, 2, 3)),
                unit_sums,
                jnp.sum(norm_part * norm_part, axis=1) * leader,
            ]
        )

    own_attn = attention_weights.astype(f32)
    own_dense = dense_weights.astype(f32)
    own_unit = unit_bias.astype(f32)
    own_norm = norm_bias.astype(f32)

    if rows == 128:
        pack = jnp.concatenate([norm_bias.astype(f32), unit_bias.astype(f32).reshape(2, 128)])
        small = (jnp.pad(pack, ((0, 5), (0, 0))), jnp.zeros((8, 128), f32), jnp.zeros((8, 128), f32))
    else:
        pack = jnp.concatenate([norm_bias.reshape(-1), unit_bias.reshape(-1)])
        pack = jnp.pad(pack, (0, 2048 - pack.shape[0])).reshape(16, 128)
        packs = small_exchange(pack, shards, False, False, 2).reshape(shards, 2, 2048)
        norm_rows = packs[:, 0, : 9 * rows].reshape(shards, 9, rows).transpose(1, 0, 2).reshape(9, D).astype(f32)
        unit_all = packs[:, :, 9 * rows : 9 * rows + 4 * unit_cols].reshape(shards, 2, 4, unit_cols)
        bias_rows = (
            unit_all.transpose(1, 2, 0, 3).reshape(2, 4, 8, HD).transpose(2, 0, 1, 3).reshape(16, COLS).astype(f32)
        )
        small = (jnp.zeros((16, 128), f32), jnp.pad(norm_rows, ((0, 7), (0, 0))), bias_rows)

    shard = jnp.concatenate(
        [attention_weights.reshape(8, rows, COLS), dense_weights.transpose(0, 2, 1, 3).reshape(8, rows, COLS)]
    )
    kept = forward(shard, tokens, jnp.pad(frames, ((0, KEYS - HALF_FRAMES), (0, 0))), cotangent, small, shards)
    layer_out = kept.layer_out
    def by_matrix(attn, dense):
        return attn.reshape(8, rows, COLS), dense.transpose(0, 2, 1, 3).reshape(8, rows, COLS)

    def from_matrix(attn, dense):
        return attn.reshape(2, 4, rows, COLS), dense.reshape(2, 4, rows, COLS).transpose(0, 2, 1, 3)

    def small_pack(norm, unit):
        if rows != 128:
            return jnp.zeros((16, 128), f32)
        return jnp.pad(jnp.concatenate([norm, unit.reshape(2, 128)]), ((0, 5), (0, 0)))

    def from_pack(pack):
        return pack[9:11].reshape(4, unit_cols), pack[:9]

    token_total = float(tokens.shape[0] * shards * 4)
    state = (
        *by_matrix(attention_mean, dense_mean), *by_matrix(attention_square, dense_square), shard, small[0],
        small_pack(norm_mean, unit_mean), small_pack(norm_square, unit_square),
    )
    done = BackwardOut(*backward(kept, state, token_total, shards))
    input_gradient, frame_gradient = done.input_out, done.frame_out
    attention_owned, dense_owned = from_matrix(done.owned_attn, done.owned_dense)
    small_grads = (done.small_out, done.bcols_out)

    if rows == 128:
        unit_owned, norm_owned = from_pack(done.small_out)
        means = (*from_matrix(done.mean_attn, done.mean_dense), *from_pack(done.small_mean))
        seconds = (*from_matrix(done.square_attn, done.square_dense), *from_pack(done.small_square))
        steps = (*from_matrix(done.step_attn, done.step_dense), *from_pack(done.small_step))
        return (
            layer_out, input_gradient, frame_gradient, attention_owned, dense_owned, unit_owned, norm_owned,
            *means, *seconds, *steps, done.norms[0, :27], done.norms[1, :27],
        )
    else:
        norm_parts = small_grads[0][:9].reshape(9, shards, rows).transpose(1, 0, 2).reshape(shards, 1, 9 * rows)
        unit_parts = small_grads[1].reshape(8, 2, 4, HD).transpose(1, 2, 0, 3).reshape(2, 4, shards, unit_cols)
        unit_parts = unit_parts.transpose(2, 0, 1, 3).reshape(shards, 2, 4 * unit_cols)
        small = jnp.concatenate([jnp.broadcast_to(norm_parts, (shards, 2, 9 * rows)), unit_parts], axis=2)
        small = jnp.pad(small, ((0, 0), (0, 0), (0, 2048 - small.shape[2]))).reshape(shards * 2, 16, 128)
        small = jnp.sum(small_exchange(small, shards, False, True, 13), axis=0).reshape(2048)
        norm_owned = small[: 9 * rows].reshape(9, rows)
        unit_owned = small[9 * rows : 9 * rows + 4 * unit_cols].reshape(4, unit_cols)

    attn_moment, attn_second, attn_dir = adapt(
        own_attn, attention_owned, attention_mean, attention_square, token_total
    )
    dense_moment, dense_second, dense_dir = adapt(
        own_dense, dense_owned, dense_mean, dense_square, token_total
    )
    unit_moment, unit_second, unit_dir = adapt(
        own_unit, unit_owned, unit_mean, unit_square, token_total
    )
    norm_moment, norm_second, norm_dir = adapt(
        own_norm, norm_owned, norm_mean, norm_square, token_total
    )
    sums = jnp.concatenate(
        [
            square_rows(own_attn, own_dense, own_unit, own_norm),
            square_rows(attn_dir, dense_dir, unit_dir, norm_dir),
        ]
    )
    sums = jnp.pad(sums, (0, 1024 - 54)).reshape(8, 128)
    sums = jnp.sum(small_exchange(sums, shards, True, False, 14), axis=0).reshape(1024)
    weight_norms = jnp.sqrt(sums[:27])
    step_norms = jnp.sqrt(sums[27:54])
    trust = weight_norms / step_norms
    attention_step = -learning_rate * trust[0:8].reshape(2, 4, 1, 1) * attn_dir
    dense_step = -learning_rate * trust[8:10].reshape(2, 1, 1, 1) * dense_dir
    unit_factor = jnp.sum(row_pick * trust[10:18][None, :], axis=1)
    unit_step = -learning_rate * unit_factor[None, :] * unit_dir
    norm_step = -learning_rate * trust[18:27][:, None] * norm_dir
    return (
        layer_out, input_gradient, frame_gradient,
        attention_owned, dense_owned, unit_owned, norm_owned,
        attn_moment, dense_moment, unit_moment, norm_moment,
        attn_second, dense_second, unit_second, norm_second,
        attention_step, dense_step, unit_step, norm_step,
        weight_norms, step_norms,
    )


def solution(mesh):
    shards = mesh.shape["dp"]
    inner = Mesh(mesh.devices.reshape(shards, 2, 2), AXES)
    tensor = ("side", "core")
    rows = P(("dp", *tensor), None)
    state = (P(None, None, "dp", tensor), P(None, "dp", None, tensor), P(tensor, "dp"), P(None, "dp"))
    return jax.shard_map(
        shards_fn,
        mesh=inner,
        in_specs=(rows, rows, rows) + state * 3,
        out_specs=(rows, rows, rows) + state * 4 + (P(), P()),
        check_vma=False,
    )
```

```python
from functools import partial
from typing import NamedTuple

import jax
import jax.numpy as jnp
from jax import lax
from jax.experimental import pallas as pl
from jax.experimental.pallas import tpu as pltpu
from jax.sharding import Mesh, PartitionSpec as P

D = 1024
HEADS = 16
HD = 64
L = 448
FRAMES = 1500
MATS = 16
COLS = 256

learning_rate = 0.3
DT = pl.DeviceIdType.MESH
AXES = ("dp", "side", "core")


def place():
    dp = lax.axis_index("dp")
    return dp // 2, lax.rem(dp, 2), lax.axis_index("side"), lax.axis_index("core")


def device(z, y, x, c):
    return (z * 2 + y, x, c)


def greet_neighbours(levels):
    z, y, x, c = place()
    bar = pltpu.get_barrier_semaphore()
    pl.semaphore_signal(bar, inc=1, device_id=device(z, y, 1 - x, c), device_id_type=DT)
    pl.semaphore_signal(bar, inc=1, device_id=device(z, 1 - y, x, c), device_id_type=DT)

    @pl.when(z > 0)
    def _():
        pl.semaphore_signal(bar, inc=1, device_id=device(z - 1, y, x, c), device_id_type=DT)

    @pl.when(z < levels - 1)
    def _():
        pl.semaphore_signal(bar, inc=1, device_id=device(z + 1, y, x, c), device_id_type=DT)

    pl.semaphore_wait(
        bar, 2 + jnp.where(z > 0, 1, 0) + jnp.where(z < levels - 1, 1, 0)
    )


class Gather:
    def __init__(self, levels, groups, shard, wide, sems):
        self.levels, self.groups, self.size = levels, groups, MATS // groups
        self.shard, self.wide = shard, wide
        self.own, self.zs, self.zr, self.xs, self.xr, self.ys, self.yr = sems
        self.at = place()
        self.done = 0
        self.total = (groups + LAG) * levels

    @staticmethod
    def semaphores(levels, groups):
        sem = pltpu.SemaphoreType.DMA
        one, pair = sem((groups, levels)), sem((groups, levels, 2))
        return [sem, pair, one, pair, pair, pair, pair]

    def block(self, g, xx, zz, yy):
        return self.wide.at[pl.ds(g * self.size, self.size), xx, zz, yy]

    def mine(self, g):
        return self.shard.at[pl.ds(g * self.size, self.size)]

    def z_copy(self, g, zz, up, own=False):
        z, y, x, c = self.at
        return pltpu.make_async_remote_copy(
            self.mine(g) if own else self.block(g, x, zz, y), self.block(g, x, zz, y), self.zs.at[g, zz, up],
            self.zr.at[g, zz], device_id=device(z + 1 if up else z - 1, y, x, c), device_id_type=DT,
        )

    def x_copy(self, g, zz, yy, own=False):
        z, y, x, c = self.at
        return pltpu.make_async_remote_copy(
            self.mine(g) if own else self.block(g, x, zz, yy), self.block(g, x, zz, yy), self.xs.at[g, zz, yy],
            self.xr.at[g, zz, yy], device_id=device(z, y, 1 - x, c), device_id_type=DT,
        )

    def y_copy(self, g, zz, xx, own=False):
        z, y, x, c = self.at
        return pltpu.make_async_remote_copy(
            self.mine(g) if own else self.block(g, xx, zz, y), self.block(g, xx, zz, y), self.ys.at[g, zz, xx],
            self.yr.at[g, zz, xx], device_id=device(z, 1 - y, x, c), device_id_type=DT,
        )

    def z_send(self, g):
        z = self.at[0]
        for up in (1, 0):
            @pl.when(z < self.levels - 1 if up else z > 0)
            def _():
                self.z_copy(g, z, up, True).start()

    def begin(self):
        z, y, x, c = self.at
        for g in range(min(Z_AHEAD, self.groups)):
            self.z_send(g)
        self.local = pltpu.make_async_copy(self.shard, self.wide.at[:, x, z, y], self.own)
        self.local.start()

    def first(self, g, d):
        z, y, x, c = self.at

        @pl.when(d == 0)
        def _():
            @pl.when(g + Z_AHEAD < self.groups)
            def _():
                self.z_send(g + Z_AHEAD)

            self.x_copy(g, z, y, True).start()
            self.y_copy(g, z, x, True).start()

        for up in (1, 0):
            zz = z - d if up else z + d

            @pl.when((d > 0) & (zz >= 0 if up else zz < self.levels))
            def _():
                self.z_copy(g, zz, up).wait_recv()

                @pl.when(z < self.levels - 1 if up else z > 0)
                def _():
                    self.z_copy(g, zz, up).start()

                self.x_copy(g, zz, y).start()
                self.y_copy(g, zz, x).start()

    def second(self, g, d):
        z, y, x, c = self.at
        for up in (1, 0):
            zz = z - d if up else z + d
            here = zz >= 0 if up else (zz < self.levels) & (d > 0)
            even = lax.rem(zz + self.levels, 2) == 0

            @pl.when(here & even)
            def _():
                self.x_copy(g, zz, y).wait_recv()
                self.y_copy(g, zz, 1 - x).start()

            @pl.when(here & jnp.logical_not(even))
            def _():
                self.y_copy(g, zz, x).wait_recv()
                self.x_copy(g, zz, 1 - y).start()

    def tick(self, t):
        g, d = t // self.levels, lax.rem(t, self.levels)

        @pl.when((g >= LAG) & (g < self.groups + LAG))
        def _():
            self.second(g - LAG, d)

        @pl.when(g < self.groups)
        def _():
            self.first(g, d)

    def run(self, count):
        count = max(0, min(count, self.total - self.done))
        start = self.done
        self.done += count
        if count:
            loop(count, lambda i: self.tick(start + i))

    def turn(self, count):
        start = self.done
        self.done = min(self.total, self.done + count)
        return lambda i: self.tick(start + i)

    def need(self, mat):
        g = mat // self.size
        self.run((g + 1 + LAG) * self.levels - self.done)
        z, y, x, c = self.at

        def body(zz):
            @pl.when(lax.rem(zz, 2) == 0)
            def _():
                self.y_copy(g, zz, x).wait_recv()
                self.y_copy(g, zz, 1 - x).wait_recv()

            @pl.when(lax.rem(zz, 2) == 1)
            def _():
                self.x_copy(g, zz, y).wait_recv()
                self.x_copy(g, zz, 1 - y).wait_recv()

        if mat % self.size == 0:
            loop(self.levels, body)
        if mat == 0:
            self.local.wait()

    def drain(self):
        z, y, x, c = self.at

        def group(g):
            def sent(zz):
                self.x_copy(g, zz, y).wait_send()
                self.y_copy(g, zz, x).wait_send()

                @pl.when(lax.rem(zz, 2) == 0)
                def _():
                    self.y_copy(g, zz, 1 - x).wait_send()

                @pl.when(lax.rem(zz, 2) == 1)
                def _():
                    self.x_copy(g, zz, 1 - y).wait_send()

            loop(self.levels, sent)

            def relayed(zz):
                @pl.when((z < self.levels - 1) & (zz <= z))
                def _():
                    self.z_copy(g, zz, 1).wait_send()

                @pl.when((z > 0) & (zz >= z))
                def _():
                    self.z_copy(g, zz, 0).wait_send()

            loop(self.levels, relayed)

        loop(self.groups, group)


LAG = 2
Z_AHEAD = 1
GROUPS = 8
HALF = L // 2
KEYS = 768
HALF_FRAMES = FRAMES // 2
BLOCK = 32
SOFT_TURNS = 14
NORM_TURNS = 7
BACK_TURNS = 6


def dot(a, b, dims):
    return lax.dot_general(a, b, (dims, ((), ())), preferred_element_type=jnp.float32)


NN, NT, TN = ((1,), (0,)), ((1,), (1,)), ((0,), (0,))


def flat_panel(ref, mat, side):
    return ref[mat, side].reshape(D, COLS)


def flat_rows(panel, j):
    per = COLS // (2 * panel.shape[2])
    return panel[pl.ds(j * per, per)].reshape(COLS, COLS)


def rows_loop(count, body, turns=1):
    def run(k, carry):
        for u in range(turns):
            i = k * turns + u
            body(pl.ds(pl.multiple_of(i * BLOCK, BLOCK), BLOCK), i)
        return carry

    lax.fori_loop(0, count // (BLOCK * turns), run, 0)


def loop(count, body):
    def run(i, carry):
        body(i)
        return carry

    lax.fori_loop(0, count, run, 0)


def normed_block(values):
    centre = values - jnp.mean(values, axis=-1, keepdims=True)
    spread = jnp.mean(centre * centre, axis=-1, keepdims=True)
    scaled = lax.rsqrt(spread + 1e-05)
    return centre * scaled, scaled


def panels_row(ref, rows):
    return jnp.concatenate([ref[j, rows, :].astype(jnp.float32) for j in range(4)], axis=1)


def forward_kernel(levels, groups, fast, *refs):
    f32, bf = jnp.float32, jnp.bfloat16
    width = len(ForwardRefs._fields)
    r = ForwardRefs(*refs[:width])
    gather = Gather(levels, groups, r.shard, r.wide, refs[width:])
    z, y, x, c = place()
    dp = z * 2 + y
    mate = (dp, x, 1 - c)
    count = levels * 4
    me = dp * 2 + x

    def peer(i):
        return (i // 2, lax.rem(i, 2), c)

    bar = pltpu.get_barrier_semaphore()
    loop(count - 1, lambda k: pl.semaphore_signal(
        bar, inc=1, device_id=peer(lax.rem(me + k + 1, count)), device_id_type=DT))
    pl.semaphore_signal(bar, inc=1, device_id=mate, device_id_type=DT)
    pl.semaphore_wait(bar, count)

    def remote(src, dst, send, recv, dev):
        return pltpu.make_async_remote_copy(src, dst, send, recv, device_id=dev, device_id_type=DT)

    inputs = ((r.tokens, r.x), (r.frames, r.e), (r.cotangent, r.dy))

    def swap(k, slot):
        src, dst = inputs[k]
        return remote(src, dst.at[slot], r.swap_send.at[k], r.swap_recv.at[k], mate)

    def local(k):
        src, dst = inputs[k]
        return pltpu.make_async_copy(src, dst.at[c], r.in_sem.at[k])

    if fast:
        def pack_copy(k, slot):
            return remote(r.pack, r.packs.at[slot], r.pack_send.at[k], r.pack_recv.at[slot],
                          peer(lax.rem(me + k + 1, count)))

        loop(count - 1, lambda k: pack_copy(k, me).start())
        own_pack = pltpu.make_async_copy(r.pack, r.packs.at[me], r.in_sem.at[3])
        own_pack.start()
    swap(0, c).start()
    local(0).start()
    gather.begin()
    gather.run(1)
    for k in (1, 2):
        swap(k, c).start()
        local(k).start()

    def arrived(k):
        local(k).wait()
        swap(k, 1 - c).wait_recv()

    outs = []

    def emit(out, scratch):
        outs.append(pltpu.make_async_copy(scratch, out, r.out_sem.at[len(outs)]))
        outs[-1].start()

    if fast:
        own_pack.wait()
        loop(count - 1, lambda k: pack_copy(k, lax.rem(me + k + 1, count)).wait_recv())
        for i in range(2 * levels):
            for xx in range(2):
                block = r.packs[i * 2 + xx]
                if xx == 0:
                    r.norm[:, i * 128 : (i + 1) * 128] = block
                r.bias[i * 2 + xx : i * 2 + xx + 1, 0:128] = block[9:10]
                r.bias[i * 2 + xx : i * 2 + xx + 1, 128:256] = block[10:11]
    else:
        r.norm[...] = r.norm_in[...]
        r.bias[...] = r.bias_in[...]
    emit(r.norm_out, r.norm)

    def norm_row(k):
        return r.norm[k : k + 1, :]

    def bias_row(k, side):
        return r.bias[pl.ds(k * 2 + side, 1), :]

    key = lax.broadcasted_iota(jnp.int32, (1, 2 * KEYS), 1)
    real = lax.rem(key, KEYS) < HALF_FRAMES
    r.padrow[0:1, :] = jnp.where(real, 0.0, -1e30).astype(f32)
    for i in range(3):
        for side in range(2):
            r.qkv[i, side, L:512, :] = jnp.zeros((512 - L, COLS), bf)

    arrived(0)

    def ln1(half):
        def body(rows, i):
            normed, _ = normed_block(r.x[half, rows, :].astype(f32))
            out = (normed * norm_row(0) + norm_row(1)).astype(bf)
            r.a1[pl.ds(pl.multiple_of(half * HALF + i * BLOCK, BLOCK), BLOCK), :] = out

        rows_loop(HALF, body, NORM_TURNS if NORM_TURNS in (1, 7) else 1)

    ln1(0)
    ln1(1)
    emit(r.a1_out, r.a1)
    emit(r.x_out, r.x)

    def project_one(i, side):
        bias = bias_row(0, side) if i == 0 else bias_row(1, side)
        acc = dot(r.a1[...], flat_panel(r.wide, i, side), NN)
        if i != 1:
            acc = acc + bias
        r.qkv[i, side, 0:L, :] = acc.astype(bf)

    for i in range(3):
        gather.need(i)
        loop(2, lambda side: project_one(i, side))
    emit(r.qkv_out, r.qkv)

    lane = lax.broadcasted_iota(jnp.int32, (1, 128), 1)
    low = lane < HD

    def attend(query, key_parts, values, width, causal, lse, ctx, per_head, tick):
        def body(t):
            side, half = t // 2, lax.rem(t, 2)
            lanes = pl.ds(pl.multiple_of(half * 128, 128), 128)
            q = query(side, lanes)
            found = []
            for sub in range(2):
                mine = low if sub == 0 else jnp.logical_not(low)
                qh = jnp.where(mine, q.astype(f32) * 0.125, 0.0).astype(bf)
                for n, part in enumerate(key_parts(side, lanes)):
                    r.s[:, n * width : (n + 1) * width] = dot(qh, part, NT)
                total = width * len(key_parts(side, lanes))

                def rows_body(rows, i):
                    s = r.s[rows, 0:total]
                    if causal:
                        row = i * BLOCK + lax.broadcasted_iota(jnp.int32, (BLOCK, total), 0)
                        col = lax.broadcasted_iota(jnp.int32, (BLOCK, total), 1)
                        s = jnp.where(col <= row, s, -1e30)
                    else:
                        s = s + r.padrow[0:1, 0:total]
                    top = jnp.max(s, axis=-1, keepdims=True)
                    e = jnp.exp(s - top)
                    weight = jnp.sum(e, axis=-1, keepdims=True)
                    r.p[rows, 0:total] = (e * (1.0 / weight)).astype(bf)
                    lse[rows, :] = jnp.where(lane == t * 2 + sub, top + jnp.log(weight), lse[rows, :])

                rows_loop(L, rows_body, 7 if causal else SOFT_TURNS)
                for i in range(per_head):
                    tick((t * 2 + sub) * per_head + i)
                acc = None
                for n, part in enumerate(values(side, lanes)):
                    more = dot(r.p[:, n * width : (n + 1) * width], part, NN)
                    acc = more if acc is None else acc + more
                found.append(acc)
            ctx[side, :, lanes] = jnp.where(low, found[0], found[1]).astype(bf)

        loop(4, body)

    attend(
        lambda side, lanes: r.qkv[0, side, 0:L, lanes],
        lambda side, lanes: [r.qkv[1, side, :, lanes]],
        lambda side, lanes: [r.qkv[2, side, :, lanes]],
        512, True, r.lse1, r.c1, 1, gather.turn(8),
    )
    emit(r.lse1_out, r.lse1)
    emit(r.c1_out, r.c1)

    def collect(n, ctx, mat):
        def body(j):
            rows = pl.ds(pl.multiple_of(j * COLS, COLS), COLS)
            acc = None
            for side in range(2):
                more = dot(ctx[side], flat_rows(r.wide.at[mat, side], j), NT)
                acc = more if acc is None else acc + more
            r.part[n, j] = acc.astype(bf)
            trade(n, j).start()

        loop(4, body)

    def trade(n, j):
        return remote(r.part.at[n, j], r.got.at[n, j], r.part_send.at[n, j], r.part_recv.at[n, j], mate)

    def traded(n):
        loop(4, lambda j: trade(n, j).wait_recv())

    def residual(n, base, bias_k, out, gain_k, normed_out):
        def body(rows, i):
            v = base(rows, i) + norm_row(bias_k) + (panels_row(r.part.at[n], rows) + panels_row(r.got.at[n], rows))
            out[rows, :] = v
            normed, _ = normed_block(v)
            normed_out[rows, :] = (normed * norm_row(gain_k) + norm_row(gain_k + 1)).astype(bf)

        rows_loop(L, body, NORM_TURNS)

    def x_rows(rows, i):
        half = i // (HALF // BLOCK)
        inner = pl.ds(pl.multiple_of((i - half * (HALF // BLOCK)) * BLOCK, BLOCK), BLOCK)
        return r.x[half, inner, :].astype(f32)

    gather.need(3)
    collect(0, r.c1, 3)
    gather.run(1)
    traded(0)
    residual(0, x_rows, 6, r.h1, 2, r.a2)
    emit(r.h1_out, r.h1)
    emit(r.a2_out, r.a2)

    gather.need(4)

    def query_two(side):
        acc = dot(r.a2[...], flat_panel(r.wide, 4, side), NN) + bias_row(2, side)
        r.q2[side] = acc.astype(bf)

    loop(2, query_two)
    emit(r.q2_out, r.q2)
    arrived(1)
    emit(r.e_out, r.e)

    gather.need(5)

    def frame_keys(t):
        side, half = t // 2, lax.rem(t, 2)
        r.ek[side, half] = dot(r.e[half], flat_panel(r.wide, 5, side), NN).astype(bf)

    loop(4, frame_keys)
    emit(r.ek_out, r.ek)
    gather.need(6)

    def frame_values(t):
        side, half = t // 2, lax.rem(t, 2)
        acc = dot(r.e[half], flat_panel(r.wide, 6, side), NN) + bias_row(3, side)
        r.ev[side, half] = acc.astype(bf)

    loop(4, frame_values)
    emit(r.ev_out, r.ev)
    attend(
        lambda side, lanes: r.q2[side, :, lanes],
        lambda side, lanes: [r.ek[side, half, :, lanes] for half in range(2)],
        lambda side, lanes: [r.ev[side, half, :, lanes] for half in range(2)],
        KEYS, False, r.lse2, r.c2, 2, gather.turn(16),
    )
    emit(r.lse2_out, r.lse2)
    emit(r.c2_out, r.c2)
    gather.need(7)
    collect(1, r.c2, 7)
    gather.run(1)
    traded(1)
    residual(1, lambda rows, i: r.h1[rows, :], 7, r.h2, 4, r.a3)
    emit(r.h2_out, r.h2)
    emit(r.a3_out, r.a3)
    arrived(2)
    emit(r.dy_out, r.dy)

    def hidden(t):
        m, side = t // 2, lax.rem(t, 2)
        u = dot(r.a3[...], flat_panel(r.wide, 8 + m, side), NN) + bias_row(4 + m, side)
        half = 0.5 * (1.0 + lax.erf(u * 0.7071067811865476))
        r.z[t] = (u * half).astype(bf)
        r.slope[t] = (half + u * jnp.exp(-0.5 * u * u) * 0.3989422804014327).astype(bf)

    def result(k):
        def tile(j):
            cols = pl.ds(pl.multiple_of(j * COLS, COLS), COLS)
            acc = None
            for t in range(4 * k, 4 * k + 4):
                more = dot(r.z[t], flat_rows(r.wide.at[12 + t // 2, t % 2], j), NT)
                acc = more if acc is None else acc + more
            if k == 0:
                r.acc[:, cols] = acc
            else:
                r.acc[:, cols] += acc

        loop(4, tile)

    emit(r.wide_out.at[0:8], r.wide.at[0:8])
    for m in range(4):
        gather.need(8 + m)
        loop(2, lambda side: hidden(2 * m + side))
    emit(r.z_out, r.z)
    emit(r.slope_out, r.slope)
    emit(r.wide_out.at[8:12], r.wide.at[8:12])
    for k in range(2):
        gather.need(12 + 2 * k)
        gather.need(13 + 2 * k)
        result(k)

    emit(r.wide_out.at[12:16], r.wide.at[12:16])

    for half in range(2):
        @pl.when(c == half)
        def _():
            far = (1 - half) * HALF

            def body(j):
                cols = pl.ds(pl.multiple_of(j * COLS, COLS), COLS)
                r.part[2, j, 0:HALF, :] = r.acc[far : far + HALF, cols].astype(bf)

            loop(4, body)

    last = remote(
        r.part.at[2, :, 0:HALF], r.got.at[2, :, 0:HALF], r.part_send.at[2, 0], r.part_recv.at[2, 0], mate
    )
    last.start()
    last.wait_recv()

    def finish(rows, i):
        here = pl.ds(pl.multiple_of(c * HALF + i * BLOCK, BLOCK), BLOCK)
        own = r.acc[here, :].astype(bf).astype(f32)
        v = r.h2[here, :] + norm_row(8) + (own + panels_row(r.got.at[2], rows))
        r.outrows[rows, :] = v.astype(bf)

    rows_loop(HALF, finish)
    emit(r.layer_out, r.outrows)

    for k in range(3):
        swap(k, c).wait_send()
    if fast:
        loop(count - 1, lambda k: pack_copy(k, me).wait_send())
    for n in range(2):
        loop(4, lambda j: trade(n, j).wait_send())
    last.wait_send()
    gather.drain()
    for copy in outs:
        copy.wait()


class ForwardRefs(NamedTuple):
    shard: object
    tokens: object
    frames: object
    cotangent: object
    pack: object
    norm_in: object
    bias_in: object
    layer_out: object
    norm_out: object
    a1_out: object
    x_out: object
    qkv_out: object
    lse1_out: object
    c1_out: object
    h1_out: object
    a2_out: object
    q2_out: object
    e_out: object
    ek_out: object
    ev_out: object
    lse2_out: object
    c2_out: object
    h2_out: object
    a3_out: object
    dy_out: object
    z_out: object
    slope_out: object
    wide_out: object
    wide: object
    x: object
    dy: object
    e: object
    norm: object
    bias: object
    a1: object
    a2: object
    a3: object
    h1: object
    h2: object
    qkv: object
    c1: object
    q2: object
    c2: object
    ek: object
    ev: object
    lse1: object
    lse2: object
    z: object
    slope: object
    s: object
    p: object
    acc: object
    part: object
    got: object
    packs: object
    padrow: object
    outrows: object
    in_sem: object
    swap_send: object
    swap_recv: object
    part_send: object
    part_recv: object
    pack_send: object
    pack_recv: object
    out_sem: object


class Kept(NamedTuple):
    layer_out: object
    norm: object
    a1: object
    x: object
    qkv: object
    lse1: object
    c1: object
    h1: object
    a2: object
    q2: object
    e: object
    ek: object
    ev: object
    lse2: object
    c2: object
    h2: object
    a3: object
    dy: object
    z: object
    slope: object
    wide: object


def forward(shard, tokens, frames, cotangent, small, shards):
    levels, rows = shards // 2, D // shards
    groups = GROUPS if levels <= 4 else 4
    fast = rows == 128
    f32, bf = jnp.float32, jnp.bfloat16
    sem = pltpu.SemaphoreType.DMA
    vm, hbm = pl.BlockSpec(memory_space=pltpu.VMEM), pl.BlockSpec(memory_space=pl.ANY)
    wide = (MATS, 2, levels, 2, rows, COLS)
    shapes = [
        ((HALF, D), bf),
        ((16, D), f32),
        ((L, D), bf),
        ((2, HALF, D), bf),
        ((3, 2, 512, COLS), bf),
        ((L, 128), f32),
        ((2, L, COLS), bf),
        ((L, D), f32),
        ((L, D), bf),
        ((2, L, COLS), bf),
        ((2, KEYS, D), bf),
        ((2, 2, KEYS, COLS), bf),
        ((2, 2, KEYS, COLS), bf),
        ((L, 128), f32),
        ((2, L, COLS), bf),
        ((L, D), f32),
        ((L, D), bf),
        ((2, HALF, D), bf),
        ((8, L, COLS), bf),
        ((8, L, COLS), bf),
        (wide, bf),
    ]
    peers = shards * 2
    scratch = [
        pltpu.VMEM(wide, bf), pltpu.VMEM((2, HALF, D), bf), pltpu.VMEM((2, HALF, D), bf), pltpu.VMEM((2, KEYS, D), bf),
        pltpu.VMEM((16, D), f32), pltpu.VMEM((16, COLS), f32),
        pltpu.VMEM((L, D), bf), pltpu.VMEM((L, D), bf), pltpu.VMEM((L, D), bf),
        pltpu.VMEM((L, D), f32), pltpu.VMEM((L, D), f32),
        pltpu.VMEM((3, 2, 512, COLS), bf), pltpu.VMEM((2, L, COLS), bf), pltpu.VMEM((2, L, COLS), bf),
        pltpu.VMEM((2, L, COLS), bf), pltpu.VMEM((2, 2, KEYS, COLS), bf), pltpu.VMEM((2, 2, KEYS, COLS), bf),
        pltpu.VMEM((L, 128), f32), pltpu.VMEM((L, 128), f32),
        pltpu.VMEM((8, L, COLS), bf), pltpu.VMEM((8, L, COLS), bf),
        pltpu.VMEM((L, 2 * KEYS), f32), pltpu.VMEM((L, 2 * KEYS), bf), pltpu.VMEM((L, D), f32),
        pltpu.VMEM((3, 4, L, COLS), bf), pltpu.VMEM((3, 4, L, COLS), bf),
        pltpu.VMEM((peers, 16, 128) if fast else (1, 16, 128), f32), pltpu.VMEM((8, 2 * KEYS), f32),
        pltpu.VMEM((HALF, D), bf),
        sem((4,)), sem((3,)), sem((3,)), sem((3, 4)), sem((3, 4)), sem((peers,)), sem((peers,)),
        sem((len(shapes) + 2,)),
    ]
    outs = pl.pallas_call(
        partial(forward_kernel, levels, groups, fast),
        out_shape=[jax.ShapeDtypeStruct(s, t) for s, t in shapes],
        in_specs=[vm, hbm, hbm, hbm, vm, vm, vm],
        out_specs=[hbm] * len(shapes),
        scratch_shapes=scratch + Gather.semaphores(levels, groups),
        compiler_params=pltpu.CompilerParams(
            collective_id=0, has_side_effects=True, vmem_limit_bytes=63 * 2**20
        ),
        name="forward",
    )(shard, tokens, frames, cotangent, *small)
    return Kept(*outs)


RING = 4


class Scatter:
    def __init__(self, levels, part, own, bufs, sems):
        self.levels, self.part, self.own = levels, part, own
        self.one_y, self.one_x, self.two_x, self.two_y, self.line = bufs
        self.s1, self.r1, self.s2, self.r2, self.s3, self.r3 = sems
        self.at = place()
        self.sent = self.steps = self.ready = 0

    @staticmethod
    def buffers(levels, rows):
        bf, half = jnp.bfloat16, levels // 2
        return [
            pltpu.VMEM((RING, 2, half, rows, COLS), bf), pltpu.VMEM((RING, half, 2, rows, COLS), bf),
            pltpu.VMEM((RING, half, rows, COLS), bf), pltpu.VMEM((RING, half, rows, COLS), bf),
            pltpu.VMEM((RING, levels, rows, COLS), bf),
        ]

    @staticmethod
    def semaphores(levels):
        sem = pltpu.SemaphoreType.DMA
        two = sem((MATS, 2))
        many = sem((MATS, levels))
        return [two, two, two, two, many, many]

    def to_x(self, src, dst, send, recv):
        z, y, x, c = self.at
        return pltpu.make_async_remote_copy(src, dst, send, recv, device_id=device(z, y, 1 - x, c), device_id_type=DT)

    def to_y(self, src, dst, send, recv):
        z, y, x, c = self.at
        return pltpu.make_async_remote_copy(src, dst, send, recv, device_id=device(z, 1 - y, x, c), device_id_type=DT)

    def first(self, g):
        z, y, x, c = self.at
        m, slot = MATS - 1 - g, lax.rem(g, RING)
        return (
            self.to_y(self.part.at[m, :, :, 0, 1 - y], self.one_y.at[slot], self.s1.at[g, 0], self.r1.at[g, 0]),
            self.to_x(self.part.at[m, 1 - x, :, 1], self.one_x.at[slot], self.s1.at[g, 1], self.r1.at[g, 1]),
        )

    def second(self, g):
        z, y, x, c = self.at
        m, slot = MATS - 1 - g, lax.rem(g, RING)
        return (
            self.to_x(self.part.at[m, 1 - x, :, 0, y], self.two_x.at[slot], self.s2.at[g, 0], self.r2.at[g, 0]),
            self.to_y(self.part.at[m, x, :, 1, 1 - y], self.two_y.at[slot], self.s2.at[g, 1], self.r2.at[g, 1]),
        )

    def third(self, g, zz, k):
        z, y, x, c = self.at
        return pltpu.make_async_remote_copy(
            self.part.at[MATS - 1 - g, x, zz // 2, lax.rem(zz, 2), y], self.line.at[lax.rem(g, RING), k],
            self.s3.at[g, zz], self.r3.at[g, k], device_id=device(zz, y, x, c), device_id_type=DT,
        )

    def send(self, count):
        def body(i):
            for copy in self.first(i):
                copy.start()

        start = self.sent
        self.sent += count
        loop(count, lambda i: body(start + i))

    def add(self, at, got):
        self.part[at] = (self.part[at].astype(jnp.float32) + got.astype(jnp.float32)).astype(jnp.bfloat16)

    def step_a(self, g):
        z, y, x, c = self.at
        m, slot = MATS - 1 - g, lax.rem(g, RING)
        along_y, along_x = self.first(g)
        then_x, then_y = self.second(g)
        along_y.wait_recv()
        for k in range(2):
            loop(self.levels // 2, lambda h: self.add((m, k, h, 0, y), self.one_y[slot, k, h]))
        then_x.start()
        along_x.wait_recv()
        for k in range(2):
            loop(self.levels // 2, lambda h: self.add((m, x, h, 1, k), self.one_x[slot, h, k]))
        then_y.start()

    def step_b(self, g):
        z, y, x, c = self.at
        m, slot = MATS - 1 - g, lax.rem(g, RING)
        then_x, then_y = self.second(g)
        then_x.wait_recv()
        loop(self.levels // 2, lambda h: self.add((m, x, h, 0, y), self.two_x[slot, h]))
        then_y.wait_recv()
        loop(self.levels // 2, lambda h: self.add((m, x, h, 1, y), self.two_y[slot, h]))
        loop(self.levels - 1, lambda k: self.third(g, lax.rem(z + k + 1, self.levels), z).start())

    def step_c(self, g):
        z, y, x, c = self.at
        m = MATS - 1 - g
        loop(self.levels - 1, lambda k: self.third(g, z, lax.rem(z + k + 1, self.levels)).wait_recv())
        self.own[m] = self.part[m, x, z // 2, lax.rem(z, 2), y].astype(jnp.float32)

        def body(k):
            @pl.when(k != z)
            def _():
                self.own[m] += self.line[lax.rem(g, RING), k].astype(jnp.float32)

        loop(self.levels, body)

    def step(self, t):
        @pl.when(t < MATS)
        def _():
            self.step_a(t)

        @pl.when((t >= 1) & (t <= MATS))
        def _():
            self.step_b(t - 1)

        @pl.when(t >= 2)
        def _():
            self.step_c(t - 2)

    def turn(self, count):
        start, first = self.steps, self.sent
        self.steps += count
        self.sent = max(first, min(MATS, self.steps + RING - 2))
        assert self.sent <= self.ready

        def body(i):
            t = start + i
            self.step(t)
            g = t + RING - 2

            @pl.when((g >= first) & (g < MATS))
            def _():
                for copy in self.first(g):
                    copy.start()

        return body

    def run(self, count):
        loop(count, self.turn(count))

    def drain(self):
        z, y, x, c = self.at

        def body(g):
            for copy in (*self.first(g), *self.second(g)):
                copy.wait_send()
            loop(self.levels - 1, lambda k: self.third(g, lax.rem(z + k + 1, self.levels), z).wait_send())

        loop(MATS, body)


class BackwardIn(NamedTuple):
    dy: object
    wide: object
    slope: object
    z: object
    a3: object
    h2: object
    norm: object
    c2: object
    q2: object
    lse2: object
    ek: object
    ev: object
    e: object
    a2: object
    h1: object
    c1: object
    qkv: object
    lse1: object
    a1: object
    x: object
    mean_attn: object
    mean_dense: object
    square_attn: object
    square_dense: object
    shard: object
    pack: object
    norm_mean: object
    unit_mean: object
    norm_square: object
    unit_square: object


class BackwardOut(NamedTuple):
    owned_attn: object
    owned_dense: object
    input_out: object
    frame_out: object
    small_out: object
    bcols_out: object
    norm_out: object
    unit_out: object
    norms: object


class BackwardRefs(NamedTuple):
    owned_attn: object
    owned_dense: object
    input_out: object
    frame_out: object
    small_out: object
    bcols_out: object
    norm_out: object
    unit_out: object
    norms: object
    part: object
    own: object
    dy: object
    slope: object
    z: object
    left: object
    h: object
    norm: object
    c2: object
    q2: object
    lse2: object
    ek: object
    ev: object
    e: object
    a2: object
    c1: object
    qkv: object
    lse1: object
    x: object
    dh: object
    dhb: object
    dc: object
    stat: object
    s: object
    dp: object
    p: object
    ds: object
    mine: object
    got: object
    fsend: object
    frecv: object
    fout: object
    cols: object
    bcols: object
    small: object
    smallgot: object
    smallsum: object
    in_sem: object
    trade_send: object
    trade_recv: object
    frame_send: object
    frame_recv: object
    frame_out_sem: object
    small_send: object
    small_recv: object
    out_sem: object
    moments: object
    held: object
    squares: object
    sums: object
    sumsgot: object
    sumspair: object
    load_sem: object
    step_sem: object
    pair_sem: object
    sums_send: object
    sums_recv: object


def backward_kernel(levels, fast, token_total, *refs):
    f32, bf = jnp.float32, jnp.bfloat16
    at, width = len(BackwardIn._fields), len(BackwardRefs._fields)
    given = BackwardIn(*refs[:at])
    r = BackwardRefs(*refs[at : at + width])
    rest = refs[at + width :]
    scatter = Scatter(levels, r.part, r.own, rest[:5], rest[5:])
    z, y, x, c = place()
    dp = z * 2 + y
    mate = (dp, x, 1 - c)
    count = levels * 4
    me = dp * 2 + x
    rows_of = D // (levels * 2)
    per = COLS // (2 * rows_of)

    def peer(i):
        return (i // 2, lax.rem(i, 2), c)

    loads = []

    def load(src, dst):
        loads.append(pltpu.make_async_copy(src, dst, r.in_sem.at[len(loads)]))
        loads[-1].start()
        return loads[-1]

    def loaded(*which):
        for copy in which:
            copy.wait()

    get_dy = load(given.dy, r.dy)
    get_w2 = load(given.wide.at[12:16], r.part.at[12:16])
    get_slope = load(given.slope, r.slope)
    get_z = load(given.z, r.z)
    get_w1 = load(given.wide.at[8:12], r.part.at[8:12])
    get_a3 = load(given.a3, r.left)
    get_h2 = load(given.h2, r.h)
    get_w0 = load(given.wide.at[0:8], r.part.at[0:8])
    get_norm = load(given.norm, r.norm)
    get_c2 = load(given.c2, r.c2)
    get_q2 = load(given.q2, r.q2)
    get_lse2 = load(given.lse2, r.lse2)
    get_ek = load(given.ek, r.ek)
    get_ev = load(given.ev, r.ev)
    get_e = load(given.e, r.e)
    get_a2 = load(given.a2, r.a2)
    get_c1 = load(given.c1, r.c1)
    get_qkv = load(given.qkv, r.qkv)
    get_lse1 = load(given.lse1, r.lse1)
    get_x = load(given.x, r.x)

    bar = pltpu.get_barrier_semaphore()
    loop(count - 1, lambda k: pl.semaphore_signal(
        bar, inc=1, device_id=peer(lax.rem(me + k + 1, count)), device_id_type=DT))
    pl.semaphore_signal(bar, inc=1, device_id=mate, device_id_type=DT)
    pl.semaphore_wait(bar, count)

    def remote(src, dst, send, recv, dev):
        return pltpu.make_async_remote_copy(src, dst, send, recv, device_id=dev, device_id_type=DT)

    def trade(n, j):
        return remote(r.mine.at[n % 2, j], r.got.at[n % 2, j], r.trade_send.at[n, j],
                      r.trade_recv.at[n, j], mate)

    def panel(mat, side):
        return r.part[mat, side].reshape(D, COLS)

    def part_rows(mat, side, j):
        if per == 1:
            return r.part[mat, side, j // 2, lax.rem(j, 2)].reshape(COLS, COLS)
        return r.part[mat, side, pl.ds(j * (per // 2), per // 2)].reshape(COLS, COLS)

    def grads(lefts, items):
        def body(j):
            cols = pl.ds(pl.multiple_of(j * COLS, COLS), COLS)
            turned = [v.T for v in lefts(cols)]
            for mat, side, rights in items:
                acc = None
                for t, right in zip(turned, rights()):
                    more = dot(t, right, NN)
                    acc = more if acc is None else acc + more
                if per == 1:
                    r.part[mat, side, j // 2, lax.rem(j, 2)] = acc.astype(bf).reshape(2, rows_of, COLS)
                else:
                    blocks = pl.ds(j * (per // 2), per // 2)
                    r.part[mat, side, blocks] = acc.astype(bf).reshape(per // 2, 2, 2, rows_of, COLS)

        loop(4, body)

    def send_back(n, items):
        if n >= 2:
            loop(4, lambda j: trade(n - 2, j).wait_send())

        def body(j):
            acc = None
            for value, mat, side in items:
                more = dot(value(), part_rows(mat, side, j), NT)
                acc = more if acc is None else acc + more
            r.mine[n % 2, j] = acc.astype(bf)
            trade(n, j).start()

        loop(4, body)

    def fold(v):
        return jnp.sum(v.reshape(BLOCK // 8, 8, D), axis=0)

    def norm_row(k):
        return r.norm[k : k + 1, :]

    def grow(k, v):
        r.cols[k * 8 : (k + 1) * 8, :] += fold(v)

    def half_rows(ref, i):
        half = i // (HALF // BLOCK)
        inner = pl.ds(pl.multiple_of((i - half * (HALF // BLOCK)) * BLOCK, BLOCK), BLOCK)
        return ref[half, inner, :].astype(f32)

    def norm_back(n, k, base, incoming, sum_k):
        loop(4, lambda j: trade(n, j).wait_recv())

        def body(rows, i):
            normed, scaled = normed_block(base(rows, i))
            dn = panels_row(r.mine.at[n % 2], rows) + panels_row(r.got.at[n % 2], rows)
            inner = dn * norm_row(k)
            back = scaled * (
                inner - jnp.mean(inner, axis=-1, keepdims=True)
                - normed * jnp.mean(inner * normed, axis=-1, keepdims=True)
            )
            came = incoming(rows, i)
            out = came + back
            r.dh[rows, :] = out
            grow(k, dn * normed)
            grow(k + 1, dn)
            if sum_k is not None:
                r.dhb[rows, :] = out.astype(bf)
                grow(sum_k, out)
            if n == 0:
                grow(8, came)

        rows_loop(L, body, NORM_TURNS)

    r.cols[...] = jnp.zeros((72, D), f32)
    loaded(get_dy, get_w2, get_slope)

    def hidden_back(t):
        m, side = t // 2, lax.rem(t, 2)
        du = (dot(r.dy[...].reshape(L, D), panel(12 + m, side), NN) * r.slope[t].astype(f32)).astype(bf)
        r.slope[t] = du
        r.bcols[pl.ds(8 + t, 1), :] = jnp.sum(du.astype(f32), axis=0, keepdims=True)

    loaded(get_z)

    def down_grads(k):
        m = 3 - k
        loop(2, lambda side: hidden_back(2 * m + side))
        grads(
            lambda cols: [r.dy[:, :, cols].reshape(L, COLS)],
            [(12 + m, side, lambda side=side: [r.z[2 * m + side]]) for side in range(2)],
        )
        for copy in scatter.first(k):
            copy.start()

    loop(4, down_grads)
    scatter.sent = 4
    loaded(get_w1)
    send_back(0, [(lambda t=t: r.slope[t], 8 + t // 2, t % 2) for t in range(8)])
    loaded(get_a3, get_h2, get_norm)
    grads(
        lambda cols: [r.left[:, cols]],
        [(8 + t // 2, t % 2, lambda t=t: [r.slope[t]]) for t in range(8)],
    )
    scatter.ready = 8
    get_a1 = load(given.a1, r.left)
    norm_back(0, 4, lambda rows, i: r.h[rows, :], lambda rows, i: half_rows(r.dy, i), 7)
    get_h1 = load(given.h1, r.h)
    scatter.run(1)
    loaded(get_w0)

    def context_back(mat):
        def body(side):
            r.dc[side] = dot(r.dhb[...], panel(mat, side), NN).astype(bf)

        loop(2, body)

    def statistics(lse, ctx):
        r.stat[0:8, :] = lse[...].T[0:8, :]
        for side in range(2):
            both = (r.dc[side].astype(f32) * ctx[side].astype(f32)).T
            r.stat[8 + side * 4 : 12 + side * 4, :] = jnp.sum(both.reshape(4, HD, L), axis=1)

    lane = lax.broadcasted_iota(jnp.int32, (1, 128), 1)
    low = lane < HD
    low_row = lax.broadcasted_iota(jnp.int32, (128, 1), 0) < HD

    def attend_back(query, keys, values, parts, width, causal, turn):
        def body(t):
            side, half = t // 2, lax.rem(t, 2)
            lanes = pl.ds(pl.multiple_of(half * 128, 128), 128)
            q = query[(side, slice(0, L), lanes)].astype(f32) * 0.125
            dc = r.dc[side, :, lanes].astype(f32)
            back = None
            for n in range(parts):
                at = (side, n, slice(None), lanes) if parts > 1 else (side, slice(0, L), lanes)
                k, v = keys[at], values[at]
                flat = k.T
                dk = dv = None
                for sub in range(2):
                    mine = low if sub == 0 else jnp.logical_not(low)
                    mine_row = low_row if sub == 0 else jnp.logical_not(low_row)
                    qh = jnp.where(mine, q, 0.0).astype(bf)
                    dm = jnp.where(mine, dc, 0.0).astype(bf)
                    kt = jnp.where(mine_row, flat.astype(f32), 0.0).astype(bf)
                    r.s[0:width, :] = dot(k, qh, NT)
                    r.dp[0:width, :] = dot(v, dm, NT)
                    lse = r.stat[pl.ds(t * 2 + sub, 1), :]
                    delta = r.stat[pl.ds(8 + t * 2 + sub, 1), :]

                    def rows_body(rows, i):
                        key = i * BLOCK + lax.broadcasted_iota(jnp.int32, (BLOCK, L), 0)
                        if causal:
                            keep = lax.broadcasted_iota(jnp.int32, (BLOCK, L), 1) >= key
                        else:
                            keep = key < HALF_FRAMES
                        p = jnp.where(keep, jnp.exp(jnp.where(keep, r.s[rows, :], -1e30) - lse), 0.0)
                        r.p[rows, :] = p.astype(bf)
                        r.ds[rows, :] = (p * (r.dp[rows, :] - delta)).astype(bf)

                    rows_loop(width, rows_body, 14 if causal else BACK_TURNS)
                    p, ds = r.p[0:width, :], r.ds[0:width, :]
                    dv = dot(p, dm, NN) if dv is None else dv + dot(p, dm, NN)
                    dk = dot(ds, qh, NN) if dk is None else dk + dot(ds, qh, NN)
                    more = dot(kt, ds, NN)
                    back = more if back is None else back + more
                keys[at] = dk.astype(bf)
                values[at] = dv.astype(bf)
            query[(side, slice(0, L), lanes)] = (back.T * 0.125).astype(bf)
            turn(t)

        loop(4, body)

    def column(k, ref, at):
        def body(side):
            r.bcols[pl.ds(k * 2 + side, 1), :] = jnp.sum(ref[at(side)].astype(f32), axis=0, keepdims=True)

        loop(2, body)

    context_back(7)
    loaded(get_c2, get_lse2)
    statistics(r.lse2, r.c2)
    grads(
        lambda cols: [r.dhb[:, cols]], [(7, side, lambda side=side: [r.c2[side]]) for side in range(2)]
    )
    scatter.ready = 9
    scatter.run(1)
    loaded(get_q2, get_ek, get_ev)
    attend_back(r.q2, r.ek, r.ev, 2, KEYS, False, scatter.turn(4))

    loaded(get_e, get_a2)

    def frame_share(half, j):
        acc = None
        for mat, ref in ((5, r.ek), (6, r.ev)):
            for side in range(2):
                more = dot(ref[side, half], part_rows(mat, side, j), NT)
                acc = more if acc is None else acc + more
        return acc

    def frame_trade(j):
        return remote(r.fsend.at[j], r.frecv.at[j], r.frame_send.at[j], r.frame_recv.at[j], mate)

    def frame_store(j):
        cols = pl.ds(pl.multiple_of(j * COLS, COLS), COLS)
        return pltpu.make_async_copy(r.fout.at[lax.rem(j, 2)], r.frame_out.at[:, cols], r.frame_out_sem.at[j])

    def frame_far(j):
        r.fsend[j] = frame_share(1 - c, j).astype(bf)
        frame_trade(j).start()

    def frame_near(j):
        @pl.when(j >= 2)
        def _():
            frame_store(j - 2).wait()

        frame_trade(j).wait_recv()
        r.fout[lax.rem(j, 2)] = (frame_share(c, j) + r.frecv[j].astype(f32))[0:HALF_FRAMES]
        frame_store(j).start()

    loop(4, frame_far)
    send_back(1, [(lambda side=side: r.q2[side], 4, side) for side in range(2)])
    loop(4, frame_near)
    scatter.run(1)
    grads(
        lambda cols: [r.e[n, :, cols] for n in range(2)],
        [(5 + i, side, lambda ref=ref, side=side: [ref[side, n] for n in range(2)])
         for i, ref in ((1, r.ev), (0, r.ek)) for side in range(2)],
    )
    scatter.ready = 11
    scatter.run(1)
    column(2, r.q2, lambda side: (side,))

    def value_column(side):
        total = sum(jnp.sum(r.ev[side, n].astype(f32), axis=0, keepdims=True) for n in range(2))
        r.bcols[pl.ds(6 + side, 1), :] = total

    loop(2, value_column)
    grads(lambda cols: [r.a2[:, cols]], [(4, side, lambda side=side: [r.q2[side]]) for side in range(2)])
    scatter.ready = 12
    loaded(get_h1)
    norm_back(1, 2, lambda rows, i: r.h[rows, :], lambda rows, i: r.dh[rows, :], 6)
    scatter.run(1)
    context_back(3)
    loaded(get_c1, get_lse1)
    statistics(r.lse1, r.c1)
    grads(
        lambda cols: [r.dhb[:, cols]], [(3, side, lambda side=side: [r.c1[side]]) for side in range(2)]
    )
    scatter.ready = 13
    scatter.run(1)
    loaded(get_qkv)
    q_ref, k_ref, v_ref = (r.qkv.at[i] for i in range(3))
    attend_back(q_ref, k_ref, v_ref, 1, L, True, lambda t: None)
    send_back(2, [(lambda i=i, side=side: r.qkv[i, side, 0:L, :], i, side) for i in range(3) for side in range(2)])
    loaded(get_a1)
    grads(
        lambda cols: [r.left[:, cols]],
        [(i, side, lambda i=i, side=side: [r.qkv[i, side, 0:L, :]]) for i in (2, 1, 0) for side in range(2)],
    )
    scatter.ready = 16
    scatter.run(1)
    column(0, q_ref, lambda side: (side, slice(0, L)))
    column(1, v_ref, lambda side: (side, slice(0, L)))
    loaded(get_x)
    norm_back(2, 0, lambda rows, i: half_rows(r.x, i), lambda rows, i: r.dh[rows, :], None)
    own_rows = pl.ds(pl.multiple_of(c * HALF, HALF), HALF)
    input_copy = pltpu.make_async_copy(r.dh.at[own_rows], r.input_out, r.out_sem.at[0])
    input_copy.start()

    sums = jnp.concatenate([jnp.sum(r.cols[k * 8 : k * 8 + 8, :], axis=0, keepdims=True) for k in range(9)], axis=0)
    if fast:
        r.small[...] = jnp.zeros(r.small.shape, f32)
        for i in range(2 * levels):
            for xx in range(2):
                k = i * 2 + xx
                r.small[k, 0:9, :] = sums[:, i * 128 : (i + 1) * 128]
                r.small[k, 9:10, :] = r.bcols[k : k + 1, 0:128]
                r.small[k, 10:11, :] = r.bcols[k : k + 1, 128:256]

        def small_copy(k, slot):
            i = lax.rem(me + k + 1, count)
            return remote(r.small.at[i], r.smallgot.at[slot], r.small_send.at[k], r.small_recv.at[slot],
                          peer(i))

        loop(count - 1, lambda k: small_copy(k, me).start())
        r.smallgot[me] = r.small[me]
    else:
        r.smallsum[0:9, :] = sums

    def either(m, attn, dense, action):
        @pl.when(m < 8)
        def _():
            action(attn())

        @pl.when(m >= 8)
        def _():
            action(dense())

    def moment_loads(g, action):
        m, slot = MATS - 1 - g, lax.rem(g, 2)
        for k, (attn, dense) in enumerate(
            ((given.mean_attn, given.mean_dense), (given.square_attn, given.square_dense))
        ):
            def copy(src, at):
                return pltpu.make_async_copy(src.at[at], r.moments.at[slot, k], r.load_sem.at[slot, k])

            either(m, lambda: copy(attn, m), lambda: copy(dense, m - 8), action)
        action(pltpu.make_async_copy(given.shard.at[m], r.held.at[slot], r.load_sem.at[slot, 2]))

    def begin(copy):
        copy.start()

    def end(copy):
        copy.wait()

    def whole_store(m, attn, dense, action):
        def copy(dst, at):
            return pltpu.make_async_copy(r.own.at[m], dst.at[at], r.step_sem.at[m])

        either(m, lambda: copy(attn, m), lambda: copy(dense, m - 8), action)

    def direction(gradient, moment, second, weight):
        scaled = gradient / token_total
        moment = 0.5 * moment + 0.5 * scaled
        second = 0.5 * second + 0.5 * scaled * scaled
        return moment / (jnp.sqrt(second) + 1e-06) + 0.01 * weight

    def update(g):
        m, slot = MATS - 1 - g, lax.rem(g, 2)
        whole_store(m, r.owned_attn, r.owned_dense, begin)
        moment_loads(g, end)

        @pl.when(g + 1 < MATS)
        def _():
            moment_loads(g + 1, begin)

        r.squares[pl.ds(m, 1), :] = jnp.zeros((1, COLS), f32)
        r.squares[pl.ds(MATS + m, 1), :] = jnp.zeros((1, COLS), f32)

        def block(rows, i):
            weight = r.held[slot, rows, :].astype(f32)
            step = direction(r.own[m, rows, :], r.moments[slot, 0, rows, :], r.moments[slot, 1, rows, :], weight)
            r.squares[pl.ds(m, 1), :] += jnp.sum(step * step, axis=0, keepdims=True)
            r.squares[pl.ds(MATS + m, 1), :] += jnp.sum(weight * weight, axis=0, keepdims=True)

        rows_loop(rows_of, block, 2)

    if fast:
        moment_loads(0, begin)
        updated = scatter.steps - 2
        loop(updated, update)
        left = MATS + 2 - scatter.steps
        final = scatter.turn(left)

        def last_turn(i):
            final(i)
            update(updated + i)

        loop(left, last_turn)
    else:
        scatter.run(MATS + 2 - scatter.steps)
        for k, dst in enumerate((r.owned_attn, r.owned_dense)):
            copy = pltpu.make_async_copy(r.own.at[8 * k : 8 * k + 8], dst, r.step_sem.at[k])
            copy.start()
            copy.wait()
    if fast:
        loop(count - 1, lambda k: small_copy(k, lax.rem(me + k + 1, count)).wait_recv())
        total = r.smallgot[0]
        for k in range(1, 4 * levels):
            total = total + r.smallgot[k]
        r.smallsum[...] = total

        def units(pack):
            return jnp.concatenate([pack[9 + k // 2 : 10 + k // 2, k % 2 * HD : k % 2 * HD + HD] for k in range(4)])

        weights = given.pack[...]
        r.norm_out[...] = total[0:9]
        r.unit_out[...] = units(total)
        norm_step = direction(total[0:9], given.norm_mean[...], given.norm_square[...], weights[0:9])
        unit_step = direction(units(total), given.unit_mean[...], given.unit_square[...], units(weights))
        lanes = lax.broadcasted_iota(jnp.int32, (1, 128), 1)
        wide_lane = lax.broadcasted_iota(jnp.int32, (9, 128), 1)
        row = lax.broadcasted_iota(jnp.int32, (9, 128), 0)
        leader = jnp.where((x == 0) & (c == 0), 1.0, 0.0)

        def spread(first_row, norm, unit):
            line = jnp.zeros((1, 128), f32)
            for m in range(MATS):
                k = first_row + m
                one = jnp.sum(r.squares[k : k + 1, :], axis=1, keepdims=True)
                line = line + jnp.where(lanes == (m if m < 8 else 8 + (m - 8) // 4), one, 0.0)
            per_row = jnp.sum(norm * norm * leader, axis=1, keepdims=True)
            line = line + jnp.sum(jnp.where(wide_lane == 18 + row, per_row, 0.0), axis=0, keepdims=True)
            one = jnp.sum(jnp.sum(unit * unit, axis=1, keepdims=True), axis=0, keepdims=True)
            return line + jnp.where(lanes == 10 + dp, one, 0.0)

        r.sums[0, 0:1, :] = spread(MATS, weights[0:9], units(weights))
        r.sums[0, 1:2, :] = spread(0, norm_step, unit_step)
        pair = remote(r.sums.at[0], r.sumspair, r.pair_sem.at[0], r.pair_sem.at[1], mate)
        pair.start()
        pair.wait_recv()
        r.sums[1] = r.sums[0] + r.sumspair[...]

        def sums_copy(k, slot):
            return remote(r.sums.at[1], r.sumsgot.at[slot], r.sums_send.at[k], r.sums_recv.at[slot],
                          peer(lax.rem(me + k + 1, count)))

        loop(count - 1, lambda k: sums_copy(k, me).start())
        r.sumsgot[me] = r.sums[1]
        loop(count - 1, lambda k: sums_copy(k, lax.rem(me + k + 1, count)).wait_recv())
        all_sums = r.sumsgot[0]
        for k in range(1, 4 * levels):
            all_sums = all_sums + r.sumsgot[k]
        r.norms[...] = jnp.sqrt(all_sums)
        pair.wait_send()
        loop(count - 1, lambda k: small_copy(k, me).wait_send())
        loop(count - 1, lambda k: sums_copy(k, me).wait_send())
    small_store = pltpu.make_async_copy(r.smallsum, r.small_out, r.out_sem.at[2])
    bcols_store = pltpu.make_async_copy(r.bcols, r.bcols_out, r.out_sem.at[3])
    small_store.start()
    bcols_store.start()
    small_store.wait()
    bcols_store.wait()
    for n in (1, 2):
        loop(4, lambda j: trade(n, j).wait_send())
    loop(4, lambda j: frame_trade(j).wait_send())
    for j in (2, 3):
        frame_store(j).wait()
    scatter.drain()
    input_copy.wait()
    if fast:
        loop(MATS, lambda m: whole_store(m, r.owned_attn, r.owned_dense, end))


def backward(kept, state, token_total, shards):
    levels, rows = shards // 2, D // shards
    fast = rows == 128
    f32, bf = jnp.float32, jnp.bfloat16
    sem = pltpu.SemaphoreType.DMA
    hbm = pl.BlockSpec(memory_space=pl.ANY)
    peers = shards * 2
    half = ((8, rows, COLS), f32)
    shapes = [half, half, ((HALF, D), f32), ((HALF_FRAMES, D), f32)]
    shapes += [((16, 128) if fast else (16, D), f32), ((16, COLS), f32)]
    shapes += [((9, 128), f32), ((4, HD), f32), ((8, 128), f32)]
    small = (peers, 16, 128) if fast else (1, 16, 128)
    vm = pltpu.VMEM
    inside = pl.BlockSpec(memory_space=pltpu.VMEM)
    scratch = [
        vm((MATS, 2, levels // 2, 2, 2, rows, COLS), bf), vm((MATS, rows, COLS), f32), vm((2, HALF, D), bf),
        vm((8, L, COLS), bf), vm((8, L, COLS), bf), vm((L, D), bf), vm((L, D), f32), vm((16, D), f32),
        vm((2, L, COLS), bf), vm((2, L, COLS), bf), vm((L, 128), f32), vm((2, 2, KEYS, COLS), bf),
        vm((2, 2, KEYS, COLS), bf), vm((2, KEYS, D), bf), vm((L, D), bf),
        vm((2, L, COLS), bf), vm((3, 2, 512, COLS), bf), vm((L, 128), f32), vm((2, HALF, D), bf),
        vm((L, D), f32), vm((L, D), bf), vm((2, L, COLS), bf), vm((16, L), f32),
        vm((KEYS, L), f32), vm((KEYS, L), f32), vm((KEYS, L), bf), vm((KEYS, L), bf),
        vm((2, 4, L, COLS), bf), vm((2, 4, L, COLS), bf), vm((4, KEYS, COLS), bf), vm((4, KEYS, COLS), bf),
        vm((2, HALF_FRAMES, COLS), f32), vm((72, D), f32), vm((16, COLS), f32), vm(small, f32), vm(small, f32),
        vm((16, 128) if fast else (16, D), f32),
        sem((24,)), sem((3, 4)), sem((3, 4)), sem((4,)), sem((4,)), sem((4,)), sem((peers,)), sem((peers,)), sem((4,)),
        vm((2, 2, rows, COLS), f32), vm((2, rows, COLS), bf), vm((2 * MATS, COLS), f32), vm((2, 8, 128), f32),
        vm((peers if fast else 1, 8, 128), f32), vm((8, 128), f32), sem((2, 3)), sem((MATS,)), sem((2,)),
        sem((peers,)), sem((peers,)),
    ]
    return pl.pallas_call(
        partial(backward_kernel, levels, fast, token_total),
        out_shape=[jax.ShapeDtypeStruct(s, t) for s, t in shapes],
        in_specs=[hbm] * (len(BackwardIn._fields) - 5) + [inside] * 5,
        out_specs=[hbm] * (len(shapes) - 3) + [inside] * 3,
        scratch_shapes=scratch + Scatter.buffers(levels, rows) + Scatter.semaphores(levels),
        compiler_params=pltpu.CompilerParams(
            collective_id=1, has_side_effects=True, vmem_limit_bytes=63 * 2**20
        ),
        name="backward",
    )(
        kept.dy, kept.wide.reshape(MATS, 2, levels // 2, 2, 2, rows, COLS), kept.slope, kept.z, kept.a3, kept.h2, kept.norm, kept.c2, kept.q2, kept.lse2,
        kept.ek, kept.ev, kept.e, kept.a2, kept.h1, kept.c1, kept.qkv, kept.lse1, kept.a1, kept.x, *state,
    )


def small_kernel(shards, every, scatter, src, out, own_sem, send_sem, recv_sem):
    dp, x, c = (lax.axis_index(a) for a in AXES)
    cores = 2 if every else 1
    count = shards * 2 * cores
    me = (dp * 2 + x) * cores + (c if every else 0)

    def peer(i):
        if every:
            return (i // 4, lax.rem(i // 2, 2), lax.rem(i, 2))
        return (i // 2, lax.rem(i, 2), c)

    bar = pltpu.get_barrier_semaphore()

    def greet(k, carry):
        pl.semaphore_signal(bar, inc=1, device_id=peer(lax.rem(me + k, count)), device_id_type=DT)
        return carry

    lax.fori_loop(1, count, greet, 0)
    pl.semaphore_wait(bar, count - 1)

    def copy(k):
        i = lax.rem(me + k, count)
        return pltpu.make_async_remote_copy(
            src.at[i] if scatter else src, out.at[me], send_sem.at[k], recv_sem.at[me],
            device_id=peer(i), device_id_type=DT,
        )

    def send(k, carry):
        copy(k).start()
        return carry

    own = pltpu.make_async_copy(src.at[me] if scatter else src, out.at[me], own_sem)
    own.start()
    lax.fori_loop(1, count, send, 0)
    own.wait()

    def finish(k, carry):
        i = lax.rem(me + k, count)
        pltpu.make_async_remote_copy(
            src.at[i] if scatter else src, out.at[i], send_sem.at[k], recv_sem.at[i],
            device_id=peer(i), device_id_type=DT,
        ).wait_recv()
        copy(k).wait_send()
        return carry

    lax.fori_loop(1, count, finish, 0)


def small_exchange(src, shards, every, scatter, call_id):
    count = shards * 2 * (2 if every else 1)
    shape = src.shape[1:] if scatter else src.shape
    sem = pltpu.SemaphoreType.DMA
    vm = pl.BlockSpec(memory_space=pltpu.VMEM)
    return pl.pallas_call(
        partial(small_kernel, shards, every, scatter),
        out_shape=jax.ShapeDtypeStruct((count, *shape), src.dtype),
        in_specs=[vm],
        out_specs=vm,
        scratch_shapes=[sem, sem((count,)), sem((count,))],
        compiler_params=pltpu.CompilerParams(collective_id=call_id, has_side_effects=True),
        name=f"small_exchange_{call_id}",
    )(src)


def adapt(weight, gradient, moment, second, token_total):
    scaled_grad = gradient / token_total
    new_moment = 0.5 * moment + 0.5 * scaled_grad
    new_second = 0.5 * second + 0.5 * scaled_grad * scaled_grad
    direction = new_moment / (jnp.sqrt(new_second) + 1e-06) + 0.01 * weight
    return (new_moment, new_second, direction)


def shards_fn(
    tokens, frames, cotangent, attention_weights, dense_weights, unit_bias, norm_bias,
    attention_mean, dense_mean, unit_mean, norm_mean,
    attention_square, dense_square, unit_square, norm_square,
):
    f32, bf = jnp.float32, jnp.bfloat16
    shards = lax.axis_size("dp")
    rows = D // shards
    c = lax.axis_index("core")
    unit_cols = unit_bias.shape[1]
    column_rows = (lax.axis_index("dp") * unit_cols + jnp.arange(unit_cols, dtype=jnp.int32)) // HD
    row_pick = (column_rows[:, None] == jnp.arange(8, dtype=jnp.int32)[None, :]).astype(f32)
    leader = ((lax.axis_index("side") == 0) & (c == 0)).astype(f32)

    def square_rows(attn_part, dense_part, unit_part, norm_part):
        unit_sums = jnp.sum(jnp.sum(unit_part * unit_part, axis=0)[:, None] * row_pick, axis=0)
        return jnp.concatenate(
            [
                jnp.sum(attn_part * attn_part, axis=(2, 3)).reshape(8),
                jnp.sum(dense_part * dense_part, axis=(1, 2, 3)),
                unit_sums,
                jnp.sum(norm_part * norm_part, axis=1) * leader,
            ]
        )

    own_attn = attention_weights.astype(f32)
    own_dense = dense_weights.astype(f32)
    own_unit = unit_bias.astype(f32)
    own_norm = norm_bias.astype(f32)

    if rows == 128:
        pack = jnp.concatenate([norm_bias.astype(f32), unit_bias.astype(f32).reshape(2, 128)])
        small = (jnp.pad(pack, ((0, 5), (0, 0))), jnp.zeros((8, 128), f32), jnp.zeros((8, 128), f32))
    else:
        pack = jnp.concatenate([norm_bias.reshape(-1), unit_bias.reshape(-1)])
        pack = jnp.pad(pack, (0, 2048 - pack.shape[0])).reshape(16, 128)
        packs = small_exchange(pack, shards, False, False, 2).reshape(shards, 2, 2048)
        norm_rows = packs[:, 0, : 9 * rows].reshape(shards, 9, rows).transpose(1, 0, 2).reshape(9, D).astype(f32)
        unit_all = packs[:, :, 9 * rows : 9 * rows + 4 * unit_cols].reshape(shards, 2, 4, unit_cols)
        bias_rows = (
            unit_all.transpose(1, 2, 0, 3).reshape(2, 4, 8, HD).transpose(2, 0, 1, 3).reshape(16, COLS).astype(f32)
        )
        small = (jnp.zeros((16, 128), f32), jnp.pad(norm_rows, ((0, 7), (0, 0))), bias_rows)

    shard = jnp.concatenate(
        [attention_weights.reshape(8, rows, COLS), dense_weights.transpose(0, 2, 1, 3).reshape(8, rows, COLS)]
    )
    kept = forward(shard, tokens, jnp.pad(frames, ((0, KEYS - HALF_FRAMES), (0, 0))), cotangent, small, shards)
    layer_out = kept.layer_out
    def by_matrix(attn, dense):
        return attn.reshape(8, rows, COLS), dense.transpose(0, 2, 1, 3).reshape(8, rows, COLS)

    def from_matrix(attn, dense):
        return attn.reshape(2, 4, rows, COLS), dense.reshape(2, 4, rows, COLS).transpose(0, 2, 1, 3)

    token_total = float(tokens.shape[0] * shards * 4)
    state = (
        *by_matrix(attention_mean, dense_mean), *by_matrix(attention_square, dense_square), shard, small[0],
        norm_mean, unit_mean, norm_square, unit_square,
    )
    done = BackwardOut(*backward(kept, state, token_total, shards))
    input_gradient, frame_gradient = done.input_out, done.frame_out
    attention_owned, dense_owned = from_matrix(done.owned_attn, done.owned_dense)
    small_grads = (done.small_out, done.bcols_out)

    if rows == 128:
        unit_owned, norm_owned = done.unit_out, done.norm_out
    else:
        norm_parts = small_grads[0][:9].reshape(9, shards, rows).transpose(1, 0, 2).reshape(shards, 1, 9 * rows)
        unit_parts = small_grads[1].reshape(8, 2, 4, HD).transpose(1, 2, 0, 3).reshape(2, 4, shards, unit_cols)
        unit_parts = unit_parts.transpose(2, 0, 1, 3).reshape(shards, 2, 4 * unit_cols)
        small = jnp.concatenate([jnp.broadcast_to(norm_parts, (shards, 2, 9 * rows)), unit_parts], axis=2)
        small = jnp.pad(small, ((0, 0), (0, 0), (0, 2048 - small.shape[2]))).reshape(shards * 2, 16, 128)
        small = jnp.sum(small_exchange(small, shards, False, True, 13), axis=0).reshape(2048)
        norm_owned = small[: 9 * rows].reshape(9, rows)
        unit_owned = small[9 * rows : 9 * rows + 4 * unit_cols].reshape(4, unit_cols)

    attn_moment, attn_second, attn_dir = adapt(
        own_attn, attention_owned, attention_mean, attention_square, token_total
    )
    dense_moment, dense_second, dense_dir = adapt(
        own_dense, dense_owned, dense_mean, dense_square, token_total
    )
    unit_moment, unit_second, unit_dir = adapt(
        own_unit, unit_owned, unit_mean, unit_square, token_total
    )
    norm_moment, norm_second, norm_dir = adapt(
        own_norm, norm_owned, norm_mean, norm_square, token_total
    )
    if rows == 128:
        weight_norms, step_norms = done.norms[0, :27], done.norms[1, :27]
    else:
        sums = jnp.concatenate(
            [
                square_rows(own_attn, own_dense, own_unit, own_norm),
                square_rows(attn_dir, dense_dir, unit_dir, norm_dir),
            ]
        )
        sums = jnp.pad(sums, (0, 1024 - 54)).reshape(8, 128)
        sums = jnp.sum(small_exchange(sums, shards, True, False, 14), axis=0).reshape(1024)
        weight_norms = jnp.sqrt(sums[:27])
        step_norms = jnp.sqrt(sums[27:54])
    trust = weight_norms / step_norms
    attention_step = -learning_rate * trust[0:8].reshape(2, 4, 1, 1) * attn_dir
    dense_step = -learning_rate * trust[8:10].reshape(2, 1, 1, 1) * dense_dir
    unit_factor = jnp.sum(row_pick * trust[10:18][None, :], axis=1)
    unit_step = -learning_rate * unit_factor[None, :] * unit_dir
    norm_step = -learning_rate * trust[18:27][:, None] * norm_dir
    return (
        layer_out, input_gradient, frame_gradient,
        attention_owned, dense_owned, unit_owned, norm_owned,
        attn_moment, dense_moment, unit_moment, norm_moment,
        attn_second, dense_second, unit_second, norm_second,
        attention_step, dense_step, unit_step, norm_step,
        weight_norms, step_norms,
    )


def solution(mesh):
    shards = mesh.shape["dp"]
    inner = Mesh(mesh.devices.reshape(shards, 2, 2), AXES)
    tensor = ("side", "core")
    rows = P(("dp", *tensor), None)
    state = (P(None, None, "dp", tensor), P(None, "dp", None, tensor), P(tensor, "dp"), P(None, "dp"))
    return jax.shard_map(
        shards_fn,
        mesh=inner,
        in_specs=(rows, rows, rows) + state * 3,
        out_specs=(rows, rows, rows) + state * 4 + (P(), P()),
        check_vma=False,
    )
```
